64 devices in a mesh: dp: 4 (over x, y), ep: 16 (over z, core).
Axes of the slice: x: 2, y: 2, z: 8, core: 2. Of those that a mesh axis runs over, the one named last changes fastest.
The devices are a block of a 4x4x8 slice.
Arguments:
- hidden: bfloat16 [8192, 1024], P(('dp', 'ep')), parts along dimension 0
- k_cache: bfloat16 [8192, 32, 8, 64], P(('dp', 'ep')), parts along dimension 0
- v_cache: bfloat16 [8192, 32, 8, 64], P(('dp', 'ep')), parts along dimension 0
- seq_lens: int32 [8192], P(('dp', 'ep')), parts along dimension 0
- expert_ids: int32 [8192, 8], P(('dp', 'ep')), parts along dimension 0
- ln_attn: bfloat16 [1024], replicated
- w_q: bfloat16 [1024, 1024], replicated
- w_k: bfloat16 [1024, 512], replicated
- w_v: bfloat16 [1024, 512], replicated
- q_gain: bfloat16 [64], replicated
- k_gain: bfloat16 [64], replicated
- w_o: bfloat16 [1024, 1024], replicated
- ln_moe: bfloat16 [1024], replicated
- w_router: bfloat16 [1024, 32], replicated
- w_gate: bfloat16 [32, 1024, 512], P('ep')
- w_up: bfloat16 [32, 1024, 512], P('ep')
- w_down: bfloat16 [32, 512, 1024], P('ep')
Outputs:
- output 1: bfloat16 [8192, 1024], P(('dp', 'ep')), parts along dimension 0
- output 2: bfloat16 [8192, 32, 8, 64], P(('dp', 'ep')), parts along dimension 0
- output 3: bfloat16 [8192, 32, 8, 64], P(('dp', 'ep')), parts along dimension 0
There are 4 independent parts. The reference program is written for one: setup_inputs(seed, part) draws one part's arguments, and reference() takes and returns one part's arrays. A program takes and returns all parts, laid end to end along the dimension named above; an argument that names none is the same for every part.
All inputs are finite; a program needn't handle non-finite values.
Results may differ from the reference program's by a relative error of at most 0.00558231.
Values are sent between devices in bfloat16 or wider.
A program may use at most 768 MiB of HBM per device.

```python
import jax
import jax.numpy as jnp
import numpy as np
from jax import lax

D = 1024
HEADS = 16
KV_HEADS = 8
HEAD = 64
EXPERTS = 32
FF = 512
TOP = 8
ROPE_BASE = 1000000
TMAX = 32
SEQ_DEV = 128
GROUP = 16

BATCH = SEQ_DEV * GROUP
CAP = 2 * SEQ_DEV // (EXPERTS // TOP)
EPS = 1e-6


def draw_routing(route_key):
    group_width = EXPERTS // TOP
    pos_table = np.array([0 if tok_num < CAP else 1 + (tok_num - CAP) % (group_width - 1) for tok_num in range(SEQ_DEV)], dtype=np.int32)
    perm_key, tok_key = jax.random.split(route_key)
    expert_perm = jax.random.permutation(perm_key, EXPERTS).astype(jnp.int32)
    tok_keys = jax.random.split(tok_key, GROUP * TOP)
    tok_perms = jax.vmap(lambda one_key: jax.random.permutation(one_key, SEQ_DEV))(tok_keys)
    positions = jnp.asarray(pos_table)[tok_perms].reshape(GROUP, TOP, SEQ_DEV)
    offsets = (jnp.arange(TOP, dtype=jnp.int32) * group_width)[None, :, None]
    chosen_ids = expert_perm[offsets + positions]
    return jnp.transpose(chosen_ids, (0, 2, 1)).reshape(BATCH, TOP).astype(jnp.int32)


def draw_lens(len_key):
    spread_key, raw_key = jax.random.split(len_key)
    spread = jax.random.randint(spread_key, (GROUP, 1), 1, 5)
    raw_lens = jax.random.randint(raw_key, (GROUP, SEQ_DEV), 0, TMAX)
    seq_lens = (raw_lens * spread // 4).reshape(BATCH)
    return seq_lens.at[0].set(TMAX - 1).astype(jnp.int32)


def setup_inputs(seed: int = 0, part: int = 0) -> dict:
    base_key = jax.random.key(seed)
    shared_keys = jax.random.split(base_key, 12)
    part_keys = jax.random.split(jax.random.fold_in(base_key, part), 5)
    hidden = jax.random.normal(part_keys[0], (BATCH, D), jnp.float32).astype(jnp.bfloat16)
    k_cache = (1.5 * jax.random.normal(part_keys[1], (BATCH, TMAX, KV_HEADS, HEAD), jnp.float32)).astype(jnp.bfloat16)
    v_cache = jax.random.normal(part_keys[2], (BATCH, TMAX, KV_HEADS, HEAD), jnp.float32).astype(jnp.bfloat16)
    seq_lens = draw_lens(part_keys[3])
    expert_ids = draw_routing(part_keys[4])
    ln_attn = (1.0 + 0.2 * jax.random.normal(shared_keys[0], (D,), jnp.float32)).astype(jnp.bfloat16)
    w_q = (jax.random.normal(shared_keys[1], (D, HEADS * HEAD), jnp.float32) * D ** -0.5).astype(jnp.bfloat16)
    w_k = (jax.random.normal(shared_keys[2], (D, KV_HEADS * HEAD), jnp.float32) * D ** -0.5).astype(jnp.bfloat16)
    w_v = (jax.random.normal(shared_keys[3], (D, KV_HEADS * HEAD), jnp.float32) * D ** -0.5).astype(jnp.bfloat16)
    q_gain = (1.6 + 0.3 * jax.random.normal(shared_keys[4], (HEAD,), jnp.float32)).astype(jnp.bfloat16)
    k_gain = (1.6 + 0.3 * jax.random.normal(shared_keys[5], (HEAD,), jnp.float32)).astype(jnp.bfloat16)
    w_o = (jax.random.normal(shared_keys[6], (HEADS * HEAD, D), jnp.float32) * (HEADS * HEAD) ** -0.5).astype(jnp.bfloat16)
    ln_moe = (1.0 + 0.2 * jax.random.normal(shared_keys[7], (D,), jnp.float32)).astype(jnp.bfloat16)
    w_router = (2.0 * jax.random.normal(shared_keys[8], (D, EXPERTS), jnp.float32) * D ** -0.5).astype(jnp.bfloat16)
    w_gate = (jax.random.normal(shared_keys[9], (EXPERTS, D, FF), jnp.float32) * D ** -0.5).astype(jnp.bfloat16)
    w_up = (jax.random.normal(shared_keys[10], (EXPERTS, D, FF), jnp.float32) * D ** -0.5).astype(jnp.bfloat16)
    w_down = (2.0 * jax.random.normal(shared_keys[11], (EXPERTS, FF, D), jnp.float32) * FF ** -0.5).astype(jnp.bfloat16)
    return {'hidden': hidden, 'k_cache': k_cache, 'v_cache': v_cache, 'seq_lens': seq_lens, 'expert_ids': expert_ids, 'ln_attn': ln_attn, 'w_q': w_q, 'w_k': w_k, 'w_v': w_v, 'q_gain': q_gain, 'k_gain': k_gain, 'w_o': w_o, 'ln_moe': ln_moe, 'w_router': w_router, 'w_gate': w_gate, 'w_up': w_up, 'w_down': w_down}


def rms_scale(values, gain_vec):
    mean_sq = jnp.mean(values * values, axis=-1, keepdims=True)
    return values * lax.rsqrt(mean_sq + EPS) * gain_vec.astype(jnp.float32)


def rotate_half(values, angles):
    half_dim = values.shape[-1] // 2
    x_low = values[..., :half_dim]
    x_high = values[..., half_dim:]
    cos_val = jnp.cos(angles)
    sin_val = jnp.sin(angles)
    return jnp.concatenate([x_low * cos_val - x_high * sin_val, x_high * cos_val + x_low * sin_val], axis=-1)


def attend(hidden, k_cache, v_cache, seq_lens, ln_attn, w_q, w_k, w_v, q_gain, k_gain, w_o):
    n_seq = hidden.shape[0]
    h_f32 = hidden.astype(jnp.float32)
    x_norm = rms_scale(h_f32, ln_attn).astype(jnp.bfloat16)
    q_proj = jnp.dot(x_norm, w_q, preferred_element_type=jnp.float32).reshape(n_seq, HEADS, HEAD)
    k_proj = jnp.dot(x_norm, w_k, preferred_element_type=jnp.float32).reshape(n_seq, KV_HEADS, HEAD)
    v_new = jnp.dot(x_norm, w_v, preferred_element_type=jnp.float32).astype(jnp.bfloat16).reshape(n_seq, KV_HEADS, HEAD)
    inv_freq = jnp.power(float(ROPE_BASE), -jnp.arange(0, HEAD, 2).astype(jnp.float32) / HEAD)
    angles = seq_lens.astype(jnp.float32)[:, None, None] * inv_freq[None, None, :]
    q_rot = rotate_half(rms_scale(q_proj, q_gain), angles).astype(jnp.bfloat16)
    k_new = rotate_half(rms_scale(k_proj, k_gain), angles).astype(jnp.bfloat16)
    positions = jnp.arange(TMAX, dtype=jnp.int32)
    at_slot = (positions[None, :] == seq_lens[:, None])[:, :, None, None]
    k_all = jnp.where(at_slot, k_new[:, None], k_cache)
    v_all = jnp.where(at_slot, v_new[:, None], v_cache)
    q_grp = q_rot.reshape(n_seq, KV_HEADS, HEADS // KV_HEADS, HEAD)
    scores = jnp.einsum('skgd,stkd->skgt', q_grp.astype(jnp.float32), k_all.astype(jnp.float32)) * (HEAD ** -0.5)
    visible = (positions[None, :] <= seq_lens[:, None])[:, None, None, :]
    scores = jnp.where(visible, scores, -1e30)
    att_probs = jax.nn.softmax(scores, axis=-1).astype(jnp.bfloat16)
    attn_out = jnp.einsum('skgt,stkd->skgd', att_probs.astype(jnp.float32), v_all.astype(jnp.float32))
    attn_out = attn_out.astype(jnp.bfloat16).reshape(n_seq, HEADS * HEAD)
    y_res = h_f32 + jnp.dot(attn_out, w_o, preferred_element_type=jnp.float32)
    return y_res, k_all, v_all


def reference(hidden, k_cache, v_cache, seq_lens, expert_ids, ln_attn, w_q, w_k, w_v, q_gain, k_gain, w_o, ln_moe, w_router, w_gate, w_up, w_down):
    def block_attn(block_in):
        h_blk, kc_blk, vc_blk, len_blk = block_in
        return attend(h_blk, kc_blk, vc_blk, len_blk, ln_attn, w_q, w_k, w_v, q_gain, k_gain, w_o)

    y_blocks, k_blocks, v_blocks = lax.map(block_attn, (hidden.reshape(GROUP, SEQ_DEV, D), k_cache.reshape(GROUP, SEQ_DEV, TMAX, KV_HEADS, HEAD), v_cache.reshape(GROUP, SEQ_DEV, TMAX, KV_HEADS, HEAD), seq_lens.reshape(GROUP, SEQ_DEV)))
    y_res = y_blocks.reshape(BATCH, D)
    k_all = k_blocks.reshape(BATCH, TMAX, KV_HEADS, HEAD)
    v_all = v_blocks.reshape(BATCH, TMAX, KV_HEADS, HEAD)

    r_norm = rms_scale(y_res, ln_moe).astype(jnp.bfloat16)
    logits = jnp.dot(r_norm, w_router, preferred_element_type=jnp.float32)
    gate_vals = jax.nn.softmax(jnp.take_along_axis(logits, expert_ids, axis=1), axis=-1)

    n_pairs = BATCH * TOP
    per_expert = GROUP * CAP
    flat_ids = expert_ids.reshape(n_pairs)
    sort_order = jnp.argsort(flat_ids, stable=True)
    sorted_tok = (sort_order // TOP).astype(jnp.int32)
    counts = jnp.bincount(flat_ids, length=EXPERTS).astype(jnp.int32)
    starts = jnp.cumsum(counts) - counts
    tok_padded = jnp.concatenate([sorted_tok, jnp.zeros((per_expert,), jnp.int32)])

    def run_expert(expert_in):
        start_at, w_gate_e, w_up_e, w_down_e = expert_in
        tok_idx = lax.dynamic_slice(tok_padded, (start_at,), (per_expert,))
        tok_rows = jnp.take(r_norm, tok_idx, axis=0)
        gate_pre = jnp.dot(tok_rows, w_gate_e, preferred_element_type=jnp.float32)
        up_pre = jnp.dot(tok_rows, w_up_e, preferred_element_type=jnp.float32)
        hidden_act = (jax.nn.silu(gate_pre) * up_pre).astype(jnp.bfloat16)
        return jnp.dot(hidden_act, w_down_e, preferred_element_type=jnp.float32).astype(jnp.bfloat16)

    expert_out = lax.map(run_expert, (starts, w_gate, w_up, w_down))
    inverse = jnp.argsort(sort_order)
    pair_rank = inverse - starts[flat_ids]
    picked = expert_out[flat_ids, pair_rank].reshape(BATCH, TOP, D).astype(jnp.float32)
    moe_out = jnp.sum(gate_vals[:, :, None] * picked, axis=1)
    return (y_res + moe_out).astype(jnp.bfloat16), k_all, v_all
```

```python
import functools

import jax
import jax.numpy as jnp
import numpy as np
from jax import lax
from jax.experimental import pallas as pl
from jax.experimental.pallas import tpu as pltpu
from jax.sharding import PartitionSpec as P

EPS = 1e-6
ROPE_BASE = 1000000.0
F32 = jnp.float32
BF16 = jnp.bfloat16
MESH = pl.DeviceIdType.MESH


def attend_kernel(h_ref, lens_ref, ids_ref, ln_a_ref, qg_ref, kg_ref, ln_m_ref, freq_ref, wr_ref,
                  wq_hbm, wk_hbm, wv_hbm, wo_hbm, kc_hbm, vc_hbm,
                  kn_hbm, vn_hbm, y_ref, r_ref, gate_ref,
                  kbuf, vbuf, wq, wk, wv, wo, qrot, knew, vnew, score, attn, in_sem, out_sem):
    t_max, n_kv, hd, n_seq = kc_hbm.shape
    n_heads = wq_hbm.shape[1] // hd
    grp = n_heads // n_kv
    half = hd // 2
    n_chunk = 4
    tc = t_max // n_chunk

    w_copies = [pltpu.make_async_copy(src, dst, in_sem.at[i])
                for i, (src, dst) in enumerate(((wk_hbm, wk), (wq_hbm, wq), (wv_hbm, wv), (wo_hbm, wo)))]
    k_in = [pltpu.make_async_copy(kc_hbm.at[pl.ds(c * tc, tc)], kbuf.at[pl.ds(c * tc, tc)], in_sem.at[4 + c]) for c in range(n_chunk)]
    v_in = [pltpu.make_async_copy(vc_hbm.at[pl.ds(c * tc, tc)], vbuf.at[pl.ds(c * tc, tc)], in_sem.at[4 + n_chunk + c]) for c in range(n_chunk)]
    k_out = [pltpu.make_async_copy(kbuf.at[pl.ds(c * tc, tc)], kn_hbm.at[pl.ds(c * tc, tc)], out_sem.at[c]) for c in range(n_chunk)]
    v_out = [pltpu.make_async_copy(vbuf.at[pl.ds(c * tc, tc)], vn_hbm.at[pl.ds(c * tc, tc)], out_sem.at[n_chunk + c]) for c in range(n_chunk)]
    for copy in w_copies[:3] + k_in + v_in + w_copies[3:]:
        copy.start()

    h32 = h_ref[...].astype(F32)
    mean_sq = jnp.mean(h32 * h32, axis=1, keepdims=True)
    x = (h32 * lax.rsqrt(mean_sq + EPS) * ln_a_ref[...].astype(F32)).astype(BF16)

    lens = lens_ref[...]
    angles = lens.astype(F32) * freq_ref[...]
    cos_v = jnp.cos(angles)
    sin_v = jnp.sin(angles)

    def gain_tile(g_ref):
        row = g_ref[...].astype(F32)
        row = jnp.concatenate([row] * (n_seq // hd), axis=1)
        return jnp.transpose(jnp.broadcast_to(row, (n_seq, n_seq)))[:hd, :]

    def rope_heads(proj, gain, dst, heads):
        for i in range(heads):
            if i % 2 == 0:
                pair = jnp.transpose(proj[:, i * hd:(i + 2) * hd])
            vals = pair[(i % 2) * hd:(i % 2 + 1) * hd, :]
            ms = jnp.mean(vals * vals, axis=0, keepdims=True)
            vals = vals * lax.rsqrt(ms + EPS) * gain
            low, high = vals[:half, :], vals[half:, :]
            dst[i * hd:i * hd + half, :] = (low * cos_v - high * sin_v).astype(BF16).astype(F32)
            dst[i * hd + half:(i + 1) * hd, :] = (high * cos_v + low * sin_v).astype(BF16).astype(F32)

    w_copies[0].wait()
    rope_heads(jnp.dot(x, wk[...], preferred_element_type=F32), gain_tile(kg_ref), knew, n_kv)
    w_copies[1].wait()
    rope_heads(jnp.dot(x, wq[...], preferred_element_type=F32), gain_tile(qg_ref), qrot, n_heads)
    w_copies[2].wait()
    v_proj = jnp.dot(x, wv[...], preferred_element_type=F32)
    for i in range(0, n_kv, 2):
        vnew[i * hd:(i + 2) * hd, :] = jnp.transpose(v_proj[:, i * hd:(i + 2) * hd]).astype(BF16).astype(F32)

    for c in range(n_chunk):
        k_in[c].wait()

        def k_body(kv, carry, c=c):
            new = knew[pl.ds(pl.multiple_of(kv * hd, hd), hd), :]
            qs = [qrot[pl.ds(pl.multiple_of((kv * grp + g) * hd, hd), hd), :] for g in range(grp)]
            rows = [[] for _ in range(grp)]
            for tt in range(tc):
                t = c * tc + tt
                kt = jnp.where(lens == t, new, kbuf[t, kv].astype(F32))
                kbuf[t, kv] = kt.astype(BF16)
                for g in range(grp):
                    rows[g].append(jnp.sum(kt * qs[g], axis=0, keepdims=True))
            for g in range(grp):
                score[kv * grp + g, c * tc:(c + 1) * tc, :] = jnp.concatenate(rows[g], axis=0)
            return carry

        lax.fori_loop(0, n_kv, k_body, 0)
        k_out[c].start()

    visible = lax.broadcasted_iota(jnp.int32, (t_max, n_seq), 0) <= lens

    def soft_body(j, carry):
        s = jnp.where(visible, score[j] * (hd ** -0.5), -1e30)
        e = jnp.exp(s - jnp.max(s, axis=0, keepdims=True))
        score[j] = (e / jnp.sum(e, axis=0, keepdims=True)).astype(BF16).astype(F32)
        return carry

    lax.fori_loop(0, n_heads, soft_body, 0, unroll=2)

    for c in range(n_chunk):
        v_in[c].wait()

        def v_body(kv, carry, c=c):
            new = vnew[pl.ds(pl.multiple_of(kv * hd, hd), hd), :]
            at = [pl.ds(pl.multiple_of((kv * grp + g) * hd, hd), hd) for g in range(grp)]
            acc = [None if c == 0 else attn[at[g], :] for g in range(grp)]
            for tt in range(tc):
                t = c * tc + tt
                vt = jnp.where(lens == t, new, vbuf[t, kv].astype(F32))
                vbuf[t, kv] = vt.astype(BF16)
                for g in range(grp):
                    term = vt * score[kv * grp + g, t:t + 1, :]
                    acc[g] = term if acc[g] is None else acc[g] + term
            for g in range(grp):
                attn[at[g], :] = acc[g]
            return carry

        lax.fori_loop(0, n_kv, v_body, 0)
        v_out[c].start()

    w_copies[3].wait()
    a_rows = jnp.concatenate([jnp.transpose(attn[i * n_seq:(i + 1) * n_seq, :]).astype(BF16) for i in range(n_heads * hd // n_seq)], axis=1)
    y = h32 + jnp.dot(a_rows, wo[...], preferred_element_type=F32)
    y_ref[...] = y
    mean_sq = jnp.mean(y * y, axis=1, keepdims=True)
    r = (y * lax.rsqrt(mean_sq + EPS) * ln_m_ref[...].astype(F32)).astype(BF16)
    r_ref[...] = r
    logits = lax.dot_general(wr_ref[...], r, (((1,), (1,)), ((), ())), preferred_element_type=F32)
    e_iota = lax.broadcasted_iota(jnp.int32, logits.shape, 0)
    ids = ids_ref[...]
    chosen = e_iota == ids[0:1, :]
    for i in range(1, ids.shape[0]):
        chosen = chosen | (e_iota == ids[i:i + 1, :])
    top = jnp.max(jnp.where(chosen, logits, -jnp.inf), axis=0, keepdims=True)
    e = jnp.where(chosen, jnp.exp(logits - top), 0.0)
    gate_ref[...] = jnp.where(chosen, e / jnp.sum(e, axis=0, keepdims=True), -1.0)

    for copy in k_out + v_out:
        copy.wait()


def attend(hidden, k_t, v_t, lens, ids_t, ln_attn, w_q, w_k, w_v, q_gain, k_gain, w_o, ln_moe, w_router_t):
    n_seq, d = hidden.shape
    t_max, n_kv, hd, _ = k_t.shape
    hq, hk = w_q.shape[1], w_k.shape[1]
    n_heads = hq // hd
    n_exp = w_router_t.shape[0]
    freq = np.power(ROPE_BASE, -np.arange(0, hd, 2).astype(np.float32) / hd).astype(np.float32)
    freq = jnp.asarray(np.broadcast_to(freq[:, None], (hd // 2, n_seq)))
    vm = pl.BlockSpec(memory_space=pltpu.VMEM)
    anyspace = pl.BlockSpec(memory_space=pl.ANY)
    return pl.pallas_call(
        attend_kernel,
        out_shape=(
            jax.ShapeDtypeStruct(k_t.shape, k_t.dtype),
            jax.ShapeDtypeStruct(v_t.shape, v_t.dtype),
            jax.ShapeDtypeStruct((n_seq, d), F32),
            jax.ShapeDtypeStruct((n_seq, d), BF16),
            jax.ShapeDtypeStruct((n_exp, n_seq), F32),
        ),
        in_specs=[vm] * 9 + [anyspace] * 6,
        out_specs=(anyspace, anyspace, vm, vm, vm),
        scratch_shapes=[
            pltpu.VMEM(k_t.shape, BF16), pltpu.VMEM(v_t.shape, BF16),
            pltpu.VMEM(w_q.shape, BF16), pltpu.VMEM(w_k.shape, BF16), pltpu.VMEM(w_v.shape, BF16), pltpu.VMEM(w_o.shape, BF16),
            pltpu.VMEM((hq, n_seq), F32), pltpu.VMEM((hk, n_seq), F32), pltpu.VMEM((hk, n_seq), F32),
            pltpu.VMEM((n_heads, t_max, n_seq), F32), pltpu.VMEM((hq, n_seq), F32),
            pltpu.SemaphoreType.DMA((12,)), pltpu.SemaphoreType.DMA((8,)),
        ],
        compiler_params=pltpu.CompilerParams(vmem_limit_bytes=30 * 1024 * 1024),
        name="attend",
    )(hidden, lens, ids_t, ln_attn, q_gain, k_gain, ln_moe, freq, w_router_t, w_q, w_k, w_v, w_o, k_t, v_t)


def moe_kernel(n, r_ref, gate_ref, y_ref, wg_hbm, wu_hbm, wd_hbm, out_ref,
               xbuf, gbuf, cboth, cpart, inc, wg, wu, wd, act, gcol,
               w_sem, own_sem, ring_send, ring_recv, gate_send, gate_recv,
               pair_send, pair_recv, pgate_send, pgate_recv, self_send, self_recv,
               sum_send, sum_recv, rs_send, rs_recv):
    me = lax.axis_index("ep")
    chip = me // 2
    core = lax.rem(me, 2)
    other = 1 - core
    half = n // 2
    n_unit = n - 1
    rows, d = r_ref.shape
    n_local = wg_hbm.shape[0]
    hr = rows // 2
    qr = hr // 2

    def at_chip(step):
        return lax.rem(chip + step + n, n)

    def ring_dev(direction):
        return {"ep": 2 * at_chip(1 if direction == 0 else -1) + core}

    pair_dev = {"ep": 2 * chip + other}

    def remote(src, dst, ssem, rsem, dev):
        return pltpu.make_async_remote_copy(src_ref=src, dst_ref=dst, send_sem=ssem, recv_sem=rsem, device_id=dev, device_id_type=MESH)

    barrier = pltpu.get_barrier_semaphore()
    for dev in (ring_dev(0), ring_dev(1), pair_dev):
        pl.semaphore_signal(barrier, inc=1, device_id=dev, device_id_type=MESH)

    w_copies = [pltpu.make_async_copy(src, dst, w_sem.at[i]) for i, (src, dst) in enumerate(((wg_hbm, wg), (wu_hbm, wu), (wd_hbm, wd)))]
    own_copies = [pltpu.make_async_copy(r_ref, xbuf.at[chip, core], own_sem.at[0]),
                  pltpu.make_async_copy(gate_ref, gbuf.at[chip, core], own_sem.at[1])]
    for copy in own_copies + w_copies:
        copy.start()
    for copy in own_copies:
        copy.wait()
    pl.semaphore_wait(barrier, 3)

    def unit_half(direction, u):
        return u % 2 if direction == 0 else 1 - u % 2

    def unit_from(direction, u):
        s = u // 2 + 1
        return at_chip(-s if direction == 0 else s)

    def has_gate(direction, u):
        return u % 2 == 0 and (direction == 0 or u < n_unit - 1)

    def x_at(i, c, direction, u):
        return xbuf.at[i, c, pl.ds(unit_half(direction, u) * hr, hr)]

    def ring_copy(direction, u, i):
        ref = x_at(i, core, direction, u)
        return remote(ref, ref, ring_send.at[direction, u], ring_recv.at[direction, u], ring_dev(direction))

    def ring_gate(direction, u, i):
        ref = gbuf.at[i, core]
        return remote(ref, ref, gate_send.at[direction, u // 2], gate_recv.at[direction, u // 2], ring_dev(direction))

    def pair_copy(direction, u, i, c):
        ref = x_at(i, c, direction, u)
        return remote(ref, ref, pair_send.at[direction, u], pair_recv.at[direction, u], pair_dev)

    def pair_gate(direction, u, i, c):
        ref = gbuf.at[i, c]
        return remote(ref, ref, pgate_send.at[direction, u // 2], pgate_recv.at[direction, u // 2], pair_dev)

    def self_copies(c):
        return [remote(xbuf.at[chip, c], xbuf.at[chip, c], self_send.at[0], self_recv.at[0], pair_dev),
                remote(gbuf.at[chip, c], gbuf.at[chip, c], self_send.at[1], self_recv.at[1], pair_dev)]

    def send_chip(direction, u):
        s = u // 2
        return at_chip(-s if direction == 0 else s)

    def start_unit(direction, u):
        i = send_chip(direction, u)
        if has_gate(direction, u):
            ring_gate(direction, u, i).start()
        ring_copy(direction, u, i).start()

    for u in range(2):
        for direction in range(2):
            start_unit(direction, u)
        if u == 0:
            for copy in self_copies(core):
                copy.start()

    def take_unit(u):
        for direction in range(2):
            i = unit_from(direction, u)
            if has_gate(direction, u):
                ring_gate(direction, u, i).wait_recv()
            ring_copy(direction, u, i).wait_recv()
            if u + 2 < n_unit:
                start_unit(direction, u + 2)
            if has_gate(direction, u):
                pair_gate(direction, u, i, core).start()
            pair_copy(direction, u, i, core).start()

    def wait_pair(direction, u):
        i = unit_from(direction, u)
        if has_gate(direction, u):
            pair_gate(direction, u, i, other).wait_recv()
        pair_copy(direction, u, i, other).wait_recv()

    def sum_copy(k, i):
        return remote(cboth.at[i, other], cpart.at[i], sum_send.at[k], sum_recv.at[k], pair_dev)

    def order_step(k):
        return 0 if k == 0 else (-((k + 1) // 2) if k % 2 == 1 and k < n - 1 else (k + 1) // 2)

    order = [order_step(k) for k in range(n)]

    def rs_list(direction):
        lh, sh = (0, 1) if direction == 0 else (1, 0)
        seq = [(half - 1, sh, 0), (half, lh, 0), (half, lh, 1), (half - 1, sh, 1)]
        for q in range(half - 1, 0, -1):
            seq += [(q, lh, 0), (q, lh, 1)]
            if q > 1:
                seq += [(q - 1, sh, 0), (q - 1, sh, 1)]
        return seq

    rs_lists = [rs_list(0), rs_list(1)]

    def rs_copy(direction, u):
        q, h, p = rs_lists[direction][u]
        t = at_chip(q if direction == 0 else -q)
        at = pl.ds(h * hr + p * qr, qr)
        return remote(cboth.at[t, core, at], inc.at[direction, q - 1, at], rs_send.at[direction, u], rs_recv.at[direction, u], ring_dev(direction))

    def rs_step(direction, u):
        q, h, p = rs_lists[direction][u]
        step = q if direction == 0 else -q
        t = at_chip(step)
        at = pl.ds(h * hr + p * qr, qr)
        total = cboth[t, core, at, :] + cpart[t, at, :]
        if (q + 1, h, p) in rs_lists[direction]:
            rs_copy(direction, rs_lists[direction].index((q + 1, h, p))).wait_recv()
            total = total + inc[direction, q, at, :]
        cboth[t, core, at, :] = total
        rs_copy(direction, u).start()

    def wait_sum(step):
        step = step if step in order else step + n if step + n in order else step - n
        k = order.index(step)
        sum_copy(k, at_chip(step)).wait_recv()

    def before(k):
        if k == 0:
            for copy in self_copies(other):
                copy.wait_recv()
            for copy in w_copies:
                copy.wait()
            return
        if k == 1:
            take_unit(0)
            take_unit(1)
        elif k < n - 2:
            take_unit(k)
        elif k == n - 1:
            take_unit(n_unit - 1)
            wait_sum(-(half - 1))
            rs_step(1, 0)
            wait_sum(half - 1)
            rs_step(0, 0)
            wait_pair(0, n_unit - 1)
            wait_pair(1, n_unit - 1)
            return
        direction = 0 if order[k] < 0 else 1
        s = abs(order[k]) - 1
        wait_pair(direction, 2 * s)
        wait_pair(direction, 2 * s + 1)

    def compute(i):
        x = xbuf[i].reshape(2 * rows, d)
        for e in range(n_local):
            for c in range(2):
                row = gbuf[i, c, pl.ds(n_local * me + e, 1), :]
                gcol[e, c * rows:(c + 1) * rows, :] = jnp.transpose(jnp.broadcast_to(row, (rows, rows)))
        ft = 256
        for e in range(n_local):
            for nt in range(wg.shape[2] // ft):
                cols = slice(nt * ft, (nt + 1) * ft)
                g = jnp.dot(x, wg[e, :, cols], preferred_element_type=F32)
                u = jnp.dot(x, wu[e, :, cols], preferred_element_type=F32)
                act[:, cols] = (jax.nn.silu(g) * u).astype(BF16)
            a = act[...]
            gc = gcol[e]
            chosen = gc >= 0.0
            for nt in range(d // ft):
                f = jnp.dot(a, wd[e, :, nt * ft:(nt + 1) * ft], preferred_element_type=F32).astype(BF16).astype(F32)
                for l in range(ft // rows):
                    cols = slice(nt * ft + l * rows, nt * ft + (l + 1) * rows)
                    term = jnp.where(chosen, f[:, l * rows:(l + 1) * rows] * gc, 0.0).reshape(2, rows, rows)
                    cboth[i, :, :, cols] = term if e == 0 else cboth[i, :, :, cols] + term

    def body(k, carry):
        for kk in range(n):
            @pl.when(k == kk)
            def _(kk=kk):
                before(kk)
        s = (k + 1) // 2
        step = jnp.where((lax.rem(k, 2) == 1) & (k < n - 1), -s, s)
        i = at_chip(step)
        compute(i)
        sum_copy(k, i).start()
        return carry

    lax.fori_loop(0, n, body, 0)

    waited = {half - 1, -(half - 1)}
    n_rs = len(rs_lists[0])
    for u in range(1, n_rs):
        for direction in range(2):
            q = rs_lists[direction][u][0]
            step = q if direction == 0 else -q
            if step == -half:
                step = half
            if step not in waited:
                wait_sum(step)
                waited.add(step)
            rs_step(direction, u)
    wait_sum(0)
    for h in range(2):
        for p in range(2):
            at = pl.ds(h * hr + p * qr, qr)
            total = y_ref[at, :] + (cboth[chip, core, at, :] + cpart[chip, at, :])
            for direction in range(2):
                rs_copy(direction, rs_lists[direction].index((1, h, p))).wait_recv()
                total = total + inc[direction, 0, at, :]
            out_ref[at, :] = total.astype(out_ref.dtype)

    for direction in range(2):
        for u in range(n_unit):
            i = send_chip(direction, u)
            ring_copy(direction, u, i).wait_send()
            j = unit_from(direction, u)
            pair_copy(direction, u, j, core).wait_send()
            if has_gate(direction, u):
                ring_gate(direction, u, i).wait_send()
                pair_gate(direction, u, j, core).wait_send()
        for u in range(n_rs):
            rs_copy(direction, u).wait_send()
    for copy in self_copies(core):
        copy.wait_send()
    for k in range(n):
        sum_copy(k, at_chip(order[k])).wait_send()


def moe(n_ep, r, gates, y, w_gate, w_up, w_down):
    n = n_ep // 2
    rows, d = r.shape
    n_exp = gates.shape[0]
    n_local, _, ff = w_gate.shape
    vm = pl.BlockSpec(memory_space=pltpu.VMEM)
    anyspace = pl.BlockSpec(memory_space=pl.ANY)
    dma = pltpu.SemaphoreType.DMA
    n_rs = 2 * (n - 1)
    return pl.pallas_call(
        functools.partial(moe_kernel, n),
        out_shape=jax.ShapeDtypeStruct((rows, d), BF16),
        in_specs=[vm] * 3 + [anyspace] * 3,
        out_specs=vm,
        scratch_shapes=[
            pltpu.VMEM((n, 2, rows, d), BF16),
            pltpu.VMEM((n, 2, n_exp, rows), F32),
            pltpu.VMEM((n, 2, rows, d), F32),
            pltpu.VMEM((n, rows, d), F32),
            pltpu.VMEM((2, n // 2, rows, d), F32),
            pltpu.VMEM(w_gate.shape, BF16), pltpu.VMEM(w_up.shape, BF16), pltpu.VMEM(w_down.shape, BF16),
            pltpu.VMEM((2 * rows, ff), BF16),
            pltpu.VMEM((n_local, 2 * rows, rows), F32),
            dma((3,)), dma((2,)),
            dma((2, n - 1)), dma((2, n - 1)), dma((2, n // 2)), dma((2, n // 2)),
            dma((2, n - 1)), dma((2, n - 1)), dma((2, n // 2)), dma((2, n // 2)),
            dma((2,)), dma((2,)),
            dma((n,)), dma((n,)),
            dma((2, n_rs)), dma((2, n_rs)),
        ],
        compiler_params=pltpu.CompilerParams(collective_id=0, has_side_effects=True, vmem_limit_bytes=40 * 1024 * 1024),
        name="moe",
    )(r, gates, y, w_gate, w_up, w_down)


def solution(mesh):
    n_ep = mesh.shape['ep']
    row_spec = P(('dp', 'ep'), None)
    cache_spec = P(('dp', 'ep'), None, None, None)
    len_spec = P(('dp', 'ep'))
    rep_vec = P(None)
    rep_mat = P(None, None)
    exp_spec = P('ep', None, None)

    def local_step(hidden, k_cache, v_cache, seq_lens, expert_ids, ln_attn, w_q, w_k, w_v, q_gain, k_gain, w_o, ln_moe, w_router, w_gate, w_up, w_down):
        k_t = jnp.transpose(k_cache, (1, 2, 3, 0))
        v_t = jnp.transpose(v_cache, (1, 2, 3, 0))
        k_new, v_new, y, r, gates = attend(
            hidden, k_t, v_t, seq_lens[None, :], expert_ids.T, ln_attn[None, :], w_q, w_k, w_v,
            q_gain[None, :], k_gain[None, :], w_o, ln_moe[None, :], w_router.T)
        out = moe(n_ep, r, gates, y, w_gate, w_up, w_down)
        return out, jnp.transpose(k_new, (3, 0, 1, 2)), jnp.transpose(v_new, (3, 0, 1, 2))

    return jax.shard_map(local_step, mesh=mesh, in_specs=(row_spec, cache_spec, cache_spec, len_spec, row_spec, rep_vec, rep_mat, rep_mat, rep_mat, rep_vec, rep_vec, rep_mat, rep_vec, rep_mat, exp_spec, exp_spec, exp_spec), out_specs=(row_spec, cache_spec, cache_spec), check_vma=False)
```

```python
import functools

import jax
import jax.numpy as jnp
import numpy as np
from jax import lax
from jax.experimental import pallas as pl
from jax.experimental.pallas import tpu as pltpu
from jax.sharding import PartitionSpec as P

EPS = 1e-6
ROPE_BASE = 1000000.0
F32 = jnp.float32
BF16 = jnp.bfloat16
MESH = pl.DeviceIdType.MESH


def in_hbm(*arrays):
    return [pltpu.with_memory_space_constraint(a, pltpu.HBM) for a in arrays]


def attend_kernel(h_hbm, lens_hbm, ids_hbm, ln_a_hbm, qg_hbm, kg_hbm, ln_m_hbm, wr_hbm,
                  wq_hbm, wk_hbm, wv_hbm, wo_hbm, kc_hbm, vc_hbm,
                  kn_hbm, vn_hbm, y_ref, r_ref, gate_ref,
                  h_ref, lens_ref, ids_ref, ln_a_ref, qg_ref, kg_ref, ln_m_ref, wr_ref,
                  kbuf, vbuf, wq, wk, wv, wo, qrot, knew, vnew, score, attn, small_sem, in_sem, out_sem):
    t_max, n_kv, hd, n_seq = kc_hbm.shape
    n_heads = wq_hbm.shape[1] // hd
    grp = n_heads // n_kv
    half = hd // 2
    n_chunk = 4
    tc = t_max // n_chunk

    w_copies = [pltpu.make_async_copy(src, dst, in_sem.at[i])
                for i, (src, dst) in enumerate(((wk_hbm, wk), (wq_hbm, wq), (wv_hbm, wv), (wo_hbm, wo)))]
    k_in = [pltpu.make_async_copy(kc_hbm.at[pl.ds(c * tc, tc)], kbuf.at[pl.ds(c * tc, tc)], in_sem.at[4 + c]) for c in range(n_chunk)]
    v_in = [pltpu.make_async_copy(vc_hbm.at[pl.ds(c * tc, tc)], vbuf.at[pl.ds(c * tc, tc)], in_sem.at[4 + n_chunk + c]) for c in range(n_chunk)]
    k_out = [pltpu.make_async_copy(kbuf.at[pl.ds(c * tc, tc)], kn_hbm.at[pl.ds(c * tc, tc)], out_sem.at[c]) for c in range(n_chunk)]
    v_out = [pltpu.make_async_copy(vbuf.at[pl.ds(c * tc, tc)], vn_hbm.at[pl.ds(c * tc, tc)], out_sem.at[n_chunk + c]) for c in range(n_chunk)]
    small = [pltpu.make_async_copy(src, dst, small_sem.at[i]) for i, (src, dst) in enumerate((
        (h_hbm, h_ref), (lens_hbm, lens_ref), (ids_hbm, ids_ref), (ln_a_hbm, ln_a_ref), (qg_hbm, qg_ref), (kg_hbm, kg_ref), (ln_m_hbm, ln_m_ref), (wr_hbm, wr_ref)))]
    for copy in small + w_copies[:3] + k_in + v_in + w_copies[3:]:
        copy.start()
    for copy in small:
        copy.wait()

    def vector(ref):
        rows = ref[...].astype(F32)
        return jnp.concatenate([rows[i:i + 1, :] for i in range(rows.shape[0])], axis=1)

    h32 = h_ref[...].astype(F32)
    mean_sq = jnp.mean(h32 * h32, axis=1, keepdims=True)
    x = (h32 * lax.rsqrt(mean_sq + EPS) * vector(ln_a_ref)).astype(BF16)

    lens = lens_ref[...]
    f_iota = lax.broadcasted_iota(jnp.int32, (half, n_seq), 0)
    inv_freq = np.power(np.float32(ROPE_BASE), -np.arange(0, hd, 2).astype(np.float32) / np.float32(hd))
    freq = jnp.zeros((half, n_seq), F32)
    for i in range(half):
        freq = jnp.where(f_iota == i, float(inv_freq[i]), freq)
    angles = lens.astype(F32) * freq
    cos_v = jnp.cos(angles)
    sin_v = jnp.sin(angles)

    def gain_tile(g_ref):
        row = g_ref[...].astype(F32)
        row = jnp.concatenate([row] * (n_seq // hd), axis=1)
        return jnp.transpose(jnp.broadcast_to(row, (n_seq, n_seq)))[:hd, :]

    def rope_heads(proj, gain, dst, heads):
        for i in range(heads):
            if i % 2 == 0:
                pair = jnp.transpose(proj[:, i * hd:(i + 2) * hd])
            vals = pair[(i % 2) * hd:(i % 2 + 1) * hd, :]
            ms = jnp.mean(vals * vals, axis=0, keepdims=True)
            vals = vals * lax.rsqrt(ms + EPS) * gain
            low, high = vals[:half, :], vals[half:, :]
            dst[i * hd:i * hd + half, :] = (low * cos_v - high * sin_v).astype(BF16).astype(F32)
            dst[i * hd + half:(i + 1) * hd, :] = (high * cos_v + low * sin_v).astype(BF16).astype(F32)

    w_copies[0].wait()
    rope_heads(jnp.dot(x, wk[...], preferred_element_type=F32), gain_tile(kg_ref), knew, n_kv)
    w_copies[1].wait()
    rope_heads(jnp.dot(x, wq[...], preferred_element_type=F32), gain_tile(qg_ref), qrot, n_heads)
    w_copies[2].wait()
    v_proj = jnp.dot(x, wv[...], preferred_element_type=F32)
    for i in range(0, n_kv, 2):
        vnew[i * hd:(i + 2) * hd, :] = jnp.transpose(v_proj[:, i * hd:(i + 2) * hd]).astype(BF16).astype(F32)

    for c in range(n_chunk):
        k_in[c].wait()

        def k_body(kv, carry, c=c):
            new = knew[pl.ds(pl.multiple_of(kv * hd, hd), hd), :]
            qs = [qrot[pl.ds(pl.multiple_of((kv * grp + g) * hd, hd), hd), :] for g in range(grp)]
            rows = [[] for _ in range(grp)]
            for tt in range(tc):
                t = c * tc + tt
                kt = jnp.where(lens == t, new, kbuf[t, kv].astype(F32))
                kbuf[t, kv] = kt.astype(BF16)
                for g in range(grp):
                    rows[g].append(jnp.sum(kt * qs[g], axis=0, keepdims=True))
            for g in range(grp):
                score[kv * grp + g, c * tc:(c + 1) * tc, :] = jnp.concatenate(rows[g], axis=0)
            return carry

        lax.fori_loop(0, n_kv, k_body, 0)
        k_out[c].start()

    visible = lax.broadcasted_iota(jnp.int32, (t_max, n_seq), 0) <= lens

    def soft_body(j, carry):
        s = jnp.where(visible, score[j] * (hd ** -0.5), -1e30)
        e = jnp.exp(s - jnp.max(s, axis=0, keepdims=True))
        score[j] = (e / jnp.sum(e, axis=0, keepdims=True)).astype(BF16).astype(F32)
        return carry

    lax.fori_loop(0, n_heads, soft_body, 0, unroll=2)

    for c in range(n_chunk):
        v_in[c].wait()

        def v_body(kv, carry, c=c):
            new = vnew[pl.ds(pl.multiple_of(kv * hd, hd), hd), :]
            at = [pl.ds(pl.multiple_of((kv * grp + g) * hd, hd), hd) for g in range(grp)]
            acc = [None if c == 0 else attn[at[g], :] for g in range(grp)]
            for tt in range(tc):
                t = c * tc + tt
                vt = jnp.where(lens == t, new, vbuf[t, kv].astype(F32))
                vbuf[t, kv] = vt.astype(BF16)
                for g in range(grp):
                    term = vt * score[kv * grp + g, t:t + 1, :]
                    acc[g] = term if acc[g] is None else acc[g] + term
            for g in range(grp):
                attn[at[g], :] = acc[g]
            return carry

        lax.fori_loop(0, n_kv, v_body, 0)
        v_out[c].start()

    w_copies[3].wait()
    a_rows = jnp.concatenate([jnp.transpose(attn[i * n_seq:(i + 1) * n_seq, :]).astype(BF16) for i in range(n_heads * hd // n_seq)], axis=1)
    y = h32 + jnp.dot(a_rows, wo[...], preferred_element_type=F32)
    y_ref[...] = y
    mean_sq = jnp.mean(y * y, axis=1, keepdims=True)
    r = (y * lax.rsqrt(mean_sq + EPS) * vector(ln_m_ref)).astype(BF16)
    r_ref[...] = r
    logits = lax.dot_general(wr_ref[...], r, (((1,), (1,)), ((), ())), preferred_element_type=F32)
    e_iota = lax.broadcasted_iota(jnp.int32, logits.shape, 0)
    ids = ids_ref[...]
    chosen = e_iota == ids[0:1, :]
    for i in range(1, ids.shape[0]):
        chosen = chosen | (e_iota == ids[i:i + 1, :])
    top = jnp.max(jnp.where(chosen, logits, -jnp.inf), axis=0, keepdims=True)
    e = jnp.where(chosen, jnp.exp(logits - top), 0.0)
    gate_ref[...] = jnp.where(chosen, e / jnp.sum(e, axis=0, keepdims=True), -1.0)

    for copy in k_out + v_out:
        copy.wait()


def attend(hidden, k_t, v_t, lens, ids_t, ln_attn, w_q, w_k, w_v, q_gain, k_gain, w_o, ln_moe, w_router_t):
    n_seq, d = hidden.shape
    t_max, n_kv, hd, _ = k_t.shape
    hq, hk = w_q.shape[1], w_k.shape[1]
    n_heads = hq // hd
    n_exp = w_router_t.shape[0]
    vm = pl.BlockSpec(memory_space=pltpu.VMEM)
    hbm = pl.BlockSpec(memory_space=pltpu.HBM)
    small = (hidden, lens, ids_t, ln_attn, q_gain, k_gain, ln_moe, w_router_t)
    return pl.pallas_call(
        attend_kernel,
        out_shape=(
            jax.ShapeDtypeStruct(k_t.shape, k_t.dtype),
            jax.ShapeDtypeStruct(v_t.shape, v_t.dtype),
            jax.ShapeDtypeStruct((n_seq, d), F32),
            jax.ShapeDtypeStruct((n_seq, d), BF16),
            jax.ShapeDtypeStruct((n_exp, n_seq), F32),
        ),
        in_specs=[hbm] * 14,
        out_specs=(hbm, hbm, vm, vm, vm),
        scratch_shapes=[pltpu.VMEM(a.shape, a.dtype) for a in small] + [
            pltpu.VMEM(k_t.shape, BF16), pltpu.VMEM(v_t.shape, BF16),
            pltpu.VMEM(w_q.shape, BF16), pltpu.VMEM(w_k.shape, BF16), pltpu.VMEM(w_v.shape, BF16), pltpu.VMEM(w_o.shape, BF16),
            pltpu.VMEM((hq, n_seq), F32), pltpu.VMEM((hk, n_seq), F32), pltpu.VMEM((hk, n_seq), F32),
            pltpu.VMEM((n_heads, t_max, n_seq), F32), pltpu.VMEM((hq, n_seq), F32),
            pltpu.SemaphoreType.DMA((len(small),)), pltpu.SemaphoreType.DMA((12,)), pltpu.SemaphoreType.DMA((8,)),
        ],
        compiler_params=pltpu.CompilerParams(vmem_limit_bytes=30 * 1024 * 1024),
        name="attend",
    )(*in_hbm(*small, w_q, w_k, w_v, w_o, k_t, v_t))


def moe_kernel(n, r_ref, gate_ref, y_ref, wg_hbm, wu_hbm, wd_hbm, out_ref,
               xbuf, gbuf, cboth, cpart, inc, wg, wu, wd, act, gcol,
               w_sem, own_sem, ring_send, ring_recv, gate_send, gate_recv,
               pair_send, pair_recv, pgate_send, pgate_recv, self_send, self_recv,
               sum_send, sum_recv, rs_send, rs_recv):
    me = lax.axis_index("ep")
    chip = me // 2
    core = lax.rem(me, 2)
    other = 1 - core
    half = n // 2
    n_unit = n - 1
    rows, d = r_ref.shape
    n_local = wg_hbm.shape[0]
    hr = rows // 2
    qr = hr // 2

    def at_chip(step):
        return lax.rem(chip + step + n, n)

    def ring_dev(direction):
        return {"ep": 2 * at_chip(1 if direction == 0 else -1) + core}

    pair_dev = {"ep": 2 * chip + other}

    def remote(src, dst, ssem, rsem, dev):
        return pltpu.make_async_remote_copy(src_ref=src, dst_ref=dst, send_sem=ssem, recv_sem=rsem, device_id=dev, device_id_type=MESH)

    barrier = pltpu.get_barrier_semaphore()
    for dev in (ring_dev(0), ring_dev(1), pair_dev):
        pl.semaphore_signal(barrier, inc=1, device_id=dev, device_id_type=MESH)

    w_copies = [pltpu.make_async_copy(src, dst, w_sem.at[i]) for i, (src, dst) in enumerate(((wg_hbm, wg), (wu_hbm, wu), (wd_hbm, wd)))]
    own_copies = [pltpu.make_async_copy(r_ref, xbuf.at[chip, core], own_sem.at[0]),
                  pltpu.make_async_copy(gate_ref, gbuf.at[chip, core], own_sem.at[1])]
    for copy in own_copies + w_copies:
        copy.start()
    for copy in own_copies:
        copy.wait()
    pl.semaphore_wait(barrier, 3)

    def unit_half(direction, u):
        return u % 2 if direction == 0 else 1 - u % 2

    def unit_from(direction, u):
        s = u // 2 + 1
        return at_chip(-s if direction == 0 else s)

    def has_gate(direction, u):
        return u % 2 == 0 and (direction == 0 or u < n_unit - 1)

    def x_at(i, c, direction, u):
        return xbuf.at[i, c, pl.ds(unit_half(direction, u) * hr, hr)]

    def ring_copy(direction, u, i):
        ref = x_at(i, core, direction, u)
        return remote(ref, ref, ring_send.at[direction, u], ring_recv.at[direction, u], ring_dev(direction))

    def ring_gate(direction, u, i):
        ref = gbuf.at[i, core]
        return remote(ref, ref, gate_send.at[direction, u // 2], gate_recv.at[direction, u // 2], ring_dev(direction))

    def pair_copy(direction, u, i, c):
        ref = x_at(i, c, direction, u)
        return remote(ref, ref, pair_send.at[direction, u], pair_recv.at[direction, u], pair_dev)

    def pair_gate(direction, u, i, c):
        ref = gbuf.at[i, c]
        return remote(ref, ref, pgate_send.at[direction, u // 2], pgate_recv.at[direction, u // 2], pair_dev)

    def self_copies(c):
        return [remote(xbuf.at[chip, c], xbuf.at[chip, c], self_send.at[0], self_recv.at[0], pair_dev),
                remote(gbuf.at[chip, c], gbuf.at[chip, c], self_send.at[1], self_recv.at[1], pair_dev)]

    def send_chip(direction, u):
        s = u // 2
        return at_chip(-s if direction == 0 else s)

    def start_unit(direction, u):
        i = send_chip(direction, u)
        if has_gate(direction, u):
            ring_gate(direction, u, i).start()
        ring_copy(direction, u, i).start()

    for u in range(2):
        for direction in range(2):
            start_unit(direction, u)
        if u == 0:
            for copy in self_copies(core):
                copy.start()

    def take_unit(u):
        for direction in range(2):
            i = unit_from(direction, u)
            if has_gate(direction, u):
                ring_gate(direction, u, i).wait_recv()
            ring_copy(direction, u, i).wait_recv()
            if u + 2 < n_unit:
                start_unit(direction, u + 2)
            if has_gate(direction, u):
                pair_gate(direction, u, i, core).start()
            pair_copy(direction, u, i, core).start()

    def wait_pair(direction, u):
        i = unit_from(direction, u)
        if has_gate(direction, u):
            pair_gate(direction, u, i, other).wait_recv()
        pair_copy(direction, u, i, other).wait_recv()

    def sum_copy(k, i):
        return remote(cboth.at[i, other], cpart.at[i], sum_send.at[k], sum_recv.at[k], pair_dev)

    def order_step(k):
        return 0 if k == 0 else (-((k + 1) // 2) if k % 2 == 1 and k < n - 1 else (k + 1) // 2)

    order = [order_step(k) for k in range(n)]

    def rs_list(direction):
        lh, sh = (0, 1) if direction == 0 else (1, 0)
        seq = [(half - 1, sh, 0), (half, lh, 0), (half, lh, 1), (half - 1, sh, 1)]
        for q in range(half - 1, 0, -1):
            seq += [(q, lh, 0), (q, lh, 1)]
            if q > 1:
                seq += [(q - 1, sh, 0), (q - 1, sh, 1)]
        return seq

    rs_lists = [rs_list(0), rs_list(1)]

    def rs_copy(direction, u):
        q, h, p = rs_lists[direction][u]
        t = at_chip(q if direction == 0 else -q)
        at = pl.ds(h * hr + p * qr, qr)
        return remote(cboth.at[t, core, at], inc.at[direction, q - 1, at], rs_send.at[direction, u], rs_recv.at[direction, u], ring_dev(direction))

    def rs_step(direction, u):
        q, h, p = rs_lists[direction][u]
        step = q if direction == 0 else -q
        t = at_chip(step)
        at = pl.ds(h * hr + p * qr, qr)
        total = cboth[t, core, at, :] + cpart[t, at, :]
        if (q + 1, h, p) in rs_lists[direction]:
            rs_copy(direction, rs_lists[direction].index((q + 1, h, p))).wait_recv()
            total = total + inc[direction, q, at, :]
        cboth[t, core, at, :] = total
        rs_copy(direction, u).start()

    def wait_sum(step):
        step = step if step in order else step + n if step + n in order else step - n
        k = order.index(step)
        sum_copy(k, at_chip(step)).wait_recv()

    def before(k):
        if k == 0:
            for copy in self_copies(other):
                copy.wait_recv()
            for copy in w_copies:
                copy.wait()
            return
        if k == 1:
            take_unit(0)
            take_unit(1)
        elif k < n - 2:
            take_unit(k)
        elif k == n - 1:
            take_unit(n_unit - 1)
            wait_sum(-(half - 1))
            rs_step(1, 0)
            wait_sum(half - 1)
            rs_step(0, 0)
            wait_pair(0, n_unit - 1)
            wait_pair(1, n_unit - 1)
            return
        direction = 0 if order[k] < 0 else 1
        s = abs(order[k]) - 1
        wait_pair(direction, 2 * s)
        wait_pair(direction, 2 * s + 1)

    def compute(i):
        x = xbuf[i].reshape(2 * rows, d)
        for e in range(n_local):
            for c in range(2):
                row = gbuf[i, c, pl.ds(n_local * me + e, 1), :]
                gcol[e, c * rows:(c + 1) * rows, :] = jnp.transpose(jnp.broadcast_to(row, (rows, rows)))
        ft = 256
        for e in range(n_local):
            for nt in range(wg.shape[2] // ft):
                cols = slice(nt * ft, (nt + 1) * ft)
                g = jnp.dot(x, wg[e, :, cols], preferred_element_type=F32)
                u = jnp.dot(x, wu[e, :, cols], preferred_element_type=F32)
                act[:, cols] = (jax.nn.silu(g) * u).astype(BF16)
            a = act[...]
            gc = gcol[e]
            chosen = gc >= 0.0
            for nt in range(d // ft):
                f = jnp.dot(a, wd[e, :, nt * ft:(nt + 1) * ft], preferred_element_type=F32).astype(BF16).astype(F32)
                for l in range(ft // rows):
                    cols = slice(nt * ft + l * rows, nt * ft + (l + 1) * rows)
                    term = jnp.where(chosen, f[:, l * rows:(l + 1) * rows] * gc, 0.0).reshape(2, rows, rows)
                    cboth[i, :, :, cols] = term if e == 0 else cboth[i, :, :, cols] + term

    def body(k, carry):
        for kk in range(n):
            @pl.when(k == kk)
            def _(kk=kk):
                before(kk)
        s = (k + 1) // 2
        step = jnp.where((lax.rem(k, 2) == 1) & (k < n - 1), -s, s)
        i = at_chip(step)
        compute(i)
        sum_copy(k, i).start()
        return carry

    lax.fori_loop(0, n, body, 0)

    waited = {half - 1, -(half - 1)}
    n_rs = len(rs_lists[0])
    for u in range(1, n_rs):
        for direction in range(2):
            q = rs_lists[direction][u][0]
            step = q if direction == 0 else -q
            if step == -half:
                step = half
            if step not in waited:
                wait_sum(step)
                waited.add(step)
            rs_step(direction, u)
    wait_sum(0)
    for h in range(2):
        for p in range(2):
            at = pl.ds(h * hr + p * qr, qr)
            total = y_ref[at, :] + (cboth[chip, core, at, :] + cpart[chip, at, :])
            for direction in range(2):
                rs_copy(direction, rs_lists[direction].index((1, h, p))).wait_recv()
                total = total + inc[direction, 0, at, :]
            out_ref[at, :] = total.astype(out_ref.dtype)

    for direction in range(2):
        for u in range(n_unit):
            i = send_chip(direction, u)
            ring_copy(direction, u, i).wait_send()
            j = unit_from(direction, u)
            pair_copy(direction, u, j, core).wait_send()
            if has_gate(direction, u):
                ring_gate(direction, u, i).wait_send()
                pair_gate(direction, u, j, core).wait_send()
        for u in range(n_rs):
            rs_copy(direction, u).wait_send()
    for copy in self_copies(core):
        copy.wait_send()
    for k in range(n):
        sum_copy(k, at_chip(order[k])).wait_send()


def moe(n_ep, r, gates, y, w_gate, w_up, w_down):
    n = n_ep // 2
    rows, d = r.shape
    n_exp = gates.shape[0]
    n_local, _, ff = w_gate.shape
    vm = pl.BlockSpec(memory_space=pltpu.VMEM)
    hbm = pl.BlockSpec(memory_space=pltpu.HBM)
    dma = pltpu.SemaphoreType.DMA
    n_rs = 2 * (n - 1)
    return pl.pallas_call(
        functools.partial(moe_kernel, n),
        out_shape=jax.ShapeDtypeStruct((rows, d), BF16),
        in_specs=[vm] * 3 + [hbm] * 3,
        out_specs=vm,
        scratch_shapes=[
            pltpu.VMEM((n, 2, rows, d), BF16),
            pltpu.VMEM((n, 2, n_exp, rows), F32),
            pltpu.VMEM((n, 2, rows, d), F32),
            pltpu.VMEM((n, rows, d), F32),
            pltpu.VMEM((2, n // 2, rows, d), F32),
            pltpu.VMEM(w_gate.shape, BF16), pltpu.VMEM(w_up.shape, BF16), pltpu.VMEM(w_down.shape, BF16),
            pltpu.VMEM((2 * rows, ff), BF16),
            pltpu.VMEM((n_local, 2 * rows, rows), F32),
            dma((3,)), dma((2,)),
            dma((2, n - 1)), dma((2, n - 1)), dma((2, n // 2)), dma((2, n // 2)),
            dma((2, n - 1)), dma((2, n - 1)), dma((2, n // 2)), dma((2, n // 2)),
            dma((2,)), dma((2,)),
            dma((n,)), dma((n,)),
            dma((2, n_rs)), dma((2, n_rs)),
        ],
        compiler_params=pltpu.CompilerParams(collective_id=0, has_side_effects=True, vmem_limit_bytes=40 * 1024 * 1024),
        name="moe",
    )(r, gates, y, *in_hbm(w_gate, w_up, w_down))


def solution(mesh):
    n_ep = mesh.shape['ep']
    row_spec = P(('dp', 'ep'), None)
    cache_spec = P(('dp', 'ep'), None, None, None)
    len_spec = P(('dp', 'ep'))
    rep_vec = P(None)
    rep_mat = P(None, None)
    exp_spec = P('ep', None, None)

    def local_step(hidden, k_cache, v_cache, seq_lens, expert_ids, ln_attn, w_q, w_k, w_v, q_gain, k_gain, w_o, ln_moe, w_router, w_gate, w_up, w_down):
        k_t = jnp.transpose(k_cache, (1, 2, 3, 0))
        v_t = jnp.transpose(v_cache, (1, 2, 3, 0))
        k_new, v_new, y, r, gates = attend(
            hidden, k_t, v_t, seq_lens[None, :], expert_ids.T, ln_attn.reshape(-1, 128), w_q, w_k, w_v,
            q_gain[None, :], k_gain[None, :], w_o, ln_moe.reshape(-1, 128), w_router.T)
        out = moe(n_ep, r, gates, y, w_gate, w_up, w_down)
        return out, jnp.transpose(k_new, (3, 0, 1, 2)), jnp.transpose(v_new, (3, 0, 1, 2))

    return jax.shard_map(local_step, mesh=mesh, in_specs=(row_spec, cache_spec, cache_spec, len_spec, row_spec, rep_vec, rep_mat, rep_mat, rep_mat, rep_vec, rep_vec, rep_mat, rep_vec, rep_mat, exp_spec, exp_spec, exp_spec), out_specs=(row_spec, cache_spec, cache_spec), check_vma=False)
```

```python
import functools

import jax
import jax.numpy as jnp
import numpy as np
from jax import lax
from jax.experimental import pallas as pl
from jax.experimental.pallas import tpu as pltpu
from jax.sharding import PartitionSpec as P

EPS = 1e-6
ROPE_BASE = 1000000.0
F32 = jnp.float32
BF16 = jnp.bfloat16
MESH = pl.DeviceIdType.MESH


def in_hbm(*arrays):
    return [pltpu.with_memory_space_constraint(a, pltpu.HBM) for a in arrays]


def attend_kernel(h_hbm, lens_hbm, ids_hbm, ln_a_hbm, qg_hbm, kg_hbm, ln_m_hbm, wr_hbm,
                  wq_hbm, wk_hbm, wv_hbm, wo_hbm, kc_hbm, vc_hbm,
                  kn_hbm, vn_hbm, y_ref, r_ref, gate_ref,
                  h_ref, lens_ref, ids_ref, ln_a_ref, qg_ref, kg_ref, ln_m_ref, wr_ref,
                  kbuf, vbuf, wq, wk, wv, wo, qrot, knew, vnew, score, attn, small_sem, in_sem, out_sem):
    t_max, n_kv, hd, n_seq = kc_hbm.shape
    n_heads = wq_hbm.shape[1] // hd
    grp = n_heads // n_kv
    half = hd // 2
    n_chunk = 4
    tc = t_max // n_chunk

    w_copies = [pltpu.make_async_copy(src, dst, in_sem.at[i])
                for i, (src, dst) in enumerate(((wk_hbm, wk), (wq_hbm, wq), (wv_hbm, wv), (wo_hbm, wo)))]
    k_in = [pltpu.make_async_copy(kc_hbm.at[pl.ds(c * tc, tc)], kbuf.at[pl.ds(c * tc, tc)], in_sem.at[4 + c]) for c in range(n_chunk)]
    v_in = [pltpu.make_async_copy(vc_hbm.at[pl.ds(c * tc, tc)], vbuf.at[pl.ds(c * tc, tc)], in_sem.at[4 + n_chunk + c]) for c in range(n_chunk)]
    k_out = [pltpu.make_async_copy(kbuf.at[pl.ds(c * tc, tc)], kn_hbm.at[pl.ds(c * tc, tc)], out_sem.at[c]) for c in range(n_chunk)]
    v_out = [pltpu.make_async_copy(vbuf.at[pl.ds(c * tc, tc)], vn_hbm.at[pl.ds(c * tc, tc)], out_sem.at[n_chunk + c]) for c in range(n_chunk)]
    small = [pltpu.make_async_copy(src, dst, small_sem.at[i]) for i, (src, dst) in enumerate((
        (h_hbm, h_ref), (lens_hbm, lens_ref), (ids_hbm, ids_ref), (ln_a_hbm, ln_a_ref), (qg_hbm, qg_ref), (kg_hbm, kg_ref), (ln_m_hbm, ln_m_ref), (wr_hbm, wr_ref)))]
    for copy in small + w_copies[:3]:
        copy.start()
    for copy in small:
        copy.wait()
    k_in[0].start()

    def vector(ref):
        rows = ref[...].astype(F32)
        return jnp.concatenate([rows[i:i + 1, :] for i in range(rows.shape[0])], axis=1)

    h32 = h_ref[...].astype(F32)
    mean_sq = jnp.mean(h32 * h32, axis=1, keepdims=True)
    x = (h32 * lax.rsqrt(mean_sq + EPS) * vector(ln_a_ref)).astype(BF16)

    lens = lens_ref[...]
    f_iota = lax.broadcasted_iota(jnp.int32, (half, n_seq), 0)
    inv_freq = np.power(np.float32(ROPE_BASE), -np.arange(0, hd, 2).astype(np.float32) / np.float32(hd))
    freq = jnp.zeros((half, n_seq), F32)
    for i in range(half):
        freq = jnp.where(f_iota == i, float(inv_freq[i]), freq)
    angles = lens.astype(F32) * freq
    cos_v = jnp.cos(angles)
    sin_v = jnp.sin(angles)

    def gain_tile(g_ref):
        row = g_ref[...].astype(F32)
        row = jnp.concatenate([row] * (n_seq // hd), axis=1)
        return jnp.transpose(jnp.broadcast_to(row, (n_seq, n_seq)))[:hd, :]

    def rope_heads(proj, gain, dst, heads):
        for i in range(heads):
            if i % 2 == 0:
                pair = jnp.transpose(proj[:, i * hd:(i + 2) * hd])
            vals = pair[(i % 2) * hd:(i % 2 + 1) * hd, :]
            ms = jnp.mean(vals * vals, axis=0, keepdims=True)
            vals = vals * lax.rsqrt(ms + EPS) * gain
            low, high = vals[:half, :], vals[half:, :]
            dst[i * hd:i * hd + half, :] = (low * cos_v - high * sin_v).astype(BF16).astype(F32)
            dst[i * hd + half:(i + 1) * hd, :] = (high * cos_v + low * sin_v).astype(BF16).astype(F32)

    w_copies[0].wait()
    for copy in k_in[1:]:
        copy.start()
    rope_heads(jnp.dot(x, wk[...], preferred_element_type=F32), gain_tile(kg_ref), knew, n_kv)
    w_copies[1].wait()
    for copy in v_in + w_copies[3:]:
        copy.start()
    rope_heads(jnp.dot(x, wq[...], preferred_element_type=F32), gain_tile(qg_ref), qrot, n_heads)
    w_copies[2].wait()
    v_proj = jnp.dot(x, wv[...], preferred_element_type=F32)
    for i in range(0, n_kv, 2):
        vnew[i * hd:(i + 2) * hd, :] = jnp.transpose(v_proj[:, i * hd:(i + 2) * hd]).astype(BF16).astype(F32)

    for c in range(n_chunk):
        k_in[c].wait()

        def k_body(kv, carry, c=c):
            new = knew[pl.ds(pl.multiple_of(kv * hd, hd), hd), :]
            qs = [qrot[pl.ds(pl.multiple_of((kv * grp + g) * hd, hd), hd), :] for g in range(grp)]
            rows = [[] for _ in range(grp)]
            for tt in range(tc):
                t = c * tc + tt
                kt = jnp.where(lens == t, new, kbuf[t, kv].astype(F32))
                kbuf[t, kv] = kt.astype(BF16)
                for g in range(grp):
                    rows[g].append(jnp.sum(kt * qs[g], axis=0, keepdims=True))
            for g in range(grp):
                score[kv * grp + g, c * tc:(c + 1) * tc, :] = jnp.concatenate(rows[g], axis=0)
            return carry

        lax.fori_loop(0, n_kv, k_body, 0)
        k_out[c].start()

    visible = lax.broadcasted_iota(jnp.int32, (t_max, n_seq), 0) <= lens

    def soft_body(j, carry):
        s = jnp.where(visible, score[j] * (hd ** -0.5), -1e30)
        e = jnp.exp(s - jnp.max(s, axis=0, keepdims=True))
        score[j] = (e / jnp.sum(e, axis=0, keepdims=True)).astype(BF16).astype(F32)
        return carry

    lax.fori_loop(0, n_heads, soft_body, 0, unroll=2)

    for c in range(n_chunk):
        v_in[c].wait()

        def v_body(kv, carry, c=c):
            new = vnew[pl.ds(pl.multiple_of(kv * hd, hd), hd), :]
            at = [pl.ds(pl.multiple_of((kv * grp + g) * hd, hd), hd) for g in range(grp)]
            acc = [None if c == 0 else attn[at[g], :] for g in range(grp)]
            for tt in range(tc):
                t = c * tc + tt
                vt = jnp.where(lens == t, new, vbuf[t, kv].astype(F32))
                vbuf[t, kv] = vt.astype(BF16)
                for g in range(grp):
                    term = vt * score[kv * grp + g, t:t + 1, :]
                    acc[g] = term if acc[g] is None else acc[g] + term
            for g in range(grp):
                attn[at[g], :] = acc[g]
            return carry

        lax.fori_loop(0, n_kv, v_body, 0)
        v_out[c].start()

    w_copies[3].wait()
    a_rows = jnp.concatenate([jnp.transpose(attn[i * n_seq:(i + 1) * n_seq, :]).astype(BF16) for i in range(n_heads * hd // n_seq)], axis=1)
    y = h32 + jnp.dot(a_rows, wo[...], preferred_element_type=F32)
    y_ref[...] = y
    mean_sq = jnp.mean(y * y, axis=1, keepdims=True)
    r = (y * lax.rsqrt(mean_sq + EPS) * vector(ln_m_ref)).astype(BF16)
    r_ref[...] = r
    logits = lax.dot_general(wr_ref[...], r, (((1,), (1,)), ((), ())), preferred_element_type=F32)
    e_iota = lax.broadcasted_iota(jnp.int32, logits.shape, 0)
    ids = ids_ref[...]
    chosen = e_iota == ids[0:1, :]
    for i in range(1, ids.shape[0]):
        chosen = chosen | (e_iota == ids[i:i + 1, :])
    top = jnp.max(jnp.where(chosen, logits, -jnp.inf), axis=0, keepdims=True)
    e = jnp.where(chosen, jnp.exp(logits - top), 0.0)
    gates = jnp.where(chosen, e / jnp.sum(e, axis=0, keepdims=True), -1.0)
    g_rows = gates.shape[0] // 2
    turned = pltpu.roll(gates, n_seq // 2, 1)
    low = lax.broadcasted_iota(jnp.int32, (g_rows, n_seq), 1) < n_seq // 2
    gate_ref[0] = jnp.where(low, gates[:g_rows, :], turned[g_rows:, :])
    gate_ref[1] = jnp.where(low, turned[:g_rows, :], gates[g_rows:, :])

    for copy in k_out + v_out:
        copy.wait()


def attend(hidden, k_t, v_t, lens, ids_t, ln_attn, w_q, w_k, w_v, q_gain, k_gain, w_o, ln_moe, w_router_t):
    n_seq, d = hidden.shape
    t_max, n_kv, hd, _ = k_t.shape
    hq, hk = w_q.shape[1], w_k.shape[1]
    n_heads = hq // hd
    n_exp = w_router_t.shape[0]
    vm = pl.BlockSpec(memory_space=pltpu.VMEM)
    hbm = pl.BlockSpec(memory_space=pltpu.HBM)
    small = (hidden, lens, ids_t, ln_attn, q_gain, k_gain, ln_moe, w_router_t)
    return pl.pallas_call(
        attend_kernel,
        out_shape=(
            jax.ShapeDtypeStruct(k_t.shape, k_t.dtype),
            jax.ShapeDtypeStruct(v_t.shape, v_t.dtype),
            jax.ShapeDtypeStruct((n_seq, d), F32),
            jax.ShapeDtypeStruct((n_seq, d), BF16),
            jax.ShapeDtypeStruct((2, n_exp // 2, n_seq), F32),
        ),
        in_specs=[hbm] * 14,
        out_specs=(hbm, hbm, vm, vm, vm),
        scratch_shapes=[pltpu.VMEM(a.shape, a.dtype) for a in small] + [
            pltpu.VMEM(k_t.shape, BF16), pltpu.VMEM(v_t.shape, BF16),
            pltpu.VMEM(w_q.shape, BF16), pltpu.VMEM(w_k.shape, BF16), pltpu.VMEM(w_v.shape, BF16), pltpu.VMEM(w_o.shape, BF16),
            pltpu.VMEM((hq, n_seq), F32), pltpu.VMEM((hk, n_seq), F32), pltpu.VMEM((hk, n_seq), F32),
            pltpu.VMEM((n_heads, t_max, n_seq), F32), pltpu.VMEM((hq, n_seq), F32),
            pltpu.SemaphoreType.DMA((len(small),)), pltpu.SemaphoreType.DMA((12,)), pltpu.SemaphoreType.DMA((8,)),
        ],
        compiler_params=pltpu.CompilerParams(vmem_limit_bytes=30 * 1024 * 1024),
        name="attend",
    )(*in_hbm(*small, w_q, w_k, w_v, w_o, k_t, v_t))


def rs_order(half):
    seq = [(half - 1, 0, 0), (half - 1, 0, 1)]
    for q in range(half, 3, -1):
        seq += [(q - 2, 0, 0), (q, 1, 0), (q, 1, 1), (q - 2, 0, 1)]
    return seq + [(3, 1, 0), (3, 1, 1), (1, 0, 0), (2, 1, 0), (2, 1, 1), (1, 0, 1), (1, 1, 0), (1, 1, 1)]


def moe_kernel(n, r_ref, gate_ref, y_ref, wg_hbm, wu_hbm, wd_hbm, out_ref,
               xbuf, gbuf, cbuf, cpart, inc, wg, wu, wd, act, gcol,
               w_sem, ring_send, ring_recv, gate_send, gate_recv,
               pair_send, pair_recv, pgate_send, pgate_recv,
               sum_send, sum_recv, rs_send, rs_recv):
    me = lax.axis_index("ep")
    chip = me // 2
    core = lax.rem(me, 2)
    other = 1 - core
    half = n // 2
    rows, d = r_ref.shape
    n_local = wg_hbm.shape[0]
    g_rows = gate_ref.shape[1]
    hr = rows // 2
    qr = hr // 2
    ring = [{"ep": 2 * lax.rem(chip + 1, n) + core}, {"ep": 2 * lax.rem(chip + n - 1, n) + core}]
    pair = {"ep": 2 * chip + other}

    def remote(src, dst, ssem, rsem, dev):
        return pltpu.make_async_remote_copy(src_ref=src, dst_ref=dst, send_sem=ssem, recv_sem=rsem, device_id=dev, device_id_type=MESH)

    barrier = pltpu.get_barrier_semaphore()
    for dev in ring + [pair]:
        pl.semaphore_signal(barrier, inc=1, device_id=dev, device_id_type=MESH)
    w_copies = [pltpu.make_async_copy(src, dst, w_sem.at[i]) for i, (src, dst) in enumerate(((wg_hbm, wg), (wu_hbm, wu), (wd_hbm, wd)))]
    for copy in w_copies:
        copy.start()
    pl.semaphore_wait(barrier, 3)

    def ring_copies(direction, v, x_src, g_src):
        return [remote(g_src, gbuf.at[v + 1, direction, core], gate_send.at[direction, v], gate_recv.at[direction, v], ring[direction]),
                remote(x_src, xbuf.at[v + 1, direction, core], ring_send.at[direction, v], ring_recv.at[direction, v], ring[direction])]

    def pair_copies(direction, k, c, x_src, g_src):
        return [remote(g_src, gbuf.at[k, direction, c], pgate_send.at[k, direction], pgate_recv.at[k, direction], pair),
                remote(x_src, xbuf.at[k, direction, c], pair_send.at[k, direction], pair_recv.at[k, direction], pair)]

    def held(direction, k, c):
        return xbuf.at[k, direction, c], gbuf.at[k, direction, c]

    def own(h):
        return r_ref.at[pl.ds(h * hr, hr)], gate_ref.at[h]

    def own_half(direction, v):
        return v if direction == 0 else 1 - v

    for v in range(2):
        for direction in range(2):
            for copy in ring_copies(direction, v, *own(own_half(direction, v))):
                copy.start()
        if v == 0:
            for h in range(2):
                for copy in pair_copies(h, 0, core, *own(h)):
                    copy.start()
    for h in range(2):
        xbuf[0, h, core] = r_ref[h * hr:(h + 1) * hr, :]
        gbuf[0, h, core] = gate_ref[h]

    def sum_copy(k, direction):
        return remote(cbuf.at[k, direction, other], cpart.at[k, direction], sum_send.at[k, direction], sum_recv.at[k, direction], pair)

    order = rs_order(half)

    def rs_place(direction, u):
        q, long_half, p = order[u]
        if long_half and q == half:
            return 2 * q - 1, direction, pl.ds(p * qr, qr)
        return 2 * q - 1 + long_half, 1 - direction, pl.ds(p * qr, qr)

    def rs_copy(direction, u):
        q, long_half, p = order[u]
        k, side, at = rs_place(direction, u)
        return remote(cbuf.at[k, side, core, at], inc.at[direction, q - 1, long_half, at], rs_send.at[direction, u], rs_recv.at[direction, u], ring[direction])

    def rs_step(direction, u):
        q, long_half, p = order[u]
        k, side, at = rs_place(direction, u)
        total = cbuf[k, side, core, at, :] + cpart[k, side, at, :]
        if (q + 1, long_half, p) in order:
            rs_copy(direction, order.index((q + 1, long_half, p))).wait_recv()
            total = total + inc[direction, q, long_half, at, :]
        cbuf[k, side, core, at, :] = total
        rs_copy(direction, u).start()

    e_first = n_local * me
    e_side = e_first // g_rows
    e_row = e_first - e_side * g_rows
    low_lanes = lax.broadcasted_iota(jnp.int32, (1, rows), 1) < hr

    def compute(k):
        x = xbuf[k].reshape(2 * rows, d)
        for e in range(n_local):
            for direction in range(2):
                a, b = [gbuf[k, direction, c, pl.ds(e_row + e, 1), :] for c in range(2)]
                ra, rb = pltpu.roll(a, hr, 1), pltpu.roll(b, hr, 1)
                row = jnp.where(low_lanes, jnp.where(e_side == 0, a, ra), jnp.where(e_side == 0, rb, b))
                gcol[e, direction * rows:(direction + 1) * rows, :] = jnp.transpose(jnp.broadcast_to(row, (rows, rows)))
        ft = 256
        for e in range(n_local):
            for nt in range(wg.shape[2] // ft):
                cols = slice(nt * ft, (nt + 1) * ft)
                g = jnp.dot(x, wg[e, :, cols], preferred_element_type=F32)
                u = jnp.dot(x, wu[e, :, cols], preferred_element_type=F32)
                act[:, cols] = (jax.nn.silu(g) * u).astype(BF16)
            a = act[...]
            gc = gcol[e]
            chosen = gc >= 0.0
            for nt in range(d // ft):
                f = jnp.dot(a, wd[e, :, nt * ft:(nt + 1) * ft], preferred_element_type=F32).astype(BF16).astype(F32)
                for l in range(ft // rows):
                    cols = slice(nt * ft + l * rows, nt * ft + (l + 1) * rows)
                    term = jnp.where(chosen, f[:, l * rows:(l + 1) * rows] * gc, 0.0).reshape(2, 2, hr, rows)
                    cbuf[k, :, :, :, cols] = term if e == 0 else cbuf[k, :, :, :, cols] + term

    for copy in w_copies:
        copy.wait()

    def body(k, carry):
        @pl.when(k > 0)
        def _():
            for direction in range(2):
                x_src, g_src = held(direction, k, core)
                for copy in ring_copies(direction, k - 1, x_src, g_src):
                    copy.wait_recv()

                @pl.when(k <= n - 3)
                def _():
                    for copy in ring_copies(direction, k + 1, x_src, g_src):
                        copy.start()

                for copy in pair_copies(direction, k, core, x_src, g_src):
                    copy.start()

        for direction in range(2):
            for copy in pair_copies(direction, k, other, *held(direction, k, other)):
                copy.wait_recv()

        @pl.when(k == n - 2)
        def _():
            for side in range(2):
                sum_copy(n - 3, side).wait_recv()
            for u in range(2):
                for direction in range(2):
                    rs_step(direction, u)

        compute(k)
        for direction in range(2):
            sum_copy(k, direction).start()
        return carry

    lax.fori_loop(0, n, body, 0)

    summed = {(n - 3, 0), (n - 3, 1)}

    def wait_sum(k, side):
        if (k, side) not in summed:
            sum_copy(k, side).wait_recv()
            summed.add((k, side))

    for u in range(2, len(order)):
        for direction in range(2):
            wait_sum(*rs_place(direction, u)[:2])
            rs_step(direction, u)
    for h in range(2):
        wait_sum(0, h)
    for long_half, p in ((0, 0), (0, 1), (1, 0), (1, 1)):
        u = order.index((1, long_half, p))
        for direction in range(2):
            h = 1 - long_half if direction == 0 else long_half
            rs_copy(direction, u).wait_recv()
            at = pl.ds(h * hr + p * qr, qr)
            part = pl.ds(p * qr, qr)
            got = inc[direction, 0, long_half, part, :]
            if long_half == 0:
                cbuf[0, h, core, part, :] = y_ref[at, :] + ((cbuf[0, h, core, part, :] + cpart[0, h, part, :]) + got)
            else:
                out_ref[at, :] = (cbuf[0, h, core, part, :] + got).astype(out_ref.dtype)

    for direction in range(2):
        for v in range(n - 1):
            src = own(own_half(direction, v)) if v < 2 else held(direction, v - 1, core)
            for copy in ring_copies(direction, v, *src):
                copy.wait_send()
        for k in range(n):
            src = own(direction) if k == 0 else held(direction, k, core)
            for copy in pair_copies(direction, k, core, *src):
                copy.wait_send()
            sum_copy(k, direction).wait_send()
        for u in range(len(order)):
            rs_copy(direction, u).wait_send()


def moe(n_ep, r, gates, y, w_gate, w_up, w_down):
    n = n_ep // 2
    rows, d = r.shape
    n_local, _, ff = w_gate.shape
    vm = pl.BlockSpec(memory_space=pltpu.VMEM)
    hbm = pl.BlockSpec(memory_space=pltpu.HBM)
    dma = pltpu.SemaphoreType.DMA
    n_rs = 2 * (n - 1)
    return pl.pallas_call(
        functools.partial(moe_kernel, n),
        out_shape=jax.ShapeDtypeStruct((rows, d), BF16),
        in_specs=[vm] * 3 + [hbm] * 3,
        out_specs=vm,
        scratch_shapes=[
            pltpu.VMEM((n, 2, 2, rows // 2, d), BF16),
            pltpu.VMEM((n, 2, 2) + gates.shape[1:], F32),
            pltpu.VMEM((n, 2, 2, rows // 2, d), F32),
            pltpu.VMEM((n, 2, rows // 2, d), F32),
            pltpu.VMEM((2, n // 2, 2, rows // 2, d), F32),
            pltpu.VMEM(w_gate.shape, BF16), pltpu.VMEM(w_up.shape, BF16), pltpu.VMEM(w_down.shape, BF16),
            pltpu.VMEM((2 * rows, ff), BF16),
            pltpu.VMEM((n_local, 2 * rows, rows), F32),
            dma((3,)),
            dma((2, n - 1)), dma((2, n - 1)), dma((2, n - 1)), dma((2, n - 1)),
            dma((n, 2)), dma((n, 2)), dma((n, 2)), dma((n, 2)),
            dma((n, 2)), dma((n, 2)),
            dma((2, n_rs)), dma((2, n_rs)),
        ],
        compiler_params=pltpu.CompilerParams(collective_id=0, has_side_effects=True, vmem_limit_bytes=40 * 1024 * 1024),
        name="moe",
    )(r, gates, y, *in_hbm(w_gate, w_up, w_down))


def solution(mesh):
    n_ep = mesh.shape['ep']
    row_spec = P(('dp', 'ep'), None)
    cache_spec = P(('dp', 'ep'), None, None, None)
    len_spec = P(('dp', 'ep'))
    rep_vec = P(None)
    rep_mat = P(None, None)
    exp_spec = P('ep', None, None)

    def local_step(hidden, k_cache, v_cache, seq_lens, expert_ids, ln_attn, w_q, w_k, w_v, q_gain, k_gain, w_o, ln_moe, w_router, w_gate, w_up, w_down):
        k_t = jnp.transpose(k_cache, (1, 2, 3, 0))
        v_t = jnp.transpose(v_cache, (1, 2, 3, 0))
        k_new, v_new, y, r, gates = attend(
            hidden, k_t, v_t, seq_lens[None, :], expert_ids.T, ln_attn.reshape(-1, 128), w_q, w_k, w_v,
            q_gain[None, :], k_gain[None, :], w_o, ln_moe.reshape(-1, 128), w_router.T)
        out = moe(n_ep, r, gates, y, w_gate, w_up, w_down)
        return out, jnp.transpose(k_new, (3, 0, 1, 2)), jnp.transpose(v_new, (3, 0, 1, 2))

    return jax.shard_map(local_step, mesh=mesh, in_specs=(row_spec, cache_spec, cache_spec, len_spec, row_spec, rep_vec, rep_mat, rep_mat, rep_mat, rep_vec, rep_vec, rep_mat, rep_vec, rep_mat, exp_spec, exp_spec, exp_spec), out_specs=(row_spec, cache_spec, cache_spec), check_vma=False)
```

```python
import functools

import jax
import jax.numpy as jnp
import numpy as np
from jax import lax
from jax.experimental import pallas as pl
from jax.experimental.pallas import tpu as pltpu
from jax.sharding import PartitionSpec as P

EPS = 1e-6
ROPE_BASE = 1000000.0
F32 = jnp.float32
BF16 = jnp.bfloat16
MESH = pl.DeviceIdType.MESH


def in_hbm(*arrays):
    return [pltpu.with_memory_space_constraint(a, pltpu.HBM) for a in arrays]


def attend_kernel(h_hbm, lens_hbm, ids_hbm, ln_a_hbm, qg_hbm, kg_hbm, ln_m_hbm, wr_hbm,
                  wq_hbm, wk_hbm, wv_hbm, wo_hbm, kc_hbm, vc_hbm,
                  kn_hbm, vn_hbm, y_ref, r_ref, gate_ref,
                  h_ref, lens_ref, ids_ref, ln_a_ref, qg_ref, kg_ref, ln_m_ref, wr_ref,
                  kbuf, vbuf, wq, wk, wv, wo, qrot, knew, vnew, score, attn, small_sem, in_sem, out_sem):
    t_max, n_kv, hd, n_seq = kc_hbm.shape
    n_heads = wq_hbm.shape[1] // hd
    grp = n_heads // n_kv
    half = hd // 2
    n_chunk = 4
    tc = t_max // n_chunk

    w_copies = [pltpu.make_async_copy(src, dst, in_sem.at[i])
                for i, (src, dst) in enumerate(((wk_hbm, wk), (wq_hbm, wq), (wv_hbm, wv), (wo_hbm, wo)))]
    k_in = [pltpu.make_async_copy(kc_hbm.at[pl.ds(c * tc, tc)], kbuf.at[pl.ds(c * tc, tc)], in_sem.at[4 + c]) for c in range(n_chunk)]
    v_in = [pltpu.make_async_copy(vc_hbm.at[pl.ds(c * tc, tc)], vbuf.at[pl.ds(c * tc, tc)], in_sem.at[4 + n_chunk + c]) for c in range(n_chunk)]
    k_out = [pltpu.make_async_copy(kbuf.at[pl.ds(c * tc, tc)], kn_hbm.at[pl.ds(c * tc, tc)], out_sem.at[c]) for c in range(n_chunk)]
    v_out = [pltpu.make_async_copy(vbuf.at[pl.ds(c * tc, tc)], vn_hbm.at[pl.ds(c * tc, tc)], out_sem.at[n_chunk + c]) for c in range(n_chunk)]
    small = [pltpu.make_async_copy(src, dst, small_sem.at[i]) for i, (src, dst) in enumerate((
        (h_hbm, h_ref), (lens_hbm, lens_ref), (ids_hbm, ids_ref), (ln_a_hbm, ln_a_ref), (qg_hbm, qg_ref), (kg_hbm, kg_ref), (ln_m_hbm, ln_m_ref), (wr_hbm, wr_ref)))]
    for copy in small + w_copies[:3]:
        copy.start()
    for copy in small:
        copy.wait()
    k_in[0].start()

    def vector(ref):
        rows = ref[...].astype(F32)
        return jnp.concatenate([rows[i:i + 1, :] for i in range(rows.shape[0])], axis=1)

    h32 = h_ref[...].astype(F32)
    mean_sq = jnp.mean(h32 * h32, axis=1, keepdims=True)
    x = (h32 * lax.rsqrt(mean_sq + EPS) * vector(ln_a_ref)).astype(BF16)

    lens = lens_ref[...]
    f_iota = lax.broadcasted_iota(jnp.int32, (half, n_seq), 0)
    inv_freq = np.power(np.float32(ROPE_BASE), -np.arange(0, hd, 2).astype(np.float32) / np.float32(hd))
    freq = jnp.zeros((half, n_seq), F32)
    for i in range(half):
        freq = jnp.where(f_iota == i, float(inv_freq[i]), freq)
    angles = lens.astype(F32) * freq
    cos_v = jnp.cos(angles)
    sin_v = jnp.sin(angles)

    def gain_tile(g_ref):
        row = g_ref[...].astype(F32)
        row = jnp.concatenate([row] * (n_seq // hd), axis=1)
        return jnp.transpose(jnp.broadcast_to(row, (n_seq, n_seq)))[:hd, :]

    def rope_heads(proj, gain, dst, heads):
        for i in range(heads):
            if i % 2 == 0:
                pair = jnp.transpose(proj[:, i * hd:(i + 2) * hd])
            vals = pair[(i % 2) * hd:(i % 2 + 1) * hd, :]
            ms = jnp.mean(vals * vals, axis=0, keepdims=True)
            vals = vals * lax.rsqrt(ms + EPS) * gain
            low, high = vals[:half, :], vals[half:, :]
            dst[i * hd:i * hd + half, :] = (low * cos_v - high * sin_v).astype(BF16).astype(F32)
            dst[i * hd + half:(i + 1) * hd, :] = (high * cos_v + low * sin_v).astype(BF16).astype(F32)

    w_copies[0].wait()
    for copy in k_in[1:]:
        copy.start()
    rope_heads(jnp.dot(x, wk[...], preferred_element_type=F32), gain_tile(kg_ref), knew, n_kv)
    w_copies[1].wait()
    for copy in v_in + w_copies[3:]:
        copy.start()
    rope_heads(jnp.dot(x, wq[...], preferred_element_type=F32), gain_tile(qg_ref), qrot, n_heads)
    w_copies[2].wait()
    v_proj = jnp.dot(x, wv[...], preferred_element_type=F32)
    for i in range(0, n_kv, 2):
        vnew[i * hd:(i + 2) * hd, :] = jnp.transpose(v_proj[:, i * hd:(i + 2) * hd]).astype(BF16).astype(F32)

    for c in range(n_chunk):
        k_in[c].wait()

        def k_body(kv, carry, c=c):
            new = knew[pl.ds(pl.multiple_of(kv * hd, hd), hd), :]
            qs = [qrot[pl.ds(pl.multiple_of((kv * grp + g) * hd, hd), hd), :] for g in range(grp)]
            rows = [[] for _ in range(grp)]
            for tt in range(tc):
                t = c * tc + tt
                kt = jnp.where(lens == t, new, kbuf[t, kv].astype(F32))
                kbuf[t, kv] = kt.astype(BF16)
                for g in range(grp):
                    rows[g].append(jnp.sum(kt * qs[g], axis=0, keepdims=True))
            for g in range(grp):
                score[kv * grp + g, c * tc:(c + 1) * tc, :] = jnp.concatenate(rows[g], axis=0)
            return carry

        lax.fori_loop(0, n_kv, k_body, 0)
        k_out[c].start()

    visible = lax.broadcasted_iota(jnp.int32, (t_max, n_seq), 0) <= lens

    def soft_body(j, carry):
        s = jnp.where(visible, score[j] * (hd ** -0.5), -1e30)
        e = jnp.exp(s - jnp.max(s, axis=0, keepdims=True))
        score[j] = (e / jnp.sum(e, axis=0, keepdims=True)).astype(BF16).astype(F32)
        return carry

    lax.fori_loop(0, n_heads, soft_body, 0, unroll=2)

    for c in range(n_chunk):
        v_in[c].wait()

        def v_body(kv, carry, c=c):
            new = vnew[pl.ds(pl.multiple_of(kv * hd, hd), hd), :]
            at = [pl.ds(pl.multiple_of((kv * grp + g) * hd, hd), hd) for g in range(grp)]
            acc = [None if c == 0 else attn[at[g], :] for g in range(grp)]
            for tt in range(tc):
                t = c * tc + tt
                vt = jnp.where(lens == t, new, vbuf[t, kv].astype(F32))
                vbuf[t, kv] = vt.astype(BF16)
                for g in range(grp):
                    term = vt * score[kv * grp + g, t:t + 1, :]
                    acc[g] = term if acc[g] is None else acc[g] + term
            for g in range(grp):
                attn[at[g], :] = acc[g]
            return carry

        lax.fori_loop(0, n_kv, v_body, 0)
        v_out[c].start()

    w_copies[3].wait()
    a_rows = jnp.concatenate([jnp.transpose(attn[i * n_seq:(i + 1) * n_seq, :]).astype(BF16) for i in range(n_heads * hd // n_seq)], axis=1)
    y = h32 + jnp.dot(a_rows, wo[...], preferred_element_type=F32)
    y_ref[...] = y
    mean_sq = jnp.mean(y * y, axis=1, keepdims=True)
    r = (y * lax.rsqrt(mean_sq + EPS) * vector(ln_m_ref)).astype(BF16)
    r_ref[...] = r
    logits = lax.dot_general(wr_ref[...], r, (((1,), (1,)), ((), ())), preferred_element_type=F32)
    e_iota = lax.broadcasted_iota(jnp.int32, logits.shape, 0)
    ids = ids_ref[...]
    chosen = e_iota == ids[0:1, :]
    for i in range(1, ids.shape[0]):
        chosen = chosen | (e_iota == ids[i:i + 1, :])
    top = jnp.max(jnp.where(chosen, logits, -jnp.inf), axis=0, keepdims=True)
    e = jnp.where(chosen, jnp.exp(logits - top), 0.0)
    gates = jnp.where(chosen, e / jnp.sum(e, axis=0, keepdims=True), -1.0)
    g_rows = gates.shape[0] // 2
    turned = pltpu.roll(gates, n_seq // 2, 1)
    low = lax.broadcasted_iota(jnp.int32, (g_rows, n_seq), 1) < n_seq // 2
    gate_ref[0] = jnp.where(low, gates[:g_rows, :], turned[g_rows:, :])
    gate_ref[1] = jnp.where(low, turned[:g_rows, :], gates[g_rows:, :])

    for copy in k_out + v_out:
        copy.wait()


def attend(hidden, k_t, v_t, lens, ids_t, ln_attn, w_q, w_k, w_v, q_gain, k_gain, w_o, ln_moe, w_router_t):
    n_seq, d = hidden.shape
    t_max, n_kv, hd, _ = k_t.shape
    hq, hk = w_q.shape[1], w_k.shape[1]
    n_heads = hq // hd
    n_exp = w_router_t.shape[0]
    vm = pl.BlockSpec(memory_space=pltpu.VMEM)
    hbm = pl.BlockSpec(memory_space=pltpu.HBM)
    small = (hidden, lens, ids_t, ln_attn, q_gain, k_gain, ln_moe, w_router_t)
    return pl.pallas_call(
        attend_kernel,
        out_shape=(
            jax.ShapeDtypeStruct(k_t.shape, k_t.dtype),
            jax.ShapeDtypeStruct(v_t.shape, v_t.dtype),
            jax.ShapeDtypeStruct((n_seq, d), F32),
            jax.ShapeDtypeStruct((n_seq, d), BF16),
            jax.ShapeDtypeStruct((2, n_exp // 2, n_seq), F32),
        ),
        in_specs=[hbm] * 14,
        out_specs=(hbm, hbm, vm, vm, vm),
        scratch_shapes=[pltpu.VMEM(a.shape, a.dtype) for a in small] + [
            pltpu.VMEM(k_t.shape, BF16), pltpu.VMEM(v_t.shape, BF16),
            pltpu.VMEM(w_q.shape, BF16), pltpu.VMEM(w_k.shape, BF16), pltpu.VMEM(w_v.shape, BF16), pltpu.VMEM(w_o.shape, BF16),
            pltpu.VMEM((hq, n_seq), F32), pltpu.VMEM((hk, n_seq), F32), pltpu.VMEM((hk, n_seq), F32),
            pltpu.VMEM((n_heads, t_max, n_seq), F32), pltpu.VMEM((hq, n_seq), F32),
            pltpu.SemaphoreType.DMA((len(small),)), pltpu.SemaphoreType.DMA((12,)), pltpu.SemaphoreType.DMA((8,)),
        ],
        compiler_params=pltpu.CompilerParams(vmem_limit_bytes=30 * 1024 * 1024),
        name="attend",
    )(*in_hbm(*small, w_q, w_k, w_v, w_o, k_t, v_t))


def rs_order(half):
    seq = [(half - 1, 0, 0), (half - 1, 0, 1)]
    for q in range(half, 3, -1):
        seq += [(q - 2, 0, 0), (q, 1, 0), (q, 1, 1), (q - 2, 0, 1)]
    return seq + [(3, 1, 0), (3, 1, 1), (1, 0, 0), (2, 1, 0), (2, 1, 1), (1, 0, 1), (1, 1, 0), (1, 1, 1)]


def moe_kernel(n, r_ref, gate_ref, y_ref, wg_hbm, wu_hbm, wd_hbm, out_ref,
               xbuf, gbuf, cbuf, cpart, inc, wg, wu, wd, act, gcol,
               w_sem, ring_send, ring_recv, gate_send, gate_recv,
               pair_send, pair_recv, pgate_send, pgate_recv,
               sum_send, sum_recv, rs_send, rs_recv):
    me = lax.axis_index("ep")
    chip = me // 2
    core = lax.rem(me, 2)
    other = 1 - core
    half = n // 2
    rows, d = r_ref.shape
    n_local = wg_hbm.shape[0]
    g_rows = gate_ref.shape[1]
    hr = rows // 2
    qr = hr // 2
    ring = [{"ep": 2 * lax.rem(chip + 1, n) + core}, {"ep": 2 * lax.rem(chip + n - 1, n) + core}]
    pair = {"ep": 2 * chip + other}

    def remote(src, dst, ssem, rsem, dev):
        return pltpu.make_async_remote_copy(src_ref=src, dst_ref=dst, send_sem=ssem, recv_sem=rsem, device_id=dev, device_id_type=MESH)

    barrier = pltpu.get_barrier_semaphore()
    for dev in ring + [pair]:
        pl.semaphore_signal(barrier, inc=1, device_id=dev, device_id_type=MESH)
    w_copies = [pltpu.make_async_copy(src, dst, w_sem.at[i]) for i, (src, dst) in enumerate(((wg_hbm, wg), (wu_hbm, wu), (wd_hbm, wd)))]
    for copy in w_copies:
        copy.start()
    pl.semaphore_wait(barrier, 3)

    def ring_copies(direction, v, x_src, g_src):
        return [remote(g_src, gbuf.at[v + 1, direction, core], gate_send.at[direction, v], gate_recv.at[direction, v], ring[direction]),
                remote(x_src, xbuf.at[v + 1, direction, core], ring_send.at[direction, v], ring_recv.at[direction, v], ring[direction])]

    def pair_copies(direction, k, c, x_src, g_src):
        return [remote(g_src, gbuf.at[k, direction, c], pgate_send.at[k, direction], pgate_recv.at[k, direction], pair),
                remote(x_src, xbuf.at[k, direction, c], pair_send.at[k, direction], pair_recv.at[k, direction], pair)]

    def held(direction, k, c):
        return xbuf.at[k, direction, c], gbuf.at[k, direction, c]

    def own(h):
        return r_ref.at[pl.ds(h * hr, hr)], gate_ref.at[h]

    def own_half(direction, v):
        return v if direction == 0 else 1 - v

    for v in range(2):
        for direction in range(2):
            for copy in ring_copies(direction, v, *own(own_half(direction, v))):
                copy.start()
        if v == 0:
            for h in range(2):
                for copy in pair_copies(h, 0, core, *own(h)):
                    copy.start()
    for h in range(2):
        xbuf[0, h, core] = r_ref[h * hr:(h + 1) * hr, :]
        gbuf[0, h, core] = gate_ref[h]

    def sum_copy(k, direction):
        return remote(cbuf.at[k, direction, other], cpart.at[k, direction], sum_send.at[k, direction], sum_recv.at[k, direction], pair)

    order = rs_order(half)

    def rs_place(direction, u):
        q, long_half, p = order[u]
        if long_half and q == half:
            return 2 * q - 1, direction, pl.ds(p * qr, qr)
        return 2 * q - 1 + long_half, 1 - direction, pl.ds(p * qr, qr)

    def rs_copy(direction, u):
        q, long_half, p = order[u]
        k, side, at = rs_place(direction, u)
        return remote(cbuf.at[k, side, core, at], inc.at[direction, q - 1, long_half, at], rs_send.at[direction, u], rs_recv.at[direction, u], ring[direction])

    def rs_step(direction, u):
        q, long_half, p = order[u]
        k, side, at = rs_place(direction, u)
        total = cbuf[k, side, core, at, :] + cpart[k, side, at, :]
        if (q + 1, long_half, p) in order:
            rs_copy(direction, order.index((q + 1, long_half, p))).wait_recv()
            total = total + inc[direction, q, long_half, at, :]
        cbuf[k, side, core, at, :] = total
        rs_copy(direction, u).start()

    e_first = n_local * me
    e_side = e_first // g_rows
    e_row = e_first - e_side * g_rows
    low_lanes = lax.broadcasted_iota(jnp.int32, (1, rows), 1) < hr

    def compute(k):
        x = xbuf[k].reshape(2 * rows, d)
        for e in range(n_local):
            for direction in range(2):
                a, b = [gbuf[k, direction, c, pl.ds(e_row + e, 1), :] for c in range(2)]
                ra, rb = pltpu.roll(a, hr, 1), pltpu.roll(b, hr, 1)
                row = jnp.where(low_lanes, jnp.where(e_side == 0, a, ra), jnp.where(e_side == 0, rb, b))
                gcol[e, direction * rows:(direction + 1) * rows, :] = jnp.transpose(jnp.broadcast_to(row, (rows, rows)))
        ft = 256
        for e in range(n_local):
            for nt in range(wg.shape[2] // ft):
                cols = slice(nt * ft, (nt + 1) * ft)
                g = jnp.dot(x, wg[e, :, cols], preferred_element_type=F32)
                u = jnp.dot(x, wu[e, :, cols], preferred_element_type=F32)
                act[:, cols] = (jax.nn.silu(g) * u).astype(BF16)
            a = act[...]
            gc = gcol[e]
            chosen = gc >= 0.0
            for nt in range(d // ft):
                f = jnp.dot(a, wd[e, :, nt * ft:(nt + 1) * ft], preferred_element_type=F32).astype(BF16).astype(F32)
                for l in range(ft // rows):
                    cols = slice(nt * ft + l * rows, nt * ft + (l + 1) * rows)
                    term = jnp.where(chosen, f[:, l * rows:(l + 1) * rows] * gc, 0.0).reshape(2, 2, hr, rows)
                    cbuf[k, :, :, :, cols] = term if e == 0 else cbuf[k, :, :, :, cols] + term

    def take(k):
        for direction in range(2):
            x_src, g_src = held(direction, k, core)
            for copy in ring_copies(direction, k - 1, x_src, g_src):
                copy.wait_recv()

            @pl.when(k <= n - 3)
            def _():
                for copy in ring_copies(direction, k + 1, x_src, g_src):
                    copy.start()

            for copy in pair_copies(direction, k, core, x_src, g_src):
                copy.start()

    def body(k, carry):
        @pl.when(k <= n - 4)
        def _():
            take(k + 1)

        @pl.when(k >= n - 2)
        def _():
            take(k)

        @pl.when(k == n - 2)
        def _():
            for side in range(2):
                sum_copy(n - 3, side).wait_recv()
            for u in range(2):
                for direction in range(2):
                    rs_step(direction, u)

        @pl.when(k == 0)
        def _():
            for copy in w_copies:
                copy.wait()

        for direction in range(2):
            for copy in pair_copies(direction, k, other, *held(direction, k, other)):
                copy.wait_recv()
        compute(k)
        for direction in range(2):
            sum_copy(k, direction).start()
        return carry

    lax.fori_loop(0, n, body, 0)

    summed = {(n - 3, 0), (n - 3, 1)}

    def wait_sum(k, side):
        if (k, side) not in summed:
            sum_copy(k, side).wait_recv()
            summed.add((k, side))

    for u in range(2, len(order)):
        for direction in range(2):
            wait_sum(*rs_place(direction, u)[:2])
            rs_step(direction, u)
    for h in range(2):
        wait_sum(0, h)
    for long_half, p in ((0, 0), (0, 1), (1, 0), (1, 1)):
        u = order.index((1, long_half, p))
        for direction in range(2):
            h = 1 - long_half if direction == 0 else long_half
            rs_copy(direction, u).wait_recv()
            at = pl.ds(h * hr + p * qr, qr)
            part = pl.ds(p * qr, qr)
            got = inc[direction, 0, long_half, part, :]
            if long_half == 0:
                cbuf[0, h, core, part, :] = y_ref[at, :] + ((cbuf[0, h, core, part, :] + cpart[0, h, part, :]) + got)
            else:
                out_ref[at, :] = (cbuf[0, h, core, part, :] + got).astype(out_ref.dtype)

    for direction in range(2):
        for v in range(n - 1):
            src = own(own_half(direction, v)) if v < 2 else held(direction, v - 1, core)
            for copy in ring_copies(direction, v, *src):
                copy.wait_send()
        for k in range(n):
            src = own(direction) if k == 0 else held(direction, k, core)
            for copy in pair_copies(direction, k, core, *src):
                copy.wait_send()
            sum_copy(k, direction).wait_send()
        for u in range(len(order)):
            rs_copy(direction, u).wait_send()


def moe(n_ep, r, gates, y, w_gate, w_up, w_down):
    n = n_ep // 2
    rows, d = r.shape
    n_local, _, ff = w_gate.shape
    vm = pl.BlockSpec(memory_space=pltpu.VMEM)
    hbm = pl.BlockSpec(memory_space=pltpu.HBM)
    dma = pltpu.SemaphoreType.DMA
    n_rs = 2 * (n - 1)
    return pl.pallas_call(
        functools.partial(moe_kernel, n),
        out_shape=jax.ShapeDtypeStruct((rows, d), BF16),
        in_specs=[vm] * 3 + [hbm] * 3,
        out_specs=vm,
        scratch_shapes=[
            pltpu.VMEM((n, 2, 2, rows // 2, d), BF16),
            pltpu.VMEM((n, 2, 2) + gates.shape[1:], F32),
            pltpu.VMEM((n, 2, 2, rows // 2, d), F32),
            pltpu.VMEM((n, 2, rows // 2, d), F32),
            pltpu.VMEM((2, n // 2, 2, rows // 2, d), F32),
            pltpu.VMEM(w_gate.shape, BF16), pltpu.VMEM(w_up.shape, BF16), pltpu.VMEM(w_down.shape, BF16),
            pltpu.VMEM((2 * rows, ff), BF16),
            pltpu.VMEM((n_local, 2 * rows, rows), F32),
            dma((3,)),
            dma((2, n - 1)), dma((2, n - 1)), dma((2, n - 1)), dma((2, n - 1)),
            dma((n, 2)), dma((n, 2)), dma((n, 2)), dma((n, 2)),
            dma((n, 2)), dma((n, 2)),
            dma((2, n_rs)), dma((2, n_rs)),
        ],
        compiler_params=pltpu.CompilerParams(collective_id=0, has_side_effects=True, vmem_limit_bytes=40 * 1024 * 1024),
        name="moe",
    )(r, gates, y, *in_hbm(w_gate, w_up, w_down))


def solution(mesh):
    n_ep = mesh.shape['ep']
    row_spec = P(('dp', 'ep'), None)
    cache_spec = P(('dp', 'ep'), None, None, None)
    len_spec = P(('dp', 'ep'))
    rep_vec = P(None)
    rep_mat = P(None, None)
    exp_spec = P('ep', None, None)

    def local_step(hidden, k_cache, v_cache, seq_lens, expert_ids, ln_attn, w_q, w_k, w_v, q_gain, k_gain, w_o, ln_moe, w_router, w_gate, w_up, w_down):
        k_t = jnp.transpose(k_cache, (1, 2, 3, 0))
        v_t = jnp.transpose(v_cache, (1, 2, 3, 0))
        k_new, v_new, y, r, gates = attend(
            hidden, k_t, v_t, seq_lens[None, :], expert_ids.T, ln_attn.reshape(-1, 128), w_q, w_k, w_v,
            q_gain[None, :], k_gain[None, :], w_o, ln_moe.reshape(-1, 128), w_router.T)
        out = moe(n_ep, r, gates, y, w_gate, w_up, w_down)
        return out, jnp.transpose(k_new, (3, 0, 1, 2)), jnp.transpose(v_new, (3, 0, 1, 2))

    return jax.shard_map(local_step, mesh=mesh, in_specs=(row_spec, cache_spec, cache_spec, len_spec, row_spec, rep_vec, rep_mat, rep_mat, rep_mat, rep_vec, rep_vec, rep_mat, rep_vec, rep_mat, exp_spec, exp_spec, exp_spec), out_specs=(row_spec, cache_spec, cache_spec), check_vma=False)
```

```python
import functools

import jax
import jax.numpy as jnp
import numpy as np
from jax import lax
from jax.experimental import pallas as pl
from jax.experimental.pallas import tpu as pltpu
from jax.sharding import PartitionSpec as P

EPS = 1e-6
ROPE_BASE = 1000000.0
F32 = jnp.float32
BF16 = jnp.bfloat16
MESH = pl.DeviceIdType.MESH


def in_hbm(*arrays):
    return [pltpu.with_memory_space_constraint(a, pltpu.HBM) for a in arrays]


def attend_kernel(h_hbm, lens_hbm, ids_hbm, ln_a_hbm, qg_hbm, kg_hbm, ln_m_hbm, wr_hbm,
                  wq_hbm, wk_hbm, wv_hbm, wo_hbm, kc_hbm, vc_hbm,
                  kn_hbm, vn_hbm, y_ref, r_ref, gate_ref,
                  h_ref, lens_ref, ids_ref, ln_a_ref, qg_ref, kg_ref, ln_m_ref, wr_ref,
                  kbuf, vbuf, wq, wk, wv, wo, qrot, knew, vnew, score, attn, small_sem, in_sem, out_sem):
    t_max, n_kv, hd, n_seq = kc_hbm.shape
    n_heads = wq_hbm.shape[1] // hd
    grp = n_heads // n_kv
    half = hd // 2
    n_chunk = 4
    tc = t_max // n_chunk

    w_copies = [pltpu.make_async_copy(src, dst, in_sem.at[i])
                for i, (src, dst) in enumerate(((wk_hbm, wk), (wq_hbm, wq), (wv_hbm, wv), (wo_hbm, wo)))]
    k_in = [pltpu.make_async_copy(kc_hbm.at[pl.ds(c * tc, tc)], kbuf.at[pl.ds(c * tc, tc)], in_sem.at[4 + c]) for c in range(n_chunk)]
    v_in = [pltpu.make_async_copy(vc_hbm.at[pl.ds(c * tc, tc)], vbuf.at[pl.ds(c * tc, tc)], in_sem.at[4 + n_chunk + c]) for c in range(n_chunk)]
    k_out = [pltpu.make_async_copy(kbuf.at[pl.ds(c * tc, tc)], kn_hbm.at[pl.ds(c * tc, tc)], out_sem.at[c]) for c in range(n_chunk)]
    v_out = [pltpu.make_async_copy(vbuf.at[pl.ds(c * tc, tc)], vn_hbm.at[pl.ds(c * tc, tc)], out_sem.at[n_chunk + c]) for c in range(n_chunk)]
    small = [pltpu.make_async_copy(src, dst, small_sem.at[i]) for i, (src, dst) in enumerate((
        (h_hbm, h_ref), (lens_hbm, lens_ref), (ids_hbm, ids_ref), (ln_a_hbm, ln_a_ref), (qg_hbm, qg_ref), (kg_hbm, kg_ref), (ln_m_hbm, ln_m_ref), (wr_hbm, wr_ref)))]
    for copy in small + w_copies[:3]:
        copy.start()
    for copy in small:
        copy.wait()
    k_in[0].start()

    def vector(ref):
        rows = ref[...].astype(F32)
        return jnp.concatenate([rows[i:i + 1, :] for i in range(rows.shape[0])], axis=1)

    h32 = h_ref[...].astype(F32)
    mean_sq = jnp.mean(h32 * h32, axis=1, keepdims=True)
    x = (h32 * lax.rsqrt(mean_sq + EPS) * vector(ln_a_ref)).astype(BF16)

    lens = lens_ref[...]
    f_iota = lax.broadcasted_iota(jnp.int32, (half, n_seq), 0)
    inv_freq = np.power(np.float32(ROPE_BASE), -np.arange(0, hd, 2).astype(np.float32) / np.float32(hd))
    freq = jnp.zeros((half, n_seq), F32)
    for i in range(half):
        freq = jnp.where(f_iota == i, float(inv_freq[i]), freq)
    angles = lens.astype(F32) * freq
    cos_v = jnp.cos(angles)
    sin_v = jnp.sin(angles)

    def gain_tile(g_ref):
        row = g_ref[...].astype(F32)
        row = jnp.concatenate([row] * (n_seq // hd), axis=1)
        return jnp.transpose(jnp.broadcast_to(row, (n_seq, n_seq)))[:hd, :]

    def rope_heads(proj, gain, dst, heads):
        for i in range(heads):
            if i % 2 == 0:
                pair = jnp.transpose(proj[:, i * hd:(i + 2) * hd])
            vals = pair[(i % 2) * hd:(i % 2 + 1) * hd, :]
            ms = jnp.mean(vals * vals, axis=0, keepdims=True)
            vals = vals * lax.rsqrt(ms + EPS) * gain
            low, high = vals[:half, :], vals[half:, :]
            dst[i * hd:i * hd + half, :] = (low * cos_v - high * sin_v).astype(BF16).astype(F32)
            dst[i * hd + half:(i + 1) * hd, :] = (high * cos_v + low * sin_v).astype(BF16).astype(F32)

    w_copies[0].wait()
    for copy in k_in[1:]:
        copy.start()
    rope_heads(jnp.dot(x, wk[...], preferred_element_type=F32), gain_tile(kg_ref), knew, n_kv)
    w_copies[1].wait()
    for copy in v_in + w_copies[3:]:
        copy.start()
    rope_heads(jnp.dot(x, wq[...], preferred_element_type=F32), gain_tile(qg_ref), qrot, n_heads)
    w_copies[2].wait()
    v_proj = jnp.dot(x, wv[...], preferred_element_type=F32)
    for i in range(0, n_kv, 2):
        vnew[i * hd:(i + 2) * hd, :] = jnp.transpose(v_proj[:, i * hd:(i + 2) * hd]).astype(BF16).astype(F32)

    for c in range(n_chunk):
        k_in[c].wait()

        def k_body(kv, carry, c=c):
            new = knew[pl.ds(pl.multiple_of(kv * hd, hd), hd), :]
            qs = [qrot[pl.ds(pl.multiple_of((kv * grp + g) * hd, hd), hd), :] for g in range(grp)]
            rows = [[] for _ in range(grp)]
            for tt in range(tc):
                t = c * tc + tt
                kt = jnp.where(lens == t, new, kbuf[t, kv].astype(F32))
                kbuf[t, kv] = kt.astype(BF16)
                for g in range(grp):
                    rows[g].append(jnp.sum(kt * qs[g], axis=0, keepdims=True))
            for g in range(grp):
                score[kv * grp + g, c * tc:(c + 1) * tc, :] = jnp.concatenate(rows[g], axis=0)
            return carry

        lax.fori_loop(0, n_kv, k_body, 0)
        k_out[c].start()

    visible = lax.broadcasted_iota(jnp.int32, (t_max, n_seq), 0) <= lens

    def soft_body(j, carry):
        s = jnp.where(visible, score[j] * (hd ** -0.5), -1e30)
        e = jnp.exp(s - jnp.max(s, axis=0, keepdims=True))
        score[j] = (e / jnp.sum(e, axis=0, keepdims=True)).astype(BF16).astype(F32)
        return carry

    lax.fori_loop(0, n_heads, soft_body, 0, unroll=2)

    for c in range(n_chunk):
        v_in[c].wait()

        def v_body(kv, carry, c=c):
            new = vnew[pl.ds(pl.multiple_of(kv * hd, hd), hd), :]
            at = [pl.ds(pl.multiple_of((kv * grp + g) * hd, hd), hd) for g in range(grp)]
            acc = [None if c == 0 else attn[at[g], :] for g in range(grp)]
            for tt in range(tc):
                t = c * tc + tt
                vt = jnp.where(lens == t, new, vbuf[t, kv].astype(F32))
                vbuf[t, kv] = vt.astype(BF16)
                for g in range(grp):
                    term = vt * score[kv * grp + g, t:t + 1, :]
                    acc[g] = term if acc[g] is None else acc[g] + term
            for g in range(grp):
                attn[at[g], :] = acc[g]
            return carry

        lax.fori_loop(0, n_kv, v_body, 0)
        v_out[c].start()

    w_copies[3].wait()
    a_rows = jnp.concatenate([jnp.transpose(attn[i * n_seq:(i + 1) * n_seq, :]).astype(BF16) for i in range(n_heads * hd // n_seq)], axis=1)
    y = h32 + jnp.dot(a_rows, wo[...], preferred_element_type=F32)
    y_ref[...] = y
    mean_sq = jnp.mean(y * y, axis=1, keepdims=True)
    r = (y * lax.rsqrt(mean_sq + EPS) * vector(ln_m_ref)).astype(BF16)
    r_ref[...] = r
    logits = lax.dot_general(wr_ref[...], r, (((1,), (1,)), ((), ())), preferred_element_type=F32)
    e_iota = lax.broadcasted_iota(jnp.int32, logits.shape, 0)
    ids = ids_ref[...]
    chosen = e_iota == ids[0:1, :]
    for i in range(1, ids.shape[0]):
        chosen = chosen | (e_iota == ids[i:i + 1, :])
    top = jnp.max(jnp.where(chosen, logits, -jnp.inf), axis=0, keepdims=True)
    e = jnp.where(chosen, jnp.exp(logits - top), 0.0)
    gates = jnp.where(chosen, e / jnp.sum(e, axis=0, keepdims=True), -1.0)
    g_rows = gates.shape[0] // 2
    turned = pltpu.roll(gates, n_seq // 2, 1)
    low = lax.broadcasted_iota(jnp.int32, (g_rows, n_seq), 1) < n_seq // 2
    gate_ref[0] = jnp.where(low, gates[:g_rows, :], turned[g_rows:, :])
    gate_ref[1] = jnp.where(low, turned[:g_rows, :], gates[g_rows:, :])

    for copy in k_out + v_out:
        copy.wait()


def attend(hidden, k_t, v_t, lens, ids_t, ln_attn, w_q, w_k, w_v, q_gain, k_gain, w_o, ln_moe, w_router_t):
    n_seq, d = hidden.shape
    t_max, n_kv, hd, _ = k_t.shape
    hq, hk = w_q.shape[1], w_k.shape[1]
    n_heads = hq // hd
    n_exp = w_router_t.shape[0]
    vm = pl.BlockSpec(memory_space=pltpu.VMEM)
    hbm = pl.BlockSpec(memory_space=pltpu.HBM)
    small = (hidden, lens, ids_t, ln_attn, q_gain, k_gain, ln_moe, w_router_t)
    return pl.pallas_call(
        attend_kernel,
        out_shape=(
            jax.ShapeDtypeStruct(k_t.shape, k_t.dtype),
            jax.ShapeDtypeStruct(v_t.shape, v_t.dtype),
            jax.ShapeDtypeStruct((n_seq, d), F32),
            jax.ShapeDtypeStruct((n_seq, d), BF16),
            jax.ShapeDtypeStruct((2, n_exp // 2, n_seq), F32),
        ),
        in_specs=[hbm] * 14,
        out_specs=(hbm, hbm, vm, vm, vm),
        scratch_shapes=[pltpu.VMEM(a.shape, a.dtype) for a in small] + [
            pltpu.VMEM(k_t.shape, BF16), pltpu.VMEM(v_t.shape, BF16),
            pltpu.VMEM(w_q.shape, BF16), pltpu.VMEM(w_k.shape, BF16), pltpu.VMEM(w_v.shape, BF16), pltpu.VMEM(w_o.shape, BF16),
            pltpu.VMEM((hq, n_seq), F32), pltpu.VMEM((hk, n_seq), F32), pltpu.VMEM((hk, n_seq), F32),
            pltpu.VMEM((n_heads, t_max, n_seq), F32), pltpu.VMEM((hq, n_seq), F32),
            pltpu.SemaphoreType.DMA((len(small),)), pltpu.SemaphoreType.DMA((12,)), pltpu.SemaphoreType.DMA((8,)),
        ],
        compiler_params=pltpu.CompilerParams(vmem_limit_bytes=30 * 1024 * 1024),
        name="attend",
    )(*in_hbm(*small, w_q, w_k, w_v, w_o, k_t, v_t))


def rs_order(half):
    seq = [(half - 2, 3), (half - 1, 2), (half + 1, 0), (half, 1)]
    last = dict((c, q) for q, c in seq)
    for c in (3, 2, 0, 1, 2, 0, 1, 0, 1, 0):
        last[c] -= 1
        seq.append((last[c], c))
    return seq


def moe_kernel(n, r_ref, gate_ref, y_ref, wg_hbm, wu_hbm, wd_hbm, out_ref,
               xbuf, gbuf, cbuf, cpart, inc, wg, wu, wd, act, gcol,
               w_sem, ring_send, ring_recv, gate_send, gate_recv,
               pair_send, pair_recv, pgate_send, pgate_recv,
               sum_send, sum_recv, rs_send, rs_recv):
    me = lax.axis_index("ep")
    chip = me // 2
    core = lax.rem(me, 2)
    other = 1 - core
    half = n // 2
    rows, d = r_ref.shape
    n_local = wg_hbm.shape[0]
    g_rows = gate_ref.shape[1]
    hr = rows // 2
    qr = hr // 2
    ring = [{"ep": 2 * lax.rem(chip + 1, n) + core}, {"ep": 2 * lax.rem(chip + n - 1, n) + core}]
    pair = {"ep": 2 * chip + other}

    def remote(src, dst, ssem, rsem, dev):
        return pltpu.make_async_remote_copy(src_ref=src, dst_ref=dst, send_sem=ssem, recv_sem=rsem, device_id=dev, device_id_type=MESH)

    barrier = pltpu.get_barrier_semaphore()
    for dev in ring + [pair]:
        pl.semaphore_signal(barrier, inc=1, device_id=dev, device_id_type=MESH)
    w_copies = [pltpu.make_async_copy(src, dst, w_sem.at[i]) for i, (src, dst) in enumerate(((wg_hbm, wg), (wu_hbm, wu), (wd_hbm, wd)))]
    for copy in w_copies:
        copy.start()
    pl.semaphore_wait(barrier, 3)

    def ring_copies(direction, v, x_src, g_src):
        return [remote(g_src, gbuf.at[v + 1, direction, core], gate_send.at[direction, v], gate_recv.at[direction, v], ring[direction]),
                remote(x_src, xbuf.at[v + 1, direction, core], ring_send.at[direction, v], ring_recv.at[direction, v], ring[direction])]

    def pair_copies(direction, k, c, x_src, g_src):
        return [remote(g_src, gbuf.at[k, direction, c], pgate_send.at[k, direction], pgate_recv.at[k, direction], pair),
                remote(x_src, xbuf.at[k, direction, c], pair_send.at[k, direction], pair_recv.at[k, direction], pair)]

    def held(direction, k, c):
        return xbuf.at[k, direction, c], gbuf.at[k, direction, c]

    def own(h):
        return r_ref.at[pl.ds(h * hr, hr)], gate_ref.at[h]

    def own_half(direction, v):
        return v if direction == 0 else 1 - v

    for v in range(2):
        for direction in range(2):
            for copy in ring_copies(direction, v, *own(own_half(direction, v))):
                copy.start()
        if v == 0:
            for h in range(2):
                for copy in pair_copies(h, 0, core, *own(h)):
                    copy.start()
    for h in range(2):
        xbuf[0, h, core] = r_ref[h * hr:(h + 1) * hr, :]
        gbuf[0, h, core] = gate_ref[h]

    def sum_copy(k, direction):
        return remote(cbuf.at[k, direction, other], cpart.at[k, direction], sum_send.at[k, direction], sum_recv.at[k, direction], pair)

    order = rs_order(half)

    def quarter(direction, chain):
        return chain if direction == 0 else 3 - chain

    def rs_place(direction, u):
        q, chain = order[u]
        i = quarter(direction, chain)
        step = q if direction == 0 else -q
        step = step - n if step > half else step + n if step <= -half else step
        h = i // 2
        if step == half:
            k, side = n - 1, h
        elif step > 0:
            k, side = 2 * step - h, 1
        else:
            k, side = -2 * step - 1 + h, 0
        return k, side, pl.ds((i % 2) * qr, qr)

    def rs_copy(direction, u):
        q, chain = order[u]
        k, side, at = rs_place(direction, u)
        return remote(cbuf.at[k, side, core, at], inc.at[direction, q - 1, chain], rs_send.at[direction, u], rs_recv.at[direction, u], ring[direction])

    def rs_step(direction, u):
        q, chain = order[u]
        k, side, at = rs_place(direction, u)
        total = cbuf[k, side, core, at, :] + cpart[k, side, at, :]
        if (q + 1, chain) in order:
            rs_copy(direction, order.index((q + 1, chain))).wait_recv()
            total = total + inc[direction, q, chain]
        cbuf[k, side, core, at, :] = total
        rs_copy(direction, u).start()

    e_first = n_local * me
    e_side = e_first // g_rows
    e_row = e_first - e_side * g_rows
    low_lanes = lax.broadcasted_iota(jnp.int32, (1, rows), 1) < hr

    def compute(k):
        x = xbuf[k].reshape(2 * rows, d)
        for e in range(n_local):
            for direction in range(2):
                a, b = [gbuf[k, direction, c, pl.ds(e_row + e, 1), :] for c in range(2)]
                ra, rb = pltpu.roll(a, hr, 1), pltpu.roll(b, hr, 1)
                row = jnp.where(low_lanes, jnp.where(e_side == 0, a, ra), jnp.where(e_side == 0, rb, b))
                gcol[e, direction * rows:(direction + 1) * rows, :] = jnp.transpose(jnp.broadcast_to(row, (rows, rows)))
        ft = 256
        for e in range(n_local):
            for nt in range(wg.shape[2] // ft):
                cols = slice(nt * ft, (nt + 1) * ft)
                g = jnp.dot(x, wg[e, :, cols], preferred_element_type=F32)
                u = jnp.dot(x, wu[e, :, cols], preferred_element_type=F32)
                act[:, cols] = (jax.nn.silu(g) * u).astype(BF16)
            a = act[...]
            gc = gcol[e]
            chosen = gc >= 0.0
            for nt in range(d // ft):
                f = jnp.dot(a, wd[e, :, nt * ft:(nt + 1) * ft], preferred_element_type=F32).astype(BF16).astype(F32)
                for l in range(ft // rows):
                    cols = slice(nt * ft + l * rows, nt * ft + (l + 1) * rows)
                    term = jnp.where(chosen, f[:, l * rows:(l + 1) * rows] * gc, 0.0).reshape(2, 2, hr, rows)
                    cbuf[k, :, :, :, cols] = term if e == 0 else cbuf[k, :, :, :, cols] + term

    def take(k):
        for direction in range(2):
            x_src, g_src = held(direction, k, core)
            for copy in ring_copies(direction, k - 1, x_src, g_src):
                copy.wait_recv()

            @pl.when(k <= n - 3)
            def _():
                for copy in ring_copies(direction, k + 1, x_src, g_src):
                    copy.start()

            for copy in pair_copies(direction, k, core, x_src, g_src):
                copy.start()

    def body(k, carry):
        @pl.when(k <= n - 4)
        def _():
            take(k + 1)

        @pl.when(k >= n - 2)
        def _():
            take(k)

        @pl.when(k == n - 3)
        def _():
            for side in range(2):
                sum_copy(n - 5, side).wait_recv()
            for direction in range(2):
                rs_step(direction, 0)

        @pl.when(k == n - 2)
        def _():
            for side in range(2):
                sum_copy(n - 3, side).wait_recv()
            for u in range(1, 3):
                for direction in range(2):
                    rs_step(direction, u)

        @pl.when(k == 0)
        def _():
            for copy in w_copies:
                copy.wait()

        for direction in range(2):
            for copy in pair_copies(direction, k, other, *held(direction, k, other)):
                copy.wait_recv()
        compute(k)
        for direction in range(2):
            sum_copy(k, direction).start()
        return carry

    lax.fori_loop(0, n, body, 0)

    summed = {(n - 5, 0), (n - 5, 1), (n - 3, 0), (n - 3, 1)}

    def wait_sum(k, side):
        if (k, side) not in summed:
            sum_copy(k, side).wait_recv()
            summed.add((k, side))

    for u in range(3, len(order)):
        for direction in range(2):
            wait_sum(*rs_place(direction, u)[:2])
            rs_step(direction, u)
    for h in range(2):
        wait_sum(0, h)
    seen = set()
    for u, (q, chain) in enumerate(order):
        for direction in range(2) if q == 1 else ():
            rs_copy(direction, u).wait_recv()
            i = quarter(direction, chain)
            part = pl.ds((i % 2) * qr, qr)
            at = pl.ds(i * qr, qr)
            if i in seen:
                out_ref[at, :] = (cbuf[0, i // 2, core, part, :] + inc[direction, 0, chain]).astype(out_ref.dtype)
            else:
                seen.add(i)
                cbuf[0, i // 2, core, part, :] = y_ref[at, :] + ((cbuf[0, i // 2, core, part, :] + cpart[0, i // 2, part, :]) + inc[direction, 0, chain])

    for direction in range(2):
        for v in range(n - 1):
            src = own(own_half(direction, v)) if v < 2 else held(direction, v - 1, core)
            for copy in ring_copies(direction, v, *src):
                copy.wait_send()
        for k in range(n):
            src = own(direction) if k == 0 else held(direction, k, core)
            for copy in pair_copies(direction, k, core, *src):
                copy.wait_send()
            sum_copy(k, direction).wait_send()
        for u in range(len(order)):
            rs_copy(direction, u).wait_send()


def moe(n_ep, r, gates, y, w_gate, w_up, w_down):
    n = n_ep // 2
    rows, d = r.shape
    n_local, _, ff = w_gate.shape
    vm = pl.BlockSpec(memory_space=pltpu.VMEM)
    hbm = pl.BlockSpec(memory_space=pltpu.HBM)
    dma = pltpu.SemaphoreType.DMA
    n_rs = 2 * (n - 1)
    return pl.pallas_call(
        functools.partial(moe_kernel, n),
        out_shape=jax.ShapeDtypeStruct((rows, d), BF16),
        in_specs=[vm] * 3 + [hbm] * 3,
        out_specs=vm,
        scratch_shapes=[
            pltpu.VMEM((n, 2, 2, rows // 2, d), BF16),
            pltpu.VMEM((n, 2, 2) + gates.shape[1:], F32),
            pltpu.VMEM((n, 2, 2, rows // 2, d), F32),
            pltpu.VMEM((n, 2, rows // 2, d), F32),
            pltpu.VMEM((2, n // 2 + 1, 4, rows // 4, d), F32),
            pltpu.VMEM(w_gate.shape, BF16), pltpu.VMEM(w_up.shape, BF16), pltpu.VMEM(w_down.shape, BF16),
            pltpu.VMEM((2 * rows, ff), BF16),
            pltpu.VMEM((n_local, 2 * rows, rows), F32),
            dma((3,)),
            dma((2, n - 1)), dma((2, n - 1)), dma((2, n - 1)), dma((2, n - 1)),
            dma((n, 2)), dma((n, 2)), dma((n, 2)), dma((n, 2)),
            dma((n, 2)), dma((n, 2)),
            dma((2, n_rs)), dma((2, n_rs)),
        ],
        compiler_params=pltpu.CompilerParams(collective_id=0, has_side_effects=True, vmem_limit_bytes=40 * 1024 * 1024),
        name="moe",
    )(r, gates, y, *in_hbm(w_gate, w_up, w_down))


def solution(mesh):
    n_ep = mesh.shape['ep']
    row_spec = P(('dp', 'ep'), None)
    cache_spec = P(('dp', 'ep'), None, None, None)
    len_spec = P(('dp', 'ep'))
    rep_vec = P(None)
    rep_mat = P(None, None)
    exp_spec = P('ep', None, None)

    def local_step(hidden, k_cache, v_cache, seq_lens, expert_ids, ln_attn, w_q, w_k, w_v, q_gain, k_gain, w_o, ln_moe, w_router, w_gate, w_up, w_down):
        k_t = jnp.transpose(k_cache, (1, 2, 3, 0))
        v_t = jnp.transpose(v_cache, (1, 2, 3, 0))
        k_new, v_new, y, r, gates = attend(
            hidden, k_t, v_t, seq_lens[None, :], expert_ids.T, ln_attn.reshape(-1, 128), w_q, w_k, w_v,
            q_gain[None, :], k_gain[None, :], w_o, ln_moe.reshape(-1, 128), w_router.T)
        out = moe(n_ep, r, gates, y, w_gate, w_up, w_down)
        return out, jnp.transpose(k_new, (3, 0, 1, 2)), jnp.transpose(v_new, (3, 0, 1, 2))

    return jax.shard_map(local_step, mesh=mesh, in_specs=(row_spec, cache_spec, cache_spec, len_spec, row_spec, rep_vec, rep_mat, rep_mat, rep_mat, rep_vec, rep_vec, rep_mat, rep_vec, rep_mat, exp_spec, exp_spec, exp_spec), out_specs=(row_spec, cache_spec, cache_spec), check_vma=False)
```

```python
import functools

import jax
import jax.numpy as jnp
import numpy as np
from jax import lax
from jax.experimental import pallas as pl
from jax.experimental.pallas import tpu as pltpu
from jax.sharding import PartitionSpec as P

EPS = 1e-6
ROPE_BASE = 1000000.0
F32 = jnp.float32
BF16 = jnp.bfloat16
MESH = pl.DeviceIdType.MESH


def in_hbm(*arrays):
    return [pltpu.with_memory_space_constraint(a, pltpu.HBM) for a in arrays]


def attend_kernel(h_hbm, lens_hbm, ids_hbm, ln_a_hbm, qg_hbm, kg_hbm, ln_m_hbm, wr_hbm,
                  wq_hbm, wk_hbm, wv_hbm, wo_hbm, kc_hbm, vc_hbm,
                  kn_hbm, vn_hbm, y_ref, r_ref, gate_ref,
                  h_ref, lens_ref, ids_ref, ln_a_ref, qg_ref, kg_ref, ln_m_ref, wr_ref,
                  kbuf, vbuf, wq, wk, wv, wo, qrot, knew, vnew, score, attn, small_sem, in_sem, out_sem):
    t_max, n_kv, hd, n_seq = kc_hbm.shape
    n_heads = wq_hbm.shape[1] // hd
    grp = n_heads // n_kv
    half = hd // 2
    n_chunk = 4
    tc = t_max // n_chunk

    w_copies = [pltpu.make_async_copy(src, dst, in_sem.at[i])
                for i, (src, dst) in enumerate(((wk_hbm, wk), (wq_hbm, wq), (wv_hbm, wv), (wo_hbm, wo)))]
    k_in = [pltpu.make_async_copy(kc_hbm.at[pl.ds(c * tc, tc)], kbuf.at[pl.ds(c * tc, tc)], in_sem.at[4 + c]) for c in range(n_chunk)]
    v_in = [pltpu.make_async_copy(vc_hbm.at[pl.ds(c * tc, tc)], vbuf.at[pl.ds(c * tc, tc)], in_sem.at[4 + n_chunk + c]) for c in range(n_chunk)]
    k_out = [pltpu.make_async_copy(kbuf.at[pl.ds(c * tc, tc)], kn_hbm.at[pl.ds(c * tc, tc)], out_sem.at[c]) for c in range(n_chunk)]
    v_out = [pltpu.make_async_copy(vbuf.at[pl.ds(c * tc, tc)], vn_hbm.at[pl.ds(c * tc, tc)], out_sem.at[n_chunk + c]) for c in range(n_chunk)]
    small = [pltpu.make_async_copy(src, dst, small_sem.at[i]) for i, (src, dst) in enumerate((
        (h_hbm, h_ref), (lens_hbm, lens_ref), (ids_hbm, ids_ref), (ln_a_hbm, ln_a_ref), (qg_hbm, qg_ref), (kg_hbm, kg_ref), (ln_m_hbm, ln_m_ref), (wr_hbm, wr_ref)))]
    for copy in small + w_copies[:2]:
        copy.start()
    for copy in small:
        copy.wait()
    k_in[0].start()

    def vector(ref):
        rows = ref[...].astype(F32)
        return jnp.concatenate([rows[i:i + 1, :] for i in range(rows.shape[0])], axis=1)

    h32 = h_ref[...].astype(F32)
    mean_sq = jnp.mean(h32 * h32, axis=1, keepdims=True)
    x = (h32 * lax.rsqrt(mean_sq + EPS) * vector(ln_a_ref)).astype(BF16)

    lens = lens_ref[...]
    f_iota = lax.broadcasted_iota(jnp.int32, (half, n_seq), 0)
    inv_freq = np.power(np.float32(ROPE_BASE), -np.arange(0, hd, 2).astype(np.float32) / np.float32(hd))
    freq = jnp.zeros((half, n_seq), F32)
    for i in range(half):
        freq = jnp.where(f_iota == i, float(inv_freq[i]), freq)
    angles = lens.astype(F32) * freq
    cos_v = jnp.cos(angles)
    sin_v = jnp.sin(angles)

    def gain_tile(g_ref):
        row = g_ref[...].astype(F32)
        row = jnp.concatenate([row] * (n_seq // hd), axis=1)
        return jnp.transpose(jnp.broadcast_to(row, (n_seq, n_seq)))[:hd, :]

    def rope_heads(proj, gain, dst, heads):
        for i in range(heads):
            if i % 2 == 0:
                pair = jnp.transpose(proj[:, i * hd:(i + 2) * hd])
            vals = pair[(i % 2) * hd:(i % 2 + 1) * hd, :]
            ms = jnp.mean(vals * vals, axis=0, keepdims=True)
            vals = vals * lax.rsqrt(ms + EPS) * gain
            low, high = vals[:half, :], vals[half:, :]
            dst[i * hd:i * hd + half, :] = (low * cos_v - high * sin_v).astype(BF16).astype(F32)
            dst[i * hd + half:(i + 1) * hd, :] = (high * cos_v + low * sin_v).astype(BF16).astype(F32)

    w_copies[0].wait()
    for copy in k_in[1:] + w_copies[2:3]:
        copy.start()
    rope_heads(jnp.dot(x, wk[...], preferred_element_type=F32), gain_tile(kg_ref), knew, n_kv)
    w_copies[1].wait()
    for copy in v_in + w_copies[3:]:
        copy.start()
    rope_heads(jnp.dot(x, wq[...], preferred_element_type=F32), gain_tile(qg_ref), qrot, n_heads)
    sub = lax.broadcasted_iota(jnp.int32, (8, n_seq), 0)

    def fold(terms):
        top = sub < 4
        pairs = [jnp.where(top, a, b) + pltpu.roll(jnp.where(top, b, a), 4, 0)
                 for a, b in ((terms[0], terms[4]), (terms[2], terms[6]), (terms[1], terms[5]), (terms[3], terms[7]))]
        for shift, keep in ((2, sub % 4 < 2), (1, sub % 2 < 1)):
            pairs = [jnp.where(keep, a, pltpu.roll(b, shift, 0)) + jnp.where(keep, pltpu.roll(a, 8 - shift, 0), b)
                     for a, b in zip(pairs[0::2], pairs[1::2])]
        return pairs[0]

    for c in range(n_chunk):
        k_in[c].wait()

        def k_body(kv, carry, c=c):
            new = knew[pl.ds(pl.multiple_of(kv * hd, hd), hd), :]
            qs = [qrot[pl.ds(pl.multiple_of((kv * grp + g) * hd, hd), hd), :] for g in range(grp)]
            rows = [[] for _ in range(grp)]
            for tt in range(tc):
                t = c * tc + tt
                kt = jnp.where(lens == t, new, kbuf[t, kv].astype(F32))
                kbuf[t, kv] = kt.astype(BF16)
                for g in range(grp):
                    rows[g].append(jnp.sum((kt * qs[g]).reshape(hd // 8, 8, n_seq), axis=0))
            for g in range(grp):
                score[kv * grp + g, c * tc:(c + 1) * tc, :] = fold(rows[g])
            return carry

        lax.fori_loop(0, n_kv, k_body, 0)
        k_out[c].start()

    w_copies[2].wait()
    v_proj = jnp.dot(x, wv[...], preferred_element_type=F32)
    for i in range(0, n_kv, 2):
        vnew[i * hd:(i + 2) * hd, :] = jnp.transpose(v_proj[:, i * hd:(i + 2) * hd]).astype(BF16).astype(F32)

    visible = lax.broadcasted_iota(jnp.int32, (t_max, n_seq), 0) <= lens

    def soft_body(j, carry):
        s = jnp.where(visible, score[j] * (hd ** -0.5), -1e30)
        e = jnp.exp(s - jnp.max(s, axis=0, keepdims=True))
        score[j] = (e / jnp.sum(e, axis=0, keepdims=True)).astype(BF16).astype(F32)
        return carry

    lax.fori_loop(0, n_heads, soft_body, 0, unroll=2)

    for c in range(n_chunk):
        v_in[c].wait()

        def v_body(kv, carry, c=c):
            new = vnew[pl.ds(pl.multiple_of(kv * hd, hd), hd), :]
            at = [pl.ds(pl.multiple_of((kv * grp + g) * hd, hd), hd) for g in range(grp)]
            acc = [None if c == 0 else attn[at[g], :] for g in range(grp)]
            for tt in range(tc):
                t = c * tc + tt
                vt = jnp.where(lens == t, new, vbuf[t, kv].astype(F32))
                vbuf[t, kv] = vt.astype(BF16)
                for g in range(grp):
                    term = vt * score[kv * grp + g, t:t + 1, :]
                    acc[g] = term if acc[g] is None else acc[g] + term
            for g in range(grp):
                attn[at[g], :] = acc[g]
            return carry

        lax.fori_loop(0, n_kv, v_body, 0)
        v_out[c].start()

    w_copies[3].wait()
    a_rows = jnp.concatenate([jnp.transpose(attn[i * n_seq:(i + 1) * n_seq, :]).astype(BF16) for i in range(n_heads * hd // n_seq)], axis=1)
    y = h32 + jnp.dot(a_rows, wo[...], preferred_element_type=F32)
    y_ref[...] = y
    mean_sq = jnp.mean(y * y, axis=1, keepdims=True)
    r = (y * lax.rsqrt(mean_sq + EPS) * vector(ln_m_ref)).astype(BF16)
    r_ref[...] = r
    logits = lax.dot_general(wr_ref[...], r, (((1,), (1,)), ((), ())), preferred_element_type=F32)
    e_iota = lax.broadcasted_iota(jnp.int32, logits.shape, 0)
    ids = ids_ref[...]
    chosen = e_iota == ids[0:1, :]
    for i in range(1, ids.shape[0]):
        chosen = chosen | (e_iota == ids[i:i + 1, :])
    top = jnp.max(jnp.where(chosen, logits, -jnp.inf), axis=0, keepdims=True)
    e = jnp.where(chosen, jnp.exp(logits - top), 0.0)
    gates = e / jnp.sum(e, axis=0, keepdims=True)
    picked = jnp.concatenate([jnp.sum(jnp.where(e_iota == ids[i:i + 1, :], gates, 0.0), axis=0, keepdims=True) for i in range(ids.shape[0])], axis=0)
    ids32 = ids.astype(F32)
    low = lax.broadcasted_iota(jnp.int32, ids.shape, 1) < n_seq // 2
    gate_ref[0] = jnp.where(low, picked, pltpu.roll(ids32, n_seq // 2, 1))
    gate_ref[1] = jnp.where(low, pltpu.roll(picked, n_seq // 2, 1), ids32)

    for copy in k_out + v_out:
        copy.wait()


def attend(hidden, k_t, v_t, lens, ids_t, ln_attn, w_q, w_k, w_v, q_gain, k_gain, w_o, ln_moe, w_router_t):
    n_seq, d = hidden.shape
    t_max, n_kv, hd, _ = k_t.shape
    hq, hk = w_q.shape[1], w_k.shape[1]
    n_heads = hq // hd
    vm = pl.BlockSpec(memory_space=pltpu.VMEM)
    hbm = pl.BlockSpec(memory_space=pltpu.HBM)
    small = (hidden, lens, ids_t, ln_attn, q_gain, k_gain, ln_moe, w_router_t)
    return pl.pallas_call(
        attend_kernel,
        out_shape=(
            jax.ShapeDtypeStruct(k_t.shape, k_t.dtype),
            jax.ShapeDtypeStruct(v_t.shape, v_t.dtype),
            jax.ShapeDtypeStruct((n_seq, d), F32),
            jax.ShapeDtypeStruct((n_seq, d), BF16),
            jax.ShapeDtypeStruct((2, ids_t.shape[0], n_seq), F32),
        ),
        in_specs=[hbm] * 14,
        out_specs=(hbm, hbm, vm, vm, vm),
        scratch_shapes=[pltpu.VMEM(a.shape, a.dtype) for a in small] + [
            pltpu.VMEM(k_t.shape, BF16), pltpu.VMEM(v_t.shape, BF16),
            pltpu.VMEM(w_q.shape, BF16), pltpu.VMEM(w_k.shape, BF16), pltpu.VMEM(w_v.shape, BF16), pltpu.VMEM(w_o.shape, BF16),
            pltpu.VMEM((hq, n_seq), F32), pltpu.VMEM((hk, n_seq), F32), pltpu.VMEM((hk, n_seq), F32),
            pltpu.VMEM((n_heads, t_max, n_seq), F32), pltpu.VMEM((hq, n_seq), F32),
            pltpu.SemaphoreType.DMA((len(small),)), pltpu.SemaphoreType.DMA((12,)), pltpu.SemaphoreType.DMA((8,)),
        ],
        compiler_params=pltpu.CompilerParams(vmem_limit_bytes=30 * 1024 * 1024),
        name="attend",
    )(*in_hbm(*small, w_q, w_k, w_v, w_o, k_t, v_t))


def rs_order(half):
    seq = [(half - 2, 3), (half + 1, 0), (half - 1, 2), (half, 1)]
    last = dict((c, q) for q, c in seq)
    for c in (0, 3, 1, 0, 2, 1, 0, 2, 1, 0):
        last[c] -= 1
        seq.append((last[c], c))
    return seq


def moe_kernel(n, r_ref, gate_ref, y_ref, wg_hbm, wu_hbm, wd_hbm, out_ref,
               xbuf, gbuf, cbuf, cpart, inc, wg, wu, wd, act, gcol,
               w_sem, ring_send, ring_recv, gate_send, gate_recv,
               pair_send, pair_recv, pgate_send, pgate_recv,
               sum_send, sum_recv, rs_send, rs_recv):
    me = lax.axis_index("ep")
    chip = me // 2
    core = lax.rem(me, 2)
    other = 1 - core
    half = n // 2
    rows, d = r_ref.shape
    n_local = wg_hbm.shape[0]
    hr = rows // 2
    qr = hr // 2
    ring = [{"ep": 2 * lax.rem(chip + 1, n) + core}, {"ep": 2 * lax.rem(chip + n - 1, n) + core}]
    pair = {"ep": 2 * chip + other}

    def remote(src, dst, ssem, rsem, dev):
        return pltpu.make_async_remote_copy(src_ref=src, dst_ref=dst, send_sem=ssem, recv_sem=rsem, device_id=dev, device_id_type=MESH)

    barrier = pltpu.get_barrier_semaphore()
    for dev in ring + [pair]:
        pl.semaphore_signal(barrier, inc=1, device_id=dev, device_id_type=MESH)
    w_copies = [pltpu.make_async_copy(src, dst, w_sem.at[i]) for i, (src, dst) in enumerate(((wg_hbm, wg), (wu_hbm, wu), (wd_hbm, wd)))]
    for copy in w_copies:
        copy.start()
    pl.semaphore_wait(barrier, 3)

    def ring_copies(direction, v, x_src, g_src):
        return [remote(g_src, gbuf.at[v + 1, direction, core], gate_send.at[direction, v], gate_recv.at[direction, v], ring[direction]),
                remote(x_src, xbuf.at[v + 1, direction, core], ring_send.at[direction, v], ring_recv.at[direction, v], ring[direction])]

    def pair_copies(direction, k, c, x_src, g_src):
        return [remote(g_src, gbuf.at[k, direction, c], pgate_send.at[k, direction], pgate_recv.at[k, direction], pair),
                remote(x_src, xbuf.at[k, direction, c], pair_send.at[k, direction], pair_recv.at[k, direction], pair)]

    def held(direction, k, c):
        return xbuf.at[k, direction, c], gbuf.at[k, direction, c]

    def own(h):
        return r_ref.at[pl.ds(h * hr, hr)], gate_ref.at[h]

    def own_half(direction, v):
        return v if direction == 0 else 1 - v

    for v in range(2):
        for direction in range(2):
            for copy in ring_copies(direction, v, *own(own_half(direction, v))):
                copy.start()
        if v == 0:
            for h in range(2):
                for copy in pair_copies(h, 0, core, *own(h)):
                    copy.start()
    for h in range(2):
        xbuf[0, h, core] = r_ref[h * hr:(h + 1) * hr, :]
        gbuf[0, h, core] = gate_ref[h]

    def sum_copy(k, direction):
        return remote(cbuf.at[k, direction, other], cpart.at[k, direction], sum_send.at[k, direction], sum_recv.at[k, direction], pair)

    order = rs_order(half)

    def quarter(direction, chain):
        return chain if direction == 0 else 3 - chain

    def rs_place(direction, u):
        q, chain = order[u]
        i = quarter(direction, chain)
        step = q if direction == 0 else -q
        step = step - n if step > half else step + n if step <= -half else step
        h = i // 2
        if step == half:
            k, side = n - 1, h
        elif step > 0:
            k, side = 2 * step - h, 1
        else:
            k, side = -2 * step - 1 + h, 0
        return k, side, pl.ds((i % 2) * qr, qr)

    def rs_copy(direction, u):
        q, chain = order[u]
        k, side, at = rs_place(direction, u)
        return remote(cbuf.at[k, side, core, at], inc.at[direction, q - 1, chain], rs_send.at[direction, u], rs_recv.at[direction, u], ring[direction])

    def rs_step(direction, u):
        q, chain = order[u]
        k, side, at = rs_place(direction, u)
        total = cbuf[k, side, core, at, :] + cpart[k, side, at, :]
        if (q + 1, chain) in order:
            rs_copy(direction, order.index((q + 1, chain))).wait_recv()
            total = total + inc[direction, q, chain]
        cbuf[k, side, core, at, :] = total
        rs_copy(direction, u).start()

    low_lanes = lax.broadcasted_iota(jnp.int32, gate_ref.shape[1:], 1) < hr

    def compute(k):
        x = xbuf[k].reshape(2 * rows, d)
        for e in range(n_local):
            for direction in range(2):
                a, b = gbuf[k, direction, 0], gbuf[k, direction, 1]
                mine = (n_local * me + e).astype(F32)
                both = jnp.where(low_lanes, a, pltpu.roll(b, hr, 1))
                ids = jnp.where(low_lanes, pltpu.roll(a, hr, 1), b)
                row = jnp.max(jnp.where(ids == mine, both, -1.0), axis=0, keepdims=True)
                gcol[e, direction * rows:(direction + 1) * rows, :] = jnp.transpose(jnp.broadcast_to(row, (rows, rows)))
        ft = 256
        for e in range(n_local):
            for nt in range(wg.shape[2] // ft):
                cols = slice(nt * ft, (nt + 1) * ft)
                g = jnp.dot(x, wg[e, :, cols], preferred_element_type=F32)
                u = jnp.dot(x, wu[e, :, cols], preferred_element_type=F32)
                act[:, cols] = (jax.nn.silu(g) * u).astype(BF16)
            a = act[...]
            gc = gcol[e]
            chosen = gc >= 0.0
            for nt in range(d // ft):
                f = jnp.dot(a, wd[e, :, nt * ft:(nt + 1) * ft], preferred_element_type=F32).astype(BF16).astype(F32)
                for l in range(ft // rows):
                    cols = slice(nt * ft + l * rows, nt * ft + (l + 1) * rows)
                    term = jnp.where(chosen, f[:, l * rows:(l + 1) * rows] * gc, 0.0).reshape(2, 2, hr, rows)
                    cbuf[k, :, :, :, cols] = term if e == 0 else cbuf[k, :, :, :, cols] + term

    def take(k):
        for direction in range(2):
            x_src, g_src = held(direction, k, core)
            for copy in ring_copies(direction, k - 1, x_src, g_src):
                copy.wait_recv()

            @pl.when(k <= n - 3)
            def _():
                for copy in ring_copies(direction, k + 1, x_src, g_src):
                    copy.start()

            for copy in pair_copies(direction, k, core, x_src, g_src):
                copy.start()

    def body(k, carry):
        @pl.when(k <= n - 4)
        def _():
            take(k + 1)

        @pl.when(k >= n - 2)
        def _():
            take(k)

        @pl.when(k == n - 3)
        def _():
            for side in range(2):
                sum_copy(n - 5, side).wait_recv()
            for direction in range(2):
                rs_step(direction, 0)

        @pl.when(k == n - 2)
        def _():
            for side in range(2):
                sum_copy(n - 3, side).wait_recv()
            for u in range(1, 3):
                for direction in range(2):
                    rs_step(direction, u)

        @pl.when(k == 0)
        def _():
            for copy in w_copies:
                copy.wait()

        for direction in range(2):
            for copy in pair_copies(direction, k, other, *held(direction, k, other)):
                copy.wait_recv()
        compute(k)
        for direction in range(2):
            sum_copy(k, direction).start()
        return carry

    lax.fori_loop(0, n, body, 0)

    summed = {(n - 5, 0), (n - 5, 1), (n - 3, 0), (n - 3, 1)}

    def wait_sum(k, side):
        if (k, side) not in summed:
            sum_copy(k, side).wait_recv()
            summed.add((k, side))

    for u in range(3, len(order)):
        for direction in range(2):
            wait_sum(*rs_place(direction, u)[:2])
            rs_step(direction, u)
    for h in range(2):
        wait_sum(0, h)
    seen = set()
    for u, (q, chain) in enumerate(order):
        for direction in range(2) if q == 1 else ():
            rs_copy(direction, u).wait_recv()
            i = quarter(direction, chain)
            part = pl.ds((i % 2) * qr, qr)
            at = pl.ds(i * qr, qr)
            if i in seen:
                out_ref[at, :] = (cbuf[0, i // 2, core, part, :] + inc[direction, 0, chain]).astype(out_ref.dtype)
            else:
                seen.add(i)
                cbuf[0, i // 2, core, part, :] = y_ref[at, :] + ((cbuf[0, i // 2, core, part, :] + cpart[0, i // 2, part, :]) + inc[direction, 0, chain])

    for direction in range(2):
        for v in range(n - 1):
            src = own(own_half(direction, v)) if v < 2 else held(direction, v - 1, core)
            for copy in ring_copies(direction, v, *src):
                copy.wait_send()
        for k in range(n):
            src = own(direction) if k == 0 else held(direction, k, core)
            for copy in pair_copies(direction, k, core, *src):
                copy.wait_send()
            sum_copy(k, direction).wait_send()
        for u in range(len(order)):
            rs_copy(direction, u).wait_send()


def moe(n_ep, r, gates, y, w_gate, w_up, w_down):
    n = n_ep // 2
    rows, d = r.shape
    n_local, _, ff = w_gate.shape
    vm = pl.BlockSpec(memory_space=pltpu.VMEM)
    hbm = pl.BlockSpec(memory_space=pltpu.HBM)
    dma = pltpu.SemaphoreType.DMA
    n_rs = 2 * (n - 1)
    return pl.pallas_call(
        functools.partial(moe_kernel, n),
        out_shape=jax.ShapeDtypeStruct((rows, d), BF16),
        in_specs=[vm] * 3 + [hbm] * 3,
        out_specs=vm,
        scratch_shapes=[
            pltpu.VMEM((n, 2, 2, rows // 2, d), BF16),
            pltpu.VMEM((n, 2, 2) + gates.shape[1:], F32),
            pltpu.VMEM((n, 2, 2, rows // 2, d), F32),
            pltpu.VMEM((n, 2, rows // 2, d), F32),
            pltpu.VMEM((2, n // 2 + 1, 4, rows // 4, d), F32),
            pltpu.VMEM(w_gate.shape, BF16), pltpu.VMEM(w_up.shape, BF16), pltpu.VMEM(w_down.shape, BF16),
            pltpu.VMEM((2 * rows, ff), BF16),
            pltpu.VMEM((n_local, 2 * rows, rows), F32),
            dma((3,)),
            dma((2, n - 1)), dma((2, n - 1)), dma((2, n - 1)), dma((2, n - 1)),
            dma((n, 2)), dma((n, 2)), dma((n, 2)), dma((n, 2)),
            dma((n, 2)), dma((n, 2)),
            dma((2, n_rs)), dma((2, n_rs)),
        ],
        compiler_params=pltpu.CompilerParams(collective_id=0, has_side_effects=True, vmem_limit_bytes=40 * 1024 * 1024),
        name="moe",
    )(r, gates, y, *in_hbm(w_gate, w_up, w_down))


def solution(mesh):
    n_ep = mesh.shape['ep']
    row_spec = P(('dp', 'ep'), None)
    cache_spec = P(('dp', 'ep'), None, None, None)
    len_spec = P(('dp', 'ep'))
    rep_vec = P(None)
    rep_mat = P(None, None)
    exp_spec = P('ep', None, None)

    def local_step(hidden, k_cache, v_cache, seq_lens, expert_ids, ln_attn, w_q, w_k, w_v, q_gain, k_gain, w_o, ln_moe, w_router, w_gate, w_up, w_down):
        k_t = jnp.transpose(k_cache, (1, 2, 3, 0))
        v_t = jnp.transpose(v_cache, (1, 2, 3, 0))
        k_new, v_new, y, r, gates = attend(
            hidden, k_t, v_t, seq_lens[None, :], expert_ids.T, ln_attn.reshape(-1, 128), w_q, w_k, w_v,
            q_gain[None, :], k_gain[None, :], w_o, ln_moe.reshape(-1, 128), w_router.T)
        out = moe(n_ep, r, gates, y, w_gate, w_up, w_down)
        return out, jnp.transpose(k_new, (3, 0, 1, 2)), jnp.transpose(v_new, (3, 0, 1, 2))

    return jax.shard_map(local_step, mesh=mesh, in_specs=(row_spec, cache_spec, cache_spec, len_spec, row_spec, rep_vec, rep_mat, rep_mat, rep_mat, rep_vec, rep_vec, rep_mat, rep_vec, rep_mat, exp_spec, exp_spec, exp_spec), out_specs=(row_spec, cache_spec, cache_spec), check_vma=False)
```

```python
import functools

import jax
import jax.numpy as jnp
import numpy as np
from jax import lax
from jax.experimental import pallas as pl
from jax.experimental.pallas import tpu as pltpu
from jax.sharding import PartitionSpec as P

EPS = 1e-6
ROPE_BASE = 1000000.0
F32 = jnp.float32
BF16 = jnp.bfloat16
MESH = pl.DeviceIdType.MESH


def in_hbm(*arrays):
    return [pltpu.with_memory_space_constraint(a, pltpu.HBM) for a in arrays]


def attend_kernel(h_hbm, lens_hbm, ids_hbm, ln_a_hbm, qg_hbm, kg_hbm, ln_m_hbm, wr_hbm,
                  wq_hbm, wk_hbm, wv_hbm, wo_hbm, kc_hbm, vc_hbm,
                  kn_hbm, vn_hbm, y_ref, r_ref, gate_ref,
                  h_ref, lens_ref, ids_ref, ln_a_ref, qg_ref, kg_ref, ln_m_ref, wr_ref,
                  kbuf, vbuf, wq, wk, wv, wo, qrot, knew, vnew, score, attn, small_sem, in_sem, out_sem):
    t_max, n_kv, hd, n_seq = kc_hbm.shape
    n_heads = wq_hbm.shape[1] // hd
    grp = n_heads // n_kv
    half = hd // 2
    n_chunk = 4
    tc = t_max // n_chunk

    w_copies = [pltpu.make_async_copy(src, dst, in_sem.at[i])
                for i, (src, dst) in enumerate(((wk_hbm, wk), (wq_hbm, wq), (wv_hbm, wv), (wo_hbm, wo)))]
    k_in = [pltpu.make_async_copy(kc_hbm.at[pl.ds(c * tc, tc)], kbuf.at[pl.ds(c * tc, tc)], in_sem.at[4 + c]) for c in range(n_chunk)]
    v_in = [pltpu.make_async_copy(vc_hbm.at[pl.ds(c * tc, tc)], vbuf.at[pl.ds(c * tc, tc)], in_sem.at[4 + n_chunk + c]) for c in range(n_chunk)]
    k_out = [pltpu.make_async_copy(kbuf.at[pl.ds(c * tc, tc)], kn_hbm.at[pl.ds(c * tc, tc)], out_sem.at[c]) for c in range(n_chunk)]
    v_out = [pltpu.make_async_copy(vbuf.at[pl.ds(c * tc, tc)], vn_hbm.at[pl.ds(c * tc, tc)], out_sem.at[n_chunk + c]) for c in range(n_chunk)]
    small = [pltpu.make_async_copy(src, dst, small_sem.at[i]) for i, (src, dst) in enumerate((
        (h_hbm, h_ref), (lens_hbm, lens_ref), (ids_hbm, ids_ref), (ln_a_hbm, ln_a_ref), (qg_hbm, qg_ref), (kg_hbm, kg_ref), (ln_m_hbm, ln_m_ref), (wr_hbm, wr_ref)))]
    for copy in small + w_copies[:2]:
        copy.start()
    for copy in small:
        copy.wait()
    k_in[0].start()

    def vector(ref):
        rows = ref[...].astype(F32)
        return jnp.concatenate([rows[i:i + 1, :] for i in range(rows.shape[0])], axis=1)

    h32 = h_ref[...].astype(F32)
    mean_sq = jnp.mean(h32 * h32, axis=1, keepdims=True)
    x = (h32 * lax.rsqrt(mean_sq + EPS) * vector(ln_a_ref)).astype(BF16)

    lens = lens_ref[...]
    f_iota = lax.broadcasted_iota(jnp.int32, (half, n_seq), 0)
    inv_freq = np.power(np.float32(ROPE_BASE), -np.arange(0, hd, 2).astype(np.float32) / np.float32(hd))
    freq = jnp.zeros((half, n_seq), F32)
    for i in range(half):
        freq = jnp.where(f_iota == i, float(inv_freq[i]), freq)
    angles = lens.astype(F32) * freq
    cos_v = jnp.cos(angles)
    sin_v = jnp.sin(angles)

    def gain_tile(g_ref):
        row = g_ref[...].astype(F32)
        row = jnp.concatenate([row] * (n_seq // hd), axis=1)
        return jnp.transpose(jnp.broadcast_to(row, (n_seq, n_seq)))[:hd, :]

    def rope_heads(proj, gain, dst, heads):
        for i in range(heads):
            if i % 2 == 0:
                pair = jnp.transpose(proj[:, i * hd:(i + 2) * hd])
            vals = pair[(i % 2) * hd:(i % 2 + 1) * hd, :]
            ms = jnp.mean(vals * vals, axis=0, keepdims=True)
            vals = vals * lax.rsqrt(ms + EPS) * gain
            low, high = vals[:half, :], vals[half:, :]
            dst[i * hd:i * hd + half, :] = (low * cos_v - high * sin_v).astype(BF16).astype(F32)
            dst[i * hd + half:(i + 1) * hd, :] = (high * cos_v + low * sin_v).astype(BF16).astype(F32)

    w_copies[0].wait()
    for copy in k_in[1:] + w_copies[2:3]:
        copy.start()
    rope_heads(jnp.dot(x, wk[...], preferred_element_type=F32), gain_tile(kg_ref), knew, n_kv)
    w_copies[1].wait()
    for copy in v_in + w_copies[3:]:
        copy.start()
    rope_heads(jnp.dot(x, wq[...], preferred_element_type=F32), gain_tile(qg_ref), qrot, n_heads)
    sub = lax.broadcasted_iota(jnp.int32, (8, n_seq), 0)

    def fold(terms):
        top = sub < 4
        pairs = [jnp.where(top, a, b) + pltpu.roll(jnp.where(top, b, a), 4, 0)
                 for a, b in ((terms[0], terms[4]), (terms[2], terms[6]), (terms[1], terms[5]), (terms[3], terms[7]))]
        for shift, keep in ((2, sub % 4 < 2), (1, sub % 2 < 1)):
            pairs = [jnp.where(keep, a, pltpu.roll(b, shift, 0)) + jnp.where(keep, pltpu.roll(a, 8 - shift, 0), b)
                     for a, b in zip(pairs[0::2], pairs[1::2])]
        return pairs[0]

    for c in range(n_chunk):
        k_in[c].wait()

        def k_body(kv, carry, c=c):
            new = knew[pl.ds(pl.multiple_of(kv * hd, hd), hd), :]
            qs = [qrot[pl.ds(pl.multiple_of((kv * grp + g) * hd, hd), hd), :] for g in range(grp)]
            rows = [[] for _ in range(grp)]
            for tt in range(tc):
                t = c * tc + tt
                kt = jnp.where(lens == t, new, kbuf[t, kv].astype(F32))
                kbuf[t, kv] = kt.astype(BF16)
                for g in range(grp):
                    rows[g].append(jnp.sum((kt * qs[g]).reshape(hd // 8, 8, n_seq), axis=0))
            for g in range(grp):
                score[kv * grp + g, c * tc:(c + 1) * tc, :] = fold(rows[g])
            return carry

        lax.fori_loop(0, n_kv, k_body, 0)
        k_out[c].start()

    w_copies[2].wait()
    v_proj = jnp.dot(x, wv[...], preferred_element_type=F32)
    for i in range(0, n_kv, 2):
        vnew[i * hd:(i + 2) * hd, :] = jnp.transpose(v_proj[:, i * hd:(i + 2) * hd]).astype(BF16).astype(F32)

    def v_new_body(kv, carry):
        new = vnew[pl.ds(pl.multiple_of(kv * hd, hd), hd), :]
        for t in range(t_max - tc, t_max):
            vbuf[t, kv] = jnp.where(lens == t, new, vbuf[t, kv].astype(F32)).astype(BF16)
        return carry

    v_in[n_chunk - 1].wait()
    lax.fori_loop(0, n_kv, v_new_body, 0)
    v_out[n_chunk - 1].start()

    visible = lax.broadcasted_iota(jnp.int32, (t_max, n_seq), 0) <= lens

    def soft_body(j, carry):
        s = jnp.where(visible, score[j] * (hd ** -0.5), -1e30)
        e = jnp.exp(s - jnp.max(s, axis=0, keepdims=True))
        score[j] = (e / jnp.sum(e, axis=0, keepdims=True)).astype(BF16).astype(F32)
        return carry

    lax.fori_loop(0, n_heads, soft_body, 0, unroll=2)

    for c in range(n_chunk):
        last = c == n_chunk - 1
        if not last:
            v_in[c].wait()

        def v_body(kv, carry, c=c, last=last):
            new = vnew[pl.ds(pl.multiple_of(kv * hd, hd), hd), :]
            at = [pl.ds(pl.multiple_of((kv * grp + g) * hd, hd), hd) for g in range(grp)]
            acc = [None if c == 0 else attn[at[g], :] for g in range(grp)]
            for tt in range(tc):
                t = c * tc + tt
                vt = vbuf[t, kv].astype(F32)
                if not last:
                    vt = jnp.where(lens == t, new, vt)
                    vbuf[t, kv] = vt.astype(BF16)
                for g in range(grp):
                    term = vt * score[kv * grp + g, t:t + 1, :]
                    acc[g] = term if acc[g] is None else acc[g] + term
            for g in range(grp):
                attn[at[g], :] = acc[g]
            return carry

        lax.fori_loop(0, n_kv, v_body, 0)
        if not last:
            v_out[c].start()

    w_copies[3].wait()
    a_rows = jnp.concatenate([jnp.transpose(attn[i * n_seq:(i + 1) * n_seq, :]).astype(BF16) for i in range(n_heads * hd // n_seq)], axis=1)
    y = h32 + jnp.dot(a_rows, wo[...], preferred_element_type=F32)
    y_ref[...] = y
    mean_sq = jnp.mean(y * y, axis=1, keepdims=True)
    r = (y * lax.rsqrt(mean_sq + EPS) * vector(ln_m_ref)).astype(BF16)
    r_ref[...] = r
    logits = lax.dot_general(wr_ref[...], r, (((1,), (1,)), ((), ())), preferred_element_type=F32)
    e_iota = lax.broadcasted_iota(jnp.int32, logits.shape, 0)
    ids = ids_ref[...]
    chosen = e_iota == ids[0:1, :]
    for i in range(1, ids.shape[0]):
        chosen = chosen | (e_iota == ids[i:i + 1, :])
    top = jnp.max(jnp.where(chosen, logits, -jnp.inf), axis=0, keepdims=True)
    e = jnp.where(chosen, jnp.exp(logits - top), 0.0)
    gates = e / jnp.sum(e, axis=0, keepdims=True)
    picked = jnp.concatenate([jnp.sum(jnp.where(e_iota == ids[i:i + 1, :], gates, 0.0), axis=0, keepdims=True) for i in range(ids.shape[0])], axis=0)
    ids32 = ids.astype(F32)
    low = lax.broadcasted_iota(jnp.int32, ids.shape, 1) < n_seq // 2
    gate_ref[0] = jnp.where(low, picked, pltpu.roll(ids32, n_seq // 2, 1))
    gate_ref[1] = jnp.where(low, pltpu.roll(picked, n_seq // 2, 1), ids32)

    for copy in k_out + v_out:
        copy.wait()


def attend(hidden, k_t, v_t, lens, ids_t, ln_attn, w_q, w_k, w_v, q_gain, k_gain, w_o, ln_moe, w_router_t):
    n_seq, d = hidden.shape
    t_max, n_kv, hd, _ = k_t.shape
    hq, hk = w_q.shape[1], w_k.shape[1]
    n_heads = hq // hd
    vm = pl.BlockSpec(memory_space=pltpu.VMEM)
    hbm = pl.BlockSpec(memory_space=pltpu.HBM)
    small = (hidden, lens, ids_t, ln_attn, q_gain, k_gain, ln_moe, w_router_t)
    return pl.pallas_call(
        attend_kernel,
        out_shape=(
            jax.ShapeDtypeStruct(k_t.shape, k_t.dtype),
            jax.ShapeDtypeStruct(v_t.shape, v_t.dtype),
            jax.ShapeDtypeStruct((n_seq, d), F32),
            jax.ShapeDtypeStruct((n_seq, d), BF16),
            jax.ShapeDtypeStruct((2, ids_t.shape[0], n_seq), F32),
        ),
        in_specs=[hbm] * 14,
        out_specs=(hbm, hbm, vm, vm, vm),
        scratch_shapes=[pltpu.VMEM(a.shape, a.dtype) for a in small] + [
            pltpu.VMEM(k_t.shape, BF16), pltpu.VMEM(v_t.shape, BF16),
            pltpu.VMEM(w_q.shape, BF16), pltpu.VMEM(w_k.shape, BF16), pltpu.VMEM(w_v.shape, BF16), pltpu.VMEM(w_o.shape, BF16),
            pltpu.VMEM((hq, n_seq), F32), pltpu.VMEM((hk, n_seq), F32), pltpu.VMEM((hk, n_seq), F32),
            pltpu.VMEM((n_heads, t_max, n_seq), F32), pltpu.VMEM((hq, n_seq), F32),
            pltpu.SemaphoreType.DMA((len(small),)), pltpu.SemaphoreType.DMA((12,)), pltpu.SemaphoreType.DMA((8,)),
        ],
        compiler_params=pltpu.CompilerParams(vmem_limit_bytes=30 * 1024 * 1024),
        name="attend",
    )(*in_hbm(*small, w_q, w_k, w_v, w_o, k_t, v_t))


def rs_order(half):
    seq = [(half - 2, 3), (half - 1, 2), (half + 1, 0), (half - 3, 3), (half, 1)]
    last = dict((c, q) for q, c in seq)
    for c in (0, 2, 1, 0, 2, 1, 0, 1, 0):
        last[c] -= 1
        seq.append((last[c], c))
    return seq


def moe_kernel(n, r_ref, gate_ref, y_ref, wg_hbm, wu_hbm, wd_hbm, out_ref,
               xbuf, gbuf, cbuf, cpart, inc, wg, wu, wd, act, gcol,
               w_sem, ring_send, ring_recv, gate_send, gate_recv,
               pair_send, pair_recv, pgate_send, pgate_recv,
               sum_send, sum_recv, rs_send, rs_recv):
    me = lax.axis_index("ep")
    chip = me // 2
    core = lax.rem(me, 2)
    other = 1 - core
    half = n // 2
    rows, d = r_ref.shape
    n_local = wg_hbm.shape[0]
    hr = rows // 2
    qr = hr // 2
    ring = [{"ep": 2 * lax.rem(chip + 1, n) + core}, {"ep": 2 * lax.rem(chip + n - 1, n) + core}]
    pair = {"ep": 2 * chip + other}

    def remote(src, dst, ssem, rsem, dev):
        return pltpu.make_async_remote_copy(src_ref=src, dst_ref=dst, send_sem=ssem, recv_sem=rsem, device_id=dev, device_id_type=MESH)

    barrier = pltpu.get_barrier_semaphore()
    for dev in ring + [pair]:
        pl.semaphore_signal(barrier, inc=1, device_id=dev, device_id_type=MESH)
    w_copies = [pltpu.make_async_copy(src, dst, w_sem.at[i]) for i, (src, dst) in enumerate(((wg_hbm, wg), (wu_hbm, wu), (wd_hbm, wd)))]
    for copy in w_copies:
        copy.start()
    pl.semaphore_wait(barrier, 3)

    def ring_copies(direction, v, x_src, g_src):
        return [remote(g_src, gbuf.at[v + 1, direction, core], gate_send.at[direction, v], gate_recv.at[direction, v], ring[direction]),
                remote(x_src, xbuf.at[v + 1, direction, core], ring_send.at[direction, v], ring_recv.at[direction, v], ring[direction])]

    def pair_copies(direction, k, c, x_src, g_src):
        return [remote(g_src, gbuf.at[k, direction, c], pgate_send.at[k, direction], pgate_recv.at[k, direction], pair),
                remote(x_src, xbuf.at[k, direction, c], pair_send.at[k, direction], pair_recv.at[k, direction], pair)]

    def held(direction, k, c):
        return xbuf.at[k, direction, c], gbuf.at[k, direction, c]

    def own(h):
        return r_ref.at[pl.ds(h * hr, hr)], gate_ref.at[h]

    def own_half(direction, v):
        return v if direction == 0 else 1 - v

    for v in range(2):
        for direction in range(2):
            for copy in ring_copies(direction, v, *own(own_half(direction, v))):
                copy.start()
        if v == 0:
            for h in range(2):
                for copy in pair_copies(h, 0, core, *own(h)):
                    copy.start()
    for h in range(2):
        xbuf[0, h, core] = r_ref[h * hr:(h + 1) * hr, :]
        gbuf[0, h, core] = gate_ref[h]

    def sum_copy(k, direction):
        return remote(cbuf.at[k, direction, other], cpart.at[k, direction], sum_send.at[k, direction], sum_recv.at[k, direction], pair)

    order = rs_order(half)

    def quarter(direction, chain):
        return chain if direction == 0 else 3 - chain

    def rs_place(direction, u):
        q, chain = order[u]
        i = quarter(direction, chain)
        step = q if direction == 0 else -q
        step = step - n if step > half else step + n if step <= -half else step
        h = i // 2
        if step == half:
            k, side = n - 1, h
        elif step > 0:
            k, side = 2 * step - h, 1
        else:
            k, side = -2 * step - 1 + h, 0
        return k, side, pl.ds((i % 2) * qr, qr)

    def rs_copy(direction, u):
        q, chain = order[u]
        k, side, at = rs_place(direction, u)
        return remote(cbuf.at[k, side, core, at], inc.at[direction, q - 1, chain], rs_send.at[direction, u], rs_recv.at[direction, u], ring[direction])

    def rs_step(direction, u):
        q, chain = order[u]
        k, side, at = rs_place(direction, u)
        total = cbuf[k, side, core, at, :] + cpart[k, side, at, :]
        if (q + 1, chain) in order:
            rs_copy(direction, order.index((q + 1, chain))).wait_recv()
            total = total + inc[direction, q, chain]
        cbuf[k, side, core, at, :] = total
        rs_copy(direction, u).start()

    low_lanes = lax.broadcasted_iota(jnp.int32, gate_ref.shape[1:], 1) < hr

    def compute(k):
        x = xbuf[k].reshape(2 * rows, d)
        for e in range(n_local):
            for direction in range(2):
                a, b = gbuf[k, direction, 0], gbuf[k, direction, 1]
                mine = (n_local * me + e).astype(F32)
                both = jnp.where(low_lanes, a, pltpu.roll(b, hr, 1))
                ids = jnp.where(low_lanes, pltpu.roll(a, hr, 1), b)
                row = jnp.max(jnp.where(ids == mine, both, -1.0), axis=0, keepdims=True)
                gcol[e, direction * rows:(direction + 1) * rows, :] = jnp.transpose(jnp.broadcast_to(row, (rows, rows)))
        ft = 256
        for e in range(n_local):
            for nt in range(wg.shape[2] // ft):
                cols = slice(nt * ft, (nt + 1) * ft)
                g = jnp.dot(x, wg[e, :, cols], preferred_element_type=F32)
                u = jnp.dot(x, wu[e, :, cols], preferred_element_type=F32)
                act[:, cols] = (jax.nn.silu(g) * u).astype(BF16)
            a = act[...]
            gc = gcol[e]
            chosen = gc >= 0.0
            for nt in range(d // ft):
                f = jnp.dot(a, wd[e, :, nt * ft:(nt + 1) * ft], preferred_element_type=F32).astype(BF16).astype(F32)
                for l in range(ft // rows):
                    cols = slice(nt * ft + l * rows, nt * ft + (l + 1) * rows)
                    term = jnp.where(chosen, f[:, l * rows:(l + 1) * rows] * gc, 0.0).reshape(2, 2, hr, rows)
                    cbuf[k, :, :, :, cols] = term if e == 0 else cbuf[k, :, :, :, cols] + term

    def take(k):
        for direction in range(2):
            x_src, g_src = held(direction, k, core)
            for copy in ring_copies(direction, k - 1, x_src, g_src):
                copy.wait_recv()

            @pl.when(k <= n - 3)
            def _():
                for copy in ring_copies(direction, k + 1, x_src, g_src):
                    copy.start()

            for copy in pair_copies(direction, k, core, x_src, g_src):
                copy.start()

    def body(i, carry):
        k = jnp.where(i < half, i, i + 1 - 2 * lax.rem(i, 2))

        @pl.when(i <= n - 2)
        def _():
            take(i + 1)

        @pl.when(i == 0)
        def _():
            for copy in w_copies:
                copy.wait()

        @pl.when(i == n - 4)
        def _():
            for side in range(2):
                sum_copy(n - 5, side).wait_recv()
            for direction in range(2):
                rs_step(direction, 0)

        @pl.when(i == n - 2)
        def _():
            for side in range(2):
                sum_copy(n - 3, side).wait_recv()
            for u in range(1, 3):
                for direction in range(2):
                    rs_step(direction, u)

        for direction in range(2):
            for copy in pair_copies(direction, k, other, *held(direction, k, other)):
                copy.wait_recv()
        compute(k)
        for direction in range(2):
            sum_copy(k, direction).start()
        return carry

    lax.fori_loop(0, n, body, 0)

    summed = {(n - 5, 0), (n - 5, 1), (n - 3, 0), (n - 3, 1)}

    def wait_sum(k, side):
        if (k, side) not in summed:
            sum_copy(k, side).wait_recv()
            summed.add((k, side))

    for u in range(3, len(order)):
        for direction in range(2):
            wait_sum(*rs_place(direction, u)[:2])
            rs_step(direction, u)
    for h in range(2):
        wait_sum(0, h)
    seen = set()
    for u, (q, chain) in enumerate(order):
        for direction in range(2) if q == 1 else ():
            rs_copy(direction, u).wait_recv()
            i = quarter(direction, chain)
            part = pl.ds((i % 2) * qr, qr)
            at = pl.ds(i * qr, qr)
            if i in seen:
                out_ref[at, :] = (cbuf[0, i // 2, core, part, :] + inc[direction, 0, chain]).astype(out_ref.dtype)
            else:
                seen.add(i)
                cbuf[0, i // 2, core, part, :] = y_ref[at, :] + ((cbuf[0, i // 2, core, part, :] + cpart[0, i // 2, part, :]) + inc[direction, 0, chain])

    for direction in range(2):
        for v in range(n - 1):
            src = own(own_half(direction, v)) if v < 2 else held(direction, v - 1, core)
            for copy in ring_copies(direction, v, *src):
                copy.wait_send()
        for k in range(n):
            src = own(direction) if k == 0 else held(direction, k, core)
            for copy in pair_copies(direction, k, core, *src):
                copy.wait_send()
            sum_copy(k, direction).wait_send()
        for u in range(len(order)):
            rs_copy(direction, u).wait_send()


def moe(n_ep, r, gates, y, w_gate, w_up, w_down):
    n = n_ep // 2
    rows, d = r.shape
    n_local, _, ff = w_gate.shape
    vm = pl.BlockSpec(memory_space=pltpu.VMEM)
    hbm = pl.BlockSpec(memory_space=pltpu.HBM)
    dma = pltpu.SemaphoreType.DMA
    n_rs = 2 * (n - 1)
    return pl.pallas_call(
        functools.partial(moe_kernel, n),
        out_shape=jax.ShapeDtypeStruct((rows, d), BF16),
        in_specs=[vm] * 3 + [hbm] * 3,
        out_specs=vm,
        scratch_shapes=[
            pltpu.VMEM((n, 2, 2, rows // 2, d), BF16),
            pltpu.VMEM((n, 2, 2) + gates.shape[1:], F32),
            pltpu.VMEM((n, 2, 2, rows // 2, d), F32),
            pltpu.VMEM((n, 2, rows // 2, d), F32),
            pltpu.VMEM((2, n // 2 + 1, 4, rows // 4, d), F32),
            pltpu.VMEM(w_gate.shape, BF16), pltpu.VMEM(w_up.shape, BF16), pltpu.VMEM(w_down.shape, BF16),
            pltpu.VMEM((2 * rows, ff), BF16),
            pltpu.VMEM((n_local, 2 * rows, rows), F32),
            dma((3,)),
            dma((2, n - 1)), dma((2, n - 1)), dma((2, n - 1)), dma((2, n - 1)),
            dma((n, 2)), dma((n, 2)), dma((n, 2)), dma((n, 2)),
            dma((n, 2)), dma((n, 2)),
            dma((2, n_rs)), dma((2, n_rs)),
        ],
        compiler_params=pltpu.CompilerParams(collective_id=0, has_side_effects=True, vmem_limit_bytes=40 * 1024 * 1024),
        name="moe",
    )(r, gates, y, *in_hbm(w_gate, w_up, w_down))


def solution(mesh):
    n_ep = mesh.shape['ep']
    row_spec = P(('dp', 'ep'), None)
    cache_spec = P(('dp', 'ep'), None, None, None)
    len_spec = P(('dp', 'ep'))
    rep_vec = P(None)
    rep_mat = P(None, None)
    exp_spec = P('ep', None, None)

    def local_step(hidden, k_cache, v_cache, seq_lens, expert_ids, ln_attn, w_q, w_k, w_v, q_gain, k_gain, w_o, ln_moe, w_router, w_gate, w_up, w_down):
        k_t = jnp.transpose(k_cache, (1, 2, 3, 0))
        v_t = jnp.transpose(v_cache, (1, 2, 3, 0))
        k_new, v_new, y, r, gates = attend(
            hidden, k_t, v_t, seq_lens[None, :], expert_ids.T, ln_attn.reshape(-1, 128), w_q, w_k, w_v,
            q_gain[None, :], k_gain[None, :], w_o, ln_moe.reshape(-1, 128), w_router.T)
        out = moe(n_ep, r, gates, y, w_gate, w_up, w_down)
        return out, jnp.transpose(k_new, (3, 0, 1, 2)), jnp.transpose(v_new, (3, 0, 1, 2))

    return jax.shard_map(local_step, mesh=mesh, in_specs=(row_spec, cache_spec, cache_spec, len_spec, row_spec, rep_vec, rep_mat, rep_mat, rep_mat, rep_vec, rep_vec, rep_mat, rep_vec, rep_mat, exp_spec, exp_spec, exp_spec), out_specs=(row_spec, cache_spec, cache_spec), check_vma=False)
```

```python
import functools

import jax
import jax.numpy as jnp
import numpy as np
from jax import lax
from jax.experimental import pallas as pl
from jax.experimental.pallas import tpu as pltpu
from jax.sharding import PartitionSpec as P

EPS = 1e-6
ROPE_BASE = 1000000.0
F32 = jnp.float32
BF16 = jnp.bfloat16
MESH = pl.DeviceIdType.MESH


def in_hbm(*arrays):
    return [pltpu.with_memory_space_constraint(a, pltpu.HBM) for a in arrays]


def attend_kernel(h_hbm, lens_hbm, ids_hbm, ln_a_hbm, qg_hbm, kg_hbm, ln_m_hbm, wr_hbm,
                  wq_hbm, wk_hbm, wv_hbm, wo_hbm, kc_hbm, vc_hbm,
                  kn_hbm, vn_hbm, y_ref, r_ref, gate_ref,
                  h_ref, lens_ref, ids_ref, ln_a_ref, qg_ref, kg_ref, ln_m_ref, wr_ref,
                  kbuf, vbuf, wq, wk, wv, wo, qrot, knew, vnew, score, attn, small_sem, in_sem, out_sem):
    t_max, n_kv, hd, n_seq = kc_hbm.shape
    n_heads = wq_hbm.shape[1] // hd
    grp = n_heads // n_kv
    half = hd // 2
    n_chunk = 4
    tc = t_max // n_chunk

    w_copies = [pltpu.make_async_copy(src, dst, in_sem.at[i])
                for i, (src, dst) in enumerate(((wk_hbm, wk), (wq_hbm, wq), (wv_hbm, wv), (wo_hbm, wo)))]
    k_in = [pltpu.make_async_copy(kc_hbm.at[pl.ds(c * tc, tc)], kbuf.at[pl.ds(c * tc, tc)], in_sem.at[4 + c]) for c in range(n_chunk)]
    v_in = [pltpu.make_async_copy(vc_hbm.at[pl.ds(c * tc, tc)], vbuf.at[pl.ds(c * tc, tc)], in_sem.at[4 + n_chunk + c]) for c in range(n_chunk)]
    k_out = [pltpu.make_async_copy(kbuf.at[pl.ds(c * tc, tc)], kn_hbm.at[pl.ds(c * tc, tc)], out_sem.at[c]) for c in range(n_chunk)]
    v_out = [pltpu.make_async_copy(vbuf.at[pl.ds(c * tc, tc)], vn_hbm.at[pl.ds(c * tc, tc)], out_sem.at[n_chunk + c]) for c in range(n_chunk)]
    small = [pltpu.make_async_copy(src, dst, small_sem.at[i]) for i, (src, dst) in enumerate((
        (h_hbm, h_ref), (lens_hbm, lens_ref), (ids_hbm, ids_ref), (ln_a_hbm, ln_a_ref), (qg_hbm, qg_ref), (kg_hbm, kg_ref), (ln_m_hbm, ln_m_ref), (wr_hbm, wr_ref)))]
    for copy in small + w_copies[:2] + k_in[:1]:
        copy.start()
    for copy in small:
        copy.wait()
    k_in[1].start()

    def vector(ref):
        rows = ref[...].astype(F32)
        return jnp.concatenate([rows[i:i + 1, :] for i in range(rows.shape[0])], axis=1)

    h32 = h_ref[...].astype(F32)
    mean_sq = jnp.mean(h32 * h32, axis=1, keepdims=True)
    x = (h32 * lax.rsqrt(mean_sq + EPS) * vector(ln_a_ref)).astype(BF16)

    lens = lens_ref[...]
    f_iota = lax.broadcasted_iota(jnp.int32, (half, n_seq), 0)
    inv_freq = np.power(np.float32(ROPE_BASE), -np.arange(0, hd, 2).astype(np.float32) / np.float32(hd))
    freq = jnp.zeros((half, n_seq), F32)
    for i in range(half):
        freq = jnp.where(f_iota == i, float(inv_freq[i]), freq)
    angles = lens.astype(F32) * freq
    cos_v = jnp.cos(angles)
    sin_v = jnp.sin(angles)

    def gain_tile(g_ref):
        row = g_ref[...].astype(F32)
        row = jnp.concatenate([row] * (n_seq // hd), axis=1)
        return jnp.transpose(jnp.broadcast_to(row, (n_seq, n_seq)))[:hd, :]

    def rope_heads(proj, gain, dst, heads):
        for i in range(heads):
            if i % 2 == 0:
                pair = jnp.transpose(proj[:, i * hd:(i + 2) * hd])
            vals = pair[(i % 2) * hd:(i % 2 + 1) * hd, :]
            ms = jnp.mean(vals * vals, axis=0, keepdims=True)
            vals = vals * lax.rsqrt(ms + EPS) * gain
            low, high = vals[:half, :], vals[half:, :]
            dst[i * hd:i * hd + half, :] = (low * cos_v - high * sin_v).astype(BF16).astype(F32)
            dst[i * hd + half:(i + 1) * hd, :] = (high * cos_v + low * sin_v).astype(BF16).astype(F32)

    w_copies[0].wait()
    for copy in k_in[2:]:
        copy.start()
    rope_heads(jnp.dot(x, wk[...], preferred_element_type=F32), gain_tile(kg_ref), knew, n_kv)
    w_copies[1].wait()
    for copy in w_copies[2:3] + v_in[:1]:
        copy.start()
    rope_heads(jnp.dot(x, wq[...], preferred_element_type=F32), gain_tile(qg_ref), qrot, n_heads)
    sub = lax.broadcasted_iota(jnp.int32, (8, n_seq), 0)

    def fold(terms):
        top = sub < 4
        pairs = [jnp.where(top, a, b) + pltpu.roll(jnp.where(top, b, a), 4, 0)
                 for a, b in ((terms[0], terms[4]), (terms[2], terms[6]), (terms[1], terms[5]), (terms[3], terms[7]))]
        for shift, keep in ((2, sub % 4 < 2), (1, sub % 2 < 1)):
            pairs = [jnp.where(keep, a, pltpu.roll(b, shift, 0)) + jnp.where(keep, pltpu.roll(a, 8 - shift, 0), b)
                     for a, b in zip(pairs[0::2], pairs[1::2])]
        return pairs[0]

    for c in range(n_chunk):
        k_in[c].wait()
        (v_in[1:] + w_copies[3:])[c].start()

        def k_body(kv, carry, c=c):
            new = knew[pl.ds(pl.multiple_of(kv * hd, hd), hd), :]
            qs = [qrot[pl.ds(pl.multiple_of((kv * grp + g) * hd, hd), hd), :] for g in range(grp)]
            rows = [[] for _ in range(grp)]
            for tt in range(tc):
                t = c * tc + tt
                kt = jnp.where(lens == t, new, kbuf[t, kv].astype(F32))
                kbuf[t, kv] = kt.astype(BF16)
                for g in range(grp):
                    rows[g].append(jnp.sum((kt * qs[g]).reshape(hd // 8, 8, n_seq), axis=0))
            for g in range(grp):
                score[kv * grp + g, c * tc:(c + 1) * tc, :] = fold(rows[g])
            return carry

        lax.fori_loop(0, n_kv, k_body, 0)
        k_out[c].start()

    w_copies[2].wait()
    v_proj = jnp.dot(x, wv[...], preferred_element_type=F32)
    for i in range(0, n_kv, 2):
        vnew[i * hd:(i + 2) * hd, :] = jnp.transpose(v_proj[:, i * hd:(i + 2) * hd]).astype(BF16).astype(F32)

    visible = lax.broadcasted_iota(jnp.int32, (t_max, n_seq), 0) <= lens

    def soft_body(j, carry):
        s = jnp.where(visible, score[j] * (hd ** -0.5), -1e30)
        e = jnp.exp(s - jnp.max(s, axis=0, keepdims=True))
        score[j] = (e / jnp.sum(e, axis=0, keepdims=True)).astype(BF16).astype(F32)
        return carry

    lax.fori_loop(0, n_heads, soft_body, 0, unroll=2)

    for c in range(n_chunk):
        v_in[c].wait()

        def v_body(kv, carry, c=c):
            new = vnew[pl.ds(pl.multiple_of(kv * hd, hd), hd), :]
            at = [pl.ds(pl.multiple_of((kv * grp + g) * hd, hd), hd) for g in range(grp)]
            acc = [None if c == 0 else attn[at[g], :] for g in range(grp)]
            for tt in range(tc):
                t = c * tc + tt
                vt = jnp.where(lens == t, new, vbuf[t, kv].astype(F32))
                vbuf[t, kv] = vt.astype(BF16)
                for g in range(grp):
                    term = vt * score[kv * grp + g, t:t + 1, :]
                    acc[g] = term if acc[g] is None else acc[g] + term
            for g in range(grp):
                attn[at[g], :] = acc[g]
            return carry

        lax.fori_loop(0, n_kv, v_body, 0)
        v_out[c].start()

    w_copies[3].wait()
    a_rows = jnp.concatenate([jnp.transpose(attn[i * n_seq:(i + 1) * n_seq, :]).astype(BF16) for i in range(n_heads * hd // n_seq)], axis=1)
    y = h32 + jnp.dot(a_rows, wo[...], preferred_element_type=F32)
    y_ref[...] = y
    mean_sq = jnp.mean(y * y, axis=1, keepdims=True)
    r = (y * lax.rsqrt(mean_sq + EPS) * vector(ln_m_ref)).astype(BF16)
    r_ref[...] = r
    logits = lax.dot_general(wr_ref[...], r, (((1,), (1,)), ((), ())), preferred_element_type=F32)
    e_iota = lax.broadcasted_iota(jnp.int32, logits.shape, 0)
    ids = ids_ref[...]
    chosen = e_iota == ids[0:1, :]
    for i in range(1, ids.shape[0]):
        chosen = chosen | (e_iota == ids[i:i + 1, :])
    top = jnp.max(jnp.where(chosen, logits, -jnp.inf), axis=0, keepdims=True)
    e = jnp.where(chosen, jnp.exp(logits - top), 0.0)
    gates = e / jnp.sum(e, axis=0, keepdims=True)
    picked = jnp.concatenate([jnp.sum(jnp.where(e_iota == ids[i:i + 1, :], gates, 0.0), axis=0, keepdims=True) for i in range(ids.shape[0])], axis=0)
    ids32 = ids.astype(F32)
    low = lax.broadcasted_iota(jnp.int32, ids.shape, 1) < n_seq // 2
    gate_ref[0] = jnp.where(low, picked, pltpu.roll(ids32, n_seq // 2, 1))
    gate_ref[1] = jnp.where(low, pltpu.roll(picked, n_seq // 2, 1), ids32)

    for copy in k_out + v_out:
        copy.wait()


def attend(hidden, k_t, v_t, lens, ids_t, ln_attn, w_q, w_k, w_v, q_gain, k_gain, w_o, ln_moe, w_router_t):
    n_seq, d = hidden.shape
    t_max, n_kv, hd, _ = k_t.shape
    hq, hk = w_q.shape[1], w_k.shape[1]
    n_heads = hq // hd
    vm = pl.BlockSpec(memory_space=pltpu.VMEM)
    hbm = pl.BlockSpec(memory_space=pltpu.HBM)
    small = (hidden, lens, ids_t, ln_attn, q_gain, k_gain, ln_moe, w_router_t)
    return pl.pallas_call(
        attend_kernel,
        out_shape=(
            jax.ShapeDtypeStruct(k_t.shape, k_t.dtype),
            jax.ShapeDtypeStruct(v_t.shape, v_t.dtype),
            jax.ShapeDtypeStruct((n_seq, d), F32),
            jax.ShapeDtypeStruct((n_seq, d), BF16),
            jax.ShapeDtypeStruct((2, ids_t.shape[0], n_seq), F32),
        ),
        in_specs=[hbm] * 14,
        out_specs=(hbm, hbm, vm, vm, vm),
        scratch_shapes=[pltpu.VMEM(a.shape, a.dtype) for a in small] + [
            pltpu.VMEM(k_t.shape, BF16), pltpu.VMEM(v_t.shape, BF16),
            pltpu.VMEM(w_q.shape, BF16), pltpu.VMEM(w_k.shape, BF16), pltpu.VMEM(w_v.shape, BF16), pltpu.VMEM(w_o.shape, BF16),
            pltpu.VMEM((hq, n_seq), F32), pltpu.VMEM((hk, n_seq), F32), pltpu.VMEM((hk, n_seq), F32),
            pltpu.VMEM((n_heads, t_max, n_seq), F32), pltpu.VMEM((hq, n_seq), F32),
            pltpu.SemaphoreType.DMA((len(small),)), pltpu.SemaphoreType.DMA((12,)), pltpu.SemaphoreType.DMA((8,)),
        ],
        compiler_params=pltpu.CompilerParams(vmem_limit_bytes=30 * 1024 * 1024),
        name="attend",
    )(*in_hbm(*small, w_q, w_k, w_v, w_o, k_t, v_t))


def rs_order(half):
    seq = [(half - 2, 3), (half - 1, 2), (half + 1, 0), (half - 3, 3), (half, 1)]
    last = dict((c, q) for q, c in seq)
    for c in (0, 2, 1, 0, 2, 1, 0, 1, 0):
        last[c] -= 1
        seq.append((last[c], c))
    return seq


def moe_kernel(n, r_ref, gate_ref, y_ref, wg_hbm, wu_hbm, wd_hbm, out_ref,
               xbuf, gbuf, cbuf, cpart, inc, wg, wu, wd, act, gcol,
               w_sem, ring_send, ring_recv, gate_send, gate_recv,
               pair_send, pair_recv, pgate_send, pgate_recv,
               sum_send, sum_recv, rs_send, rs_recv):
    me = lax.axis_index("ep")
    chip = me // 2
    core = lax.rem(me, 2)
    other = 1 - core
    half = n // 2
    rows, d = r_ref.shape
    n_local = wg_hbm.shape[0]
    hr = rows // 2
    qr = hr // 2
    ring = [{"ep": 2 * lax.rem(chip + 1, n) + core}, {"ep": 2 * lax.rem(chip + n - 1, n) + core}]
    pair = {"ep": 2 * chip + other}

    def remote(src, dst, ssem, rsem, dev):
        return pltpu.make_async_remote_copy(src_ref=src, dst_ref=dst, send_sem=ssem, recv_sem=rsem, device_id=dev, device_id_type=MESH)

    barrier = pltpu.get_barrier_semaphore()
    for dev in ring + [pair]:
        pl.semaphore_signal(barrier, inc=1, device_id=dev, device_id_type=MESH)
    w_copies = [pltpu.make_async_copy(src, dst, w_sem.at[i]) for i, (src, dst) in enumerate(((wg_hbm, wg), (wu_hbm, wu), (wd_hbm, wd)))]
    for copy in w_copies:
        copy.start()
    pl.semaphore_wait(barrier, 3)

    def ring_copies(direction, v, x_src, g_src):
        return [remote(g_src, gbuf.at[v + 1, direction, core], gate_send.at[direction, v], gate_recv.at[direction, v], ring[direction]),
                remote(x_src, xbuf.at[v + 1, direction, core], ring_send.at[direction, v], ring_recv.at[direction, v], ring[direction])]

    def pair_copies(direction, k, c, x_src, g_src):
        return [remote(g_src, gbuf.at[k, direction, c], pgate_send.at[k, direction], pgate_recv.at[k, direction], pair),
                remote(x_src, xbuf.at[k, direction, c], pair_send.at[k, direction], pair_recv.at[k, direction], pair)]

    def held(direction, k, c):
        return xbuf.at[k, direction, c], gbuf.at[k, direction, c]

    def own(h):
        return r_ref.at[pl.ds(h * hr, hr)], gate_ref.at[h]

    def own_half(direction, v):
        return v if direction == 0 else 1 - v

    for v in range(2):
        for direction in range(2):
            for copy in ring_copies(direction, v, *own(own_half(direction, v))):
                copy.start()
        if v == 0:
            for h in range(2):
                for copy in pair_copies(h, 0, core, *own(h)):
                    copy.start()
    for h in range(2):
        xbuf[0, h, core] = r_ref[h * hr:(h + 1) * hr, :]
        gbuf[0, h, core] = gate_ref[h]

    def sum_copy(k, direction):
        return remote(cbuf.at[k, direction, other], cpart.at[k, direction], sum_send.at[k, direction], sum_recv.at[k, direction], pair)

    order = rs_order(half)

    def quarter(direction, chain):
        return chain if direction == 0 else 3 - chain

    def rs_place(direction, u):
        q, chain = order[u]
        i = quarter(direction, chain)
        step = q if direction == 0 else -q
        step = step - n if step > half else step + n if step <= -half else step
        h = i // 2
        if step == half:
            k, side = n - 1, h
        elif step > 0:
            k, side = 2 * step - h, 1
        else:
            k, side = -2 * step - 1 + h, 0
        return k, side, pl.ds((i % 2) * qr, qr)

    def rs_copy(direction, u):
        q, chain = order[u]
        k, side, at = rs_place(direction, u)
        return remote(cbuf.at[k, side, core, at], inc.at[direction, q - 1, chain], rs_send.at[direction, u], rs_recv.at[direction, u], ring[direction])

    def rs_step(direction, u):
        q, chain = order[u]
        k, side, at = rs_place(direction, u)
        total = cbuf[k, side, core, at, :] + cpart[k, side, at, :]
        if (q + 1, chain) in order:
            rs_copy(direction, order.index((q + 1, chain))).wait_recv()
            total = total + inc[direction, q, chain]
        cbuf[k, side, core, at, :] = total
        rs_copy(direction, u).start()

    low_lanes = lax.broadcasted_iota(jnp.int32, gate_ref.shape[1:], 1) < hr

    def compute(k):
        x = xbuf[k].reshape(2 * rows, d)
        for e in range(n_local):
            for direction in range(2):
                a, b = gbuf[k, direction, 0], gbuf[k, direction, 1]
                mine = (n_local * me + e).astype(F32)
                both = jnp.where(low_lanes, a, pltpu.roll(b, hr, 1))
                ids = jnp.where(low_lanes, pltpu.roll(a, hr, 1), b)
                row = jnp.max(jnp.where(ids == mine, both, -1.0), axis=0, keepdims=True)
                gcol[e, direction * rows:(direction + 1) * rows, :] = jnp.transpose(jnp.broadcast_to(row, (rows, rows)))
        ft = 256
        for e in range(n_local):
            for nt in range(wg.shape[2] // ft):
                cols = slice(nt * ft, (nt + 1) * ft)
                g = jnp.dot(x, wg[e, :, cols], preferred_element_type=F32)
                u = jnp.dot(x, wu[e, :, cols], preferred_element_type=F32)
                act[:, cols] = (jax.nn.silu(g) * u).astype(BF16)
            a = act[...]
            gc = gcol[e]
            chosen = gc >= 0.0
            for nt in range(d // ft):
                f = jnp.dot(a, wd[e, :, nt * ft:(nt + 1) * ft], preferred_element_type=F32).astype(BF16).astype(F32)
                for l in range(ft // rows):
                    cols = slice(nt * ft + l * rows, nt * ft + (l + 1) * rows)
                    term = jnp.where(chosen, f[:, l * rows:(l + 1) * rows] * gc, 0.0).reshape(2, 2, hr, rows)
                    cbuf[k, :, :, :, cols] = term if e == 0 else cbuf[k, :, :, :, cols] + term

    def take(k):
        for direction in range(2):
            x_src, g_src = held(direction, k, core)
            for copy in ring_copies(direction, k - 1, x_src, g_src):
                copy.wait_recv()

            @pl.when(k <= n - 3)
            def _():
                for copy in ring_copies(direction, k + 1, x_src, g_src):
                    copy.start()

            for copy in pair_copies(direction, k, core, x_src, g_src):
                copy.start()

    def body(i, carry):
        k = jnp.where(i < half, i, i + 1 - 2 * lax.rem(i, 2))

        @pl.when(i <= n - 2)
        def _():
            take(i + 1)

        @pl.when(i == 0)
        def _():
            for copy in w_copies:
                copy.wait()

        @pl.when(i == n - 4)
        def _():
            for side in range(2):
                sum_copy(n - 5, side).wait_recv()
            for direction in range(2):
                rs_step(direction, 0)

        @pl.when(i == n - 2)
        def _():
            for side in range(2):
                sum_copy(n - 3, side).wait_recv()
            for u in range(1, 3):
                for direction in range(2):
                    rs_step(direction, u)

        for direction in range(2):
            for copy in pair_copies(direction, k, other, *held(direction, k, other)):
                copy.wait_recv()
        compute(k)
        for direction in range(2):
            sum_copy(k, direction).start()
        return carry

    lax.fori_loop(0, n, body, 0)

    summed = {(n - 5, 0), (n - 5, 1), (n - 3, 0), (n - 3, 1)}

    def wait_sum(k, side):
        if (k, side) not in summed:
            sum_copy(k, side).wait_recv()
            summed.add((k, side))

    for u in range(3, len(order)):
        for direction in range(2):
            wait_sum(*rs_place(direction, u)[:2])
            rs_step(direction, u)
    for h in range(2):
        wait_sum(0, h)
    seen = set()
    for u, (q, chain) in enumerate(order):
        for direction in range(2) if q == 1 else ():
            rs_copy(direction, u).wait_recv()
            i = quarter(direction, chain)
            part = pl.ds((i % 2) * qr, qr)
            at = pl.ds(i * qr, qr)
            if i in seen:
                out_ref[at, :] = (cbuf[0, i // 2, core, part, :] + inc[direction, 0, chain]).astype(out_ref.dtype)
            else:
                seen.add(i)
                cbuf[0, i // 2, core, part, :] = y_ref[at, :] + ((cbuf[0, i // 2, core, part, :] + cpart[0, i // 2, part, :]) + inc[direction, 0, chain])

    for direction in range(2):
        for v in range(n - 1):
            src = own(own_half(direction, v)) if v < 2 else held(direction, v - 1, core)
            for copy in ring_copies(direction, v, *src):
                copy.wait_send()
        for k in range(n):
            src = own(direction) if k == 0 else held(direction, k, core)
            for copy in pair_copies(direction, k, core, *src):
                copy.wait_send()
            sum_copy(k, direction).wait_send()
        for u in range(len(order)):
            rs_copy(direction, u).wait_send()


def moe(n_ep, r, gates, y, w_gate, w_up, w_down):
    n = n_ep // 2
    rows, d = r.shape
    n_local, _, ff = w_gate.shape
    vm = pl.BlockSpec(memory_space=pltpu.VMEM)
    hbm = pl.BlockSpec(memory_space=pltpu.HBM)
    dma = pltpu.SemaphoreType.DMA
    n_rs = 2 * (n - 1)
    return pl.pallas_call(
        functools.partial(moe_kernel, n),
        out_shape=jax.ShapeDtypeStruct((rows, d), BF16),
        in_specs=[vm] * 3 + [hbm] * 3,
        out_specs=vm,
        scratch_shapes=[
            pltpu.VMEM((n, 2, 2, rows // 2, d), BF16),
            pltpu.VMEM((n, 2, 2) + gates.shape[1:], F32),
            pltpu.VMEM((n, 2, 2, rows // 2, d), F32),
            pltpu.VMEM((n, 2, rows // 2, d), F32),
            pltpu.VMEM((2, n // 2 + 1, 4, rows // 4, d), F32),
            pltpu.VMEM(w_gate.shape, BF16), pltpu.VMEM(w_up.shape, BF16), pltpu.VMEM(w_down.shape, BF16),
            pltpu.VMEM((2 * rows, ff), BF16),
            pltpu.VMEM((n_local, 2 * rows, rows), F32),
            dma((3,)),
            dma((2, n - 1)), dma((2, n - 1)), dma((2, n - 1)), dma((2, n - 1)),
            dma((n, 2)), dma((n, 2)), dma((n, 2)), dma((n, 2)),
            dma((n, 2)), dma((n, 2)),
            dma((2, n_rs)), dma((2, n_rs)),
        ],
        compiler_params=pltpu.CompilerParams(collective_id=0, has_side_effects=True, vmem_limit_bytes=40 * 1024 * 1024),
        name="moe",
    )(r, gates, y, *in_hbm(w_gate, w_up, w_down))


def solution(mesh):
    n_ep = mesh.shape['ep']
    row_spec = P(('dp', 'ep'), None)
    cache_spec = P(('dp', 'ep'), None, None, None)
    len_spec = P(('dp', 'ep'))
    rep_vec = P(None)
    rep_mat = P(None, None)
    exp_spec = P('ep', None, None)

    def local_step(hidden, k_cache, v_cache, seq_lens, expert_ids, ln_attn, w_q, w_k, w_v, q_gain, k_gain, w_o, ln_moe, w_router, w_gate, w_up, w_down):
        k_t = jnp.transpose(k_cache, (1, 2, 3, 0))
        v_t = jnp.transpose(v_cache, (1, 2, 3, 0))
        k_new, v_new, y, r, gates = attend(
            hidden, k_t, v_t, seq_lens[None, :], expert_ids.T, ln_attn.reshape(-1, 128), w_q, w_k, w_v,
            q_gain[None, :], k_gain[None, :], w_o, ln_moe.reshape(-1, 128), w_router.T)
        out = moe(n_ep, r, gates, y, w_gate, w_up, w_down)
        return out, jnp.transpose(k_new, (3, 0, 1, 2)), jnp.transpose(v_new, (3, 0, 1, 2))

    return jax.shard_map(local_step, mesh=mesh, in_specs=(row_spec, cache_spec, cache_spec, len_spec, row_spec, rep_vec, rep_mat, rep_mat, rep_mat, rep_vec, rep_vec, rep_mat, rep_vec, rep_mat, exp_spec, exp_spec, exp_spec), out_specs=(row_spec, cache_spec, cache_spec), check_vma=False)
```

```python
import functools

import jax
import jax.numpy as jnp
import numpy as np
from jax import lax
from jax.experimental import pallas as pl
from jax.experimental.pallas import tpu as pltpu
from jax.sharding import PartitionSpec as P

EPS = 1e-6
ROPE_BASE = 1000000.0
F32 = jnp.float32
BF16 = jnp.bfloat16
MESH = pl.DeviceIdType.MESH


def in_hbm(*arrays):
    return [pltpu.with_memory_space_constraint(a, pltpu.HBM) for a in arrays]


def attend_kernel(h_hbm, lens_hbm, ids_hbm, ln_a_hbm, qg_hbm, kg_hbm, ln_m_hbm, wr_hbm,
                  wq_hbm, wk_hbm, wv_hbm, wo_hbm, kc_hbm, vc_hbm,
                  kn_hbm, vn_hbm, y_ref, r_ref, gate_ref,
                  h_ref, lens_ref, ids_ref, ln_a_ref, qg_ref, kg_ref, ln_m_ref, wr_ref,
                  kbuf, vbuf, wq, wk, wv, wo, qrot, knew, vnew, score, attn, small_sem, in_sem, out_sem):
    t_max, n_kv, hd, n_seq = kc_hbm.shape
    n_heads = wq_hbm.shape[1] // hd
    grp = n_heads // n_kv
    half = hd // 2
    n_chunk = 4
    tc = t_max // n_chunk

    w_copies = [pltpu.make_async_copy(src, dst, in_sem.at[i])
                for i, (src, dst) in enumerate(((wk_hbm, wk), (wq_hbm, wq), (wv_hbm, wv), (wo_hbm, wo)))]
    k_in = [pltpu.make_async_copy(kc_hbm.at[pl.ds(c * tc, tc)], kbuf.at[pl.ds(c * tc, tc)], in_sem.at[4 + c]) for c in range(n_chunk)]
    v_in = [pltpu.make_async_copy(vc_hbm.at[pl.ds(c * tc, tc)], vbuf.at[pl.ds(c * tc, tc)], in_sem.at[4 + n_chunk + c]) for c in range(n_chunk)]
    k_out = [pltpu.make_async_copy(kbuf.at[pl.ds(c * tc, tc)], kn_hbm.at[pl.ds(c * tc, tc)], out_sem.at[c]) for c in range(n_chunk)]
    v_out = [pltpu.make_async_copy(vbuf.at[pl.ds(c * tc, tc)], vn_hbm.at[pl.ds(c * tc, tc)], out_sem.at[n_chunk + c]) for c in range(n_chunk)]
    small = [pltpu.make_async_copy(src, dst, small_sem.at[i]) for i, (src, dst) in enumerate((
        (h_hbm, h_ref), (lens_hbm, lens_ref), (ids_hbm, ids_ref), (ln_a_hbm, ln_a_ref), (qg_hbm, qg_ref), (kg_hbm, kg_ref), (ln_m_hbm, ln_m_ref), (wr_hbm, wr_ref)))]
    for copy in small + w_copies[:2]:
        copy.start()
    for copy in small:
        copy.wait()
    for copy in k_in:
        copy.start()

    def vector(ref):
        rows = ref[...].astype(F32)
        return jnp.concatenate([rows[i:i + 1, :] for i in range(rows.shape[0])], axis=1)

    h32 = h_ref[...].astype(F32)
    mean_sq = jnp.mean(h32 * h32, axis=1, keepdims=True)
    x = (h32 * lax.rsqrt(mean_sq + EPS) * vector(ln_a_ref)).astype(BF16)

    lens = lens_ref[...]
    f_iota = lax.broadcasted_iota(jnp.int32, (half, n_seq), 0)
    inv_freq = np.power(np.float32(ROPE_BASE), -np.arange(0, hd, 2).astype(np.float32) / np.float32(hd))
    freq = jnp.zeros((half, n_seq), F32)
    for i in range(half):
        freq = jnp.where(f_iota == i, float(inv_freq[i]), freq)
    angles = lens.astype(F32) * freq
    cos_v = jnp.cos(angles)
    sin_v = jnp.sin(angles)

    def gain_tile(g_ref):
        row = g_ref[...].astype(F32)
        row = jnp.concatenate([row] * (n_seq // hd), axis=1)
        return jnp.transpose(jnp.broadcast_to(row, (n_seq, n_seq)))[:hd, :]

    def rope_heads(proj, gain, dst, heads):
        for i in range(heads):
            if i % 2 == 0:
                pair = jnp.transpose(proj[:, i * hd:(i + 2) * hd])
            vals = pair[(i % 2) * hd:(i % 2 + 1) * hd, :]
            ms = jnp.mean(vals * vals, axis=0, keepdims=True)
            vals = vals * lax.rsqrt(ms + EPS) * gain
            low, high = vals[:half, :], vals[half:, :]
            dst[i * hd:i * hd + half, :] = (low * cos_v - high * sin_v).astype(BF16).astype(F32)
            dst[i * hd + half:(i + 1) * hd, :] = (high * cos_v + low * sin_v).astype(BF16).astype(F32)

    w_copies[0].wait()
    for copy in w_copies[2:3] + v_in + w_copies[3:]:
        copy.start()
    rope_heads(jnp.dot(x, wk[...], preferred_element_type=F32), gain_tile(kg_ref), knew, n_kv)
    w_copies[1].wait()
    rope_heads(jnp.dot(x, wq[...], preferred_element_type=F32), gain_tile(qg_ref), qrot, n_heads)
    sub = lax.broadcasted_iota(jnp.int32, (8, n_seq), 0)

    def fold(terms):
        top = sub < 4
        pairs = [jnp.where(top, a, b) + pltpu.roll(jnp.where(top, b, a), 4, 0)
                 for a, b in ((terms[0], terms[4]), (terms[2], terms[6]), (terms[1], terms[5]), (terms[3], terms[7]))]
        for shift, keep in ((2, sub % 4 < 2), (1, sub % 2 < 1)):
            pairs = [jnp.where(keep, a, pltpu.roll(b, shift, 0)) + jnp.where(keep, pltpu.roll(a, 8 - shift, 0), b)
                     for a, b in zip(pairs[0::2], pairs[1::2])]
        return pairs[0]

    for c in range(n_chunk):
        k_in[c].wait()

        def k_body(kv, carry, c=c):
            new = knew[pl.ds(pl.multiple_of(kv * hd, hd), hd), :]
            qs = [qrot[pl.ds(pl.multiple_of((kv * grp + g) * hd, hd), hd), :] for g in range(grp)]
            rows = [[] for _ in range(grp)]
            for tt in range(tc):
                t = c * tc + tt
                kt = jnp.where(lens == t, new, kbuf[t, kv].astype(F32))
                kbuf[t, kv] = kt.astype(BF16)
                for g in range(grp):
                    rows[g].append(jnp.sum((kt * qs[g]).reshape(hd // 8, 8, n_seq), axis=0))
            for g in range(grp):
                score[kv * grp + g, c * tc:(c + 1) * tc, :] = fold(rows[g])
            return carry

        lax.fori_loop(0, n_kv, k_body, 0)
        k_out[c].start()

    w_copies[2].wait()
    v_proj = jnp.dot(x, wv[...], preferred_element_type=F32)
    for i in range(0, n_kv, 2):
        vnew[i * hd:(i + 2) * hd, :] = jnp.transpose(v_proj[:, i * hd:(i + 2) * hd]).astype(BF16).astype(F32)

    visible = lax.broadcasted_iota(jnp.int32, (t_max, n_seq), 0) <= lens

    def soft_body(j, carry):
        s = jnp.where(visible, score[j] * (hd ** -0.5), -1e30)
        e = jnp.exp(s - jnp.max(s, axis=0, keepdims=True))
        score[j] = (e / jnp.sum(e, axis=0, keepdims=True)).astype(BF16).astype(F32)
        return carry

    lax.fori_loop(0, n_heads, soft_body, 0, unroll=2)

    for c in range(n_chunk):
        v_in[c].wait()

        def v_body(kv, carry, c=c):
            new = vnew[pl.ds(pl.multiple_of(kv * hd, hd), hd), :]
            at = [pl.ds(pl.multiple_of((kv * grp + g) * hd, hd), hd) for g in range(grp)]
            acc = [None if c == 0 else attn[at[g], :] for g in range(grp)]
            for tt in range(tc):
                t = c * tc + tt
                vt = jnp.where(lens == t, new, vbuf[t, kv].astype(F32))
                vbuf[t, kv] = vt.astype(BF16)
                for g in range(grp):
                    term = vt * score[kv * grp + g, t:t + 1, :]
                    acc[g] = term if acc[g] is None else acc[g] + term
            for g in range(grp):
                attn[at[g], :] = acc[g]
            return carry

        lax.fori_loop(0, n_kv, v_body, 0)
        v_out[c].start()

    w_copies[3].wait()
    a_rows = jnp.concatenate([jnp.transpose(attn[i * n_seq:(i + 1) * n_seq, :]).astype(BF16) for i in range(n_heads * hd // n_seq)], axis=1)
    y = h32 + jnp.dot(a_rows, wo[...], preferred_element_type=F32)
    y_ref[...] = y
    mean_sq = jnp.mean(y * y, axis=1, keepdims=True)
    r = (y * lax.rsqrt(mean_sq + EPS) * vector(ln_m_ref)).astype(BF16)
    r_ref[...] = r
    logits = lax.dot_general(wr_ref[...], r, (((1,), (1,)), ((), ())), preferred_element_type=F32)
    e_iota = lax.broadcasted_iota(jnp.int32, logits.shape, 0)
    ids = ids_ref[...]
    chosen = e_iota == ids[0:1, :]
    for i in range(1, ids.shape[0]):
        chosen = chosen | (e_iota == ids[i:i + 1, :])
    top = jnp.max(jnp.where(chosen, logits, -jnp.inf), axis=0, keepdims=True)
    e = jnp.where(chosen, jnp.exp(logits - top), 0.0)
    gates = e / jnp.sum(e, axis=0, keepdims=True)
    picked = jnp.concatenate([jnp.sum(jnp.where(e_iota == ids[i:i + 1, :], gates, 0.0), axis=0, keepdims=True) for i in range(ids.shape[0])], axis=0)
    ids32 = ids.astype(F32)
    low = lax.broadcasted_iota(jnp.int32, ids.shape, 1) < n_seq // 2
    gate_ref[0] = jnp.where(low, picked, pltpu.roll(ids32, n_seq // 2, 1))
    gate_ref[1] = jnp.where(low, pltpu.roll(picked, n_seq // 2, 1), ids32)

    for copy in k_out + v_out:
        copy.wait()


def attend(hidden, k_t, v_t, lens, ids_t, ln_attn, w_q, w_k, w_v, q_gain, k_gain, w_o, ln_moe, w_router_t):
    n_seq, d = hidden.shape
    t_max, n_kv, hd, _ = k_t.shape
    hq, hk = w_q.shape[1], w_k.shape[1]
    n_heads = hq // hd
    vm = pl.BlockSpec(memory_space=pltpu.VMEM)
    hbm = pl.BlockSpec(memory_space=pltpu.HBM)
    small = (hidden, lens, ids_t, ln_attn, q_gain, k_gain, ln_moe, w_router_t)
    return pl.pallas_call(
        attend_kernel,
        out_shape=(
            jax.ShapeDtypeStruct(k_t.shape, k_t.dtype),
            jax.ShapeDtypeStruct(v_t.shape, v_t.dtype),
            jax.ShapeDtypeStruct((n_seq, d), F32),
            jax.ShapeDtypeStruct((n_seq, d), BF16),
            jax.ShapeDtypeStruct((2, ids_t.shape[0], n_seq), F32),
        ),
        in_specs=[hbm] * 14,
        out_specs=(hbm, hbm, vm, vm, vm),
        scratch_shapes=[pltpu.VMEM(a.shape, a.dtype) for a in small] + [
            pltpu.VMEM(k_t.shape, BF16), pltpu.VMEM(v_t.shape, BF16),
            pltpu.VMEM(w_q.shape, BF16), pltpu.VMEM(w_k.shape, BF16), pltpu.VMEM(w_v.shape, BF16), pltpu.VMEM(w_o.shape, BF16),
            pltpu.VMEM((hq, n_seq), F32), pltpu.VMEM((hk, n_seq), F32), pltpu.VMEM((hk, n_seq), F32),
            pltpu.VMEM((n_heads, t_max, n_seq), F32), pltpu.VMEM((hq, n_seq), F32),
            pltpu.SemaphoreType.DMA((len(small),)), pltpu.SemaphoreType.DMA((12,)), pltpu.SemaphoreType.DMA((8,)),
        ],
        compiler_params=pltpu.CompilerParams(vmem_limit_bytes=30 * 1024 * 1024),
        name="attend",
    )(*in_hbm(*small, w_q, w_k, w_v, w_o, k_t, v_t))


def rs_order(half):
    seq = [(half - 2, 3), (half + 1, 0), (half - 1, 2), (half, 1)]
    last = dict((c, q) for q, c in seq)
    for c in (0, 3, 1, 0, 2, 1, 0, 2, 1, 0):
        last[c] -= 1
        seq.append((last[c], c))
    return seq


def moe_kernel(n, r_ref, gate_ref, y_ref, wg_hbm, wu_hbm, wd_hbm, out_ref,
               xbuf, gbuf, cbuf, cpart, inc, wg, wu, wd, act, gcol,
               w_sem, ring_send, ring_recv, gate_send, gate_recv,
               pair_send, pair_recv, pgate_send, pgate_recv,
               sum_send, sum_recv, rs_send, rs_recv):
    me = lax.axis_index("ep")
    chip = me // 2
    core = lax.rem(me, 2)
    other = 1 - core
    half = n // 2
    rows, d = r_ref.shape
    n_local = wg_hbm.shape[0]
    hr = rows // 2
    qr = hr // 2
    ring = [{"ep": 2 * lax.rem(chip + 1, n) + core}, {"ep": 2 * lax.rem(chip + n - 1, n) + core}]
    pair = {"ep": 2 * chip + other}

    def remote(src, dst, ssem, rsem, dev):
        return pltpu.make_async_remote_copy(src_ref=src, dst_ref=dst, send_sem=ssem, recv_sem=rsem, device_id=dev, device_id_type=MESH)

    barrier = pltpu.get_barrier_semaphore()
    for dev in ring + [pair]:
        pl.semaphore_signal(barrier, inc=1, device_id=dev, device_id_type=MESH)
    w_copies = [pltpu.make_async_copy(src, dst, w_sem.at[i]) for i, (src, dst) in enumerate(((wg_hbm, wg), (wu_hbm, wu), (wd_hbm, wd)))]
    for copy in w_copies:
        copy.start()
    pl.semaphore_wait(barrier, 3)

    def ring_copies(direction, v, x_src, g_src):
        return [remote(g_src, gbuf.at[v + 1, direction, core], gate_send.at[direction, v], gate_recv.at[direction, v], ring[direction]),
                remote(x_src, xbuf.at[v + 1, direction, core], ring_send.at[direction, v], ring_recv.at[direction, v], ring[direction])]

    def pair_copies(direction, k, c, x_src, g_src):
        return [remote(g_src, gbuf.at[k, direction, c], pgate_send.at[k, direction], pgate_recv.at[k, direction], pair),
                remote(x_src, xbuf.at[k, direction, c], pair_send.at[k, direction], pair_recv.at[k, direction], pair)]

    def held(direction, k, c):
        return xbuf.at[k, direction, c], gbuf.at[k, direction, c]

    def own(h):
        return r_ref.at[pl.ds(h * hr, hr)], gate_ref.at[h]

    def own_half(direction, v):
        return v if direction == 0 else 1 - v

    for v in range(2):
        for direction in range(2):
            for copy in ring_copies(direction, v, *own(own_half(direction, v))):
                copy.start()
        if v == 0:
            for h in range(2):
                for copy in pair_copies(h, 0, core, *own(h)):
                    copy.start()
    for h in range(2):
        xbuf[0, h, core] = r_ref[h * hr:(h + 1) * hr, :]
        gbuf[0, h, core] = gate_ref[h]

    def sum_copy(k, direction):
        return remote(cbuf.at[k, direction, other], cpart.at[k, direction], sum_send.at[k, direction], sum_recv.at[k, direction], pair)

    order = rs_order(half)

    def quarter(direction, chain):
        return chain if direction == 0 else 3 - chain

    def rs_place(direction, u):
        q, chain = order[u]
        i = quarter(direction, chain)
        step = q if direction == 0 else -q
        step = step - n if step > half else step + n if step <= -half else step
        h = i // 2
        if step == half:
            k, side = n - 1, h
        elif step > 0:
            k, side = 2 * step - h, 1
        else:
            k, side = -2 * step - 1 + h, 0
        return k, side, pl.ds((i % 2) * qr, qr)

    def rs_copy(direction, u):
        q, chain = order[u]
        k, side, at = rs_place(direction, u)
        return remote(cbuf.at[k, side, core, at], inc.at[direction, q - 1, chain], rs_send.at[direction, u], rs_recv.at[direction, u], ring[direction])

    def rs_step(direction, u):
        q, chain = order[u]
        k, side, at = rs_place(direction, u)
        total = cbuf[k, side, core, at, :] + cpart[k, side, at, :]
        if (q + 1, chain) in order:
            rs_copy(direction, order.index((q + 1, chain))).wait_recv()
            total = total + inc[direction, q, chain]
        cbuf[k, side, core, at, :] = total
        rs_copy(direction, u).start()

    low_lanes = lax.broadcasted_iota(jnp.int32, gate_ref.shape[1:], 1) < hr

    def compute(k):
        x = xbuf[k].reshape(2 * rows, d)
        for e in range(n_local):
            for direction in range(2):
                a, b = gbuf[k, direction, 0], gbuf[k, direction, 1]
                mine = (n_local * me + e).astype(F32)
                both = jnp.where(low_lanes, a, pltpu.roll(b, hr, 1))
                ids = jnp.where(low_lanes, pltpu.roll(a, hr, 1), b)
                row = jnp.max(jnp.where(ids == mine, both, -1.0), axis=0, keepdims=True)
                gcol[e, direction * rows:(direction + 1) * rows, :] = jnp.transpose(jnp.broadcast_to(row, (rows, rows)))
        ft = 256
        for e in range(n_local):
            for nt in range(wg.shape[2] // ft):
                cols = slice(nt * ft, (nt + 1) * ft)
                g = jnp.dot(x, wg[e, :, cols], preferred_element_type=F32)
                u = jnp.dot(x, wu[e, :, cols], preferred_element_type=F32)
                act[:, cols] = (jax.nn.silu(g) * u).astype(BF16)
            a = act[...]
            gc = gcol[e]
            chosen = gc >= 0.0
            for nt in range(d // ft):
                f = jnp.dot(a, wd[e, :, nt * ft:(nt + 1) * ft], preferred_element_type=F32).astype(BF16).astype(F32)
                for l in range(ft // rows):
                    cols = slice(nt * ft + l * rows, nt * ft + (l + 1) * rows)
                    term = jnp.where(chosen, f[:, l * rows:(l + 1) * rows] * gc, 0.0).reshape(2, 2, hr, rows)
                    cbuf[k, :, :, :, cols] = term if e == 0 else cbuf[k, :, :, :, cols] + term

    def take(k):
        for direction in range(2):
            x_src, g_src = held(direction, k, core)
            for copy in ring_copies(direction, k - 1, x_src, g_src):
                copy.wait_recv()

            @pl.when(k <= n - 3)
            def _():
                for copy in ring_copies(direction, k + 1, x_src, g_src):
                    copy.start()

            for copy in pair_copies(direction, k, core, x_src, g_src):
                copy.start()

    def body(i, carry):
        k = jnp.where(i < half, i, i + 1 - 2 * lax.rem(i, 2))

        @pl.when(i <= n - 2)
        def _():
            take(i + 1)

        @pl.when(i == 0)
        def _():
            for copy in w_copies:
                copy.wait()

        @pl.when(i == n - 4)
        def _():
            for side in range(2):
                sum_copy(n - 5, side).wait_recv()
            for direction in range(2):
                rs_step(direction, 0)

        @pl.when(i == n - 2)
        def _():
            for side in range(2):
                sum_copy(n - 3, side).wait_recv()
            for u in range(1, 3):
                for direction in range(2):
                    rs_step(direction, u)

        for direction in range(2):
            for copy in pair_copies(direction, k, other, *held(direction, k, other)):
                copy.wait_recv()
        compute(k)
        for direction in range(2):
            sum_copy(k, direction).start()
        return carry

    lax.fori_loop(0, n, body, 0)

    summed = {(n - 5, 0), (n - 5, 1), (n - 3, 0), (n - 3, 1)}

    def wait_sum(k, side):
        if (k, side) not in summed:
            sum_copy(k, side).wait_recv()
            summed.add((k, side))

    for u in range(3, len(order)):
        for direction in range(2):
            wait_sum(*rs_place(direction, u)[:2])
            rs_step(direction, u)
    for h in range(2):
        wait_sum(0, h)
    seen = set()
    for u, (q, chain) in enumerate(order):
        for direction in range(2) if q == 1 else ():
            rs_copy(direction, u).wait_recv()
            i = quarter(direction, chain)
            part = pl.ds((i % 2) * qr, qr)
            at = pl.ds(i * qr, qr)
            if i in seen:
                out_ref[at, :] = (cbuf[0, i // 2, core, part, :] + inc[direction, 0, chain]).astype(out_ref.dtype)
            else:
                seen.add(i)
                cbuf[0, i // 2, core, part, :] = y_ref[at, :] + ((cbuf[0, i // 2, core, part, :] + cpart[0, i // 2, part, :]) + inc[direction, 0, chain])

    for direction in range(2):
        for v in range(n - 1):
            src = own(own_half(direction, v)) if v < 2 else held(direction, v - 1, core)
            for copy in ring_copies(direction, v, *src):
                copy.wait_send()
        for k in range(n):
            src = own(direction) if k == 0 else held(direction, k, core)
            for copy in pair_copies(direction, k, core, *src):
                copy.wait_send()
            sum_copy(k, direction).wait_send()
        for u in range(len(order)):
            rs_copy(direction, u).wait_send()


def moe(n_ep, r, gates, y, w_gate, w_up, w_down):
    n = n_ep // 2
    rows, d = r.shape
    n_local, _, ff = w_gate.shape
    vm = pl.BlockSpec(memory_space=pltpu.VMEM)
    hbm = pl.BlockSpec(memory_space=pltpu.HBM)
    dma = pltpu.SemaphoreType.DMA
    n_rs = 2 * (n - 1)
    return pl.pallas_call(
        functools.partial(moe_kernel, n),
        out_shape=jax.ShapeDtypeStruct((rows, d), BF16),
        in_specs=[vm] * 3 + [hbm] * 3,
        out_specs=vm,
        scratch_shapes=[
            pltpu.VMEM((n, 2, 2, rows // 2, d), BF16),
            pltpu.VMEM((n, 2, 2) + gates.shape[1:], F32),
            pltpu.VMEM((n, 2, 2, rows // 2, d), F32),
            pltpu.VMEM((n, 2, rows // 2, d), F32),
            pltpu.VMEM((2, n // 2 + 1, 4, rows // 4, d), F32),
            pltpu.VMEM(w_gate.shape, BF16), pltpu.VMEM(w_up.shape, BF16), pltpu.VMEM(w_down.shape, BF16),
            pltpu.VMEM((2 * rows, ff), BF16),
            pltpu.VMEM((n_local, 2 * rows, rows), F32),
            dma((3,)),
            dma((2, n - 1)), dma((2, n - 1)), dma((2, n - 1)), dma((2, n - 1)),
            dma((n, 2)), dma((n, 2)), dma((n, 2)), dma((n, 2)),
            dma((n, 2)), dma((n, 2)),
            dma((2, n_rs)), dma((2, n_rs)),
        ],
        compiler_params=pltpu.CompilerParams(collective_id=0, has_side_effects=True, vmem_limit_bytes=40 * 1024 * 1024),
        name="moe",
    )(r, gates, y, *in_hbm(w_gate, w_up, w_down))


def solution(mesh):
    n_ep = mesh.shape['ep']
    row_spec = P(('dp', 'ep'), None)
    cache_spec = P(('dp', 'ep'), None, None, None)
    len_spec = P(('dp', 'ep'))
    rep_vec = P(None)
    rep_mat = P(None, None)
    exp_spec = P('ep', None, None)

    def local_step(hidden, k_cache, v_cache, seq_lens, expert_ids, ln_attn, w_q, w_k, w_v, q_gain, k_gain, w_o, ln_moe, w_router, w_gate, w_up, w_down):
        k_t = jnp.transpose(k_cache, (1, 2, 3, 0))
        v_t = jnp.transpose(v_cache, (1, 2, 3, 0))
        k_new, v_new, y, r, gates = attend(
            hidden, k_t, v_t, seq_lens[None, :], expert_ids.T, ln_attn.reshape(-1, 128), w_q, w_k, w_v,
            q_gain[None, :], k_gain[None, :], w_o, ln_moe.reshape(-1, 128), w_router.T)
        out = moe(n_ep, r, gates, y, w_gate, w_up, w_down)
        return out, jnp.transpose(k_new, (3, 0, 1, 2)), jnp.transpose(v_new, (3, 0, 1, 2))

    return jax.shard_map(local_step, mesh=mesh, in_specs=(row_spec, cache_spec, cache_spec, len_spec, row_spec, rep_vec, rep_mat, rep_mat, rep_mat, rep_vec, rep_vec, rep_mat, rep_vec, rep_mat, exp_spec, exp_spec, exp_spec), out_specs=(row_spec, cache_spec, cache_spec), check_vma=False)
```

```python
import functools

import jax
import jax.numpy as jnp
import numpy as np
from jax import lax
from jax.experimental import pallas as pl
from jax.experimental.pallas import tpu as pltpu
from jax.sharding import PartitionSpec as P

EPS = 1e-6
ROPE_BASE = 1000000.0
F32 = jnp.float32
BF16 = jnp.bfloat16
MESH = pl.DeviceIdType.MESH


def in_hbm(*arrays):
    return [pltpu.with_memory_space_constraint(a, pltpu.HBM) for a in arrays]


def attend_kernel(h_hbm, lens_hbm, ids_hbm, ln_a_hbm, qg_hbm, kg_hbm, ln_m_hbm, wr_hbm,
                  wq_hbm, wk_hbm, wv_hbm, wo_hbm, kc_hbm, vc_hbm,
                  kn_hbm, vn_hbm, y_ref, r_ref, gate_ref,
                  h_ref, lens_ref, ids_ref, ln_a_ref, qg_ref, kg_ref, ln_m_ref, wr_ref,
                  kbuf, vbuf, wq, wk, wv, wo, qrot, knew, vnew, score, attn, small_sem, piece_sem, in_sem, out_sem):
    t_max, n_kv, hd, n_seq = kc_hbm.shape
    n_heads = wq_hbm.shape[1] // hd
    grp = n_heads // n_kv
    half = hd // 2
    n_chunk = 4
    tc = t_max // n_chunk

    w_copies = [pltpu.make_async_copy(src, dst, in_sem.at[i]) for i, (src, dst) in enumerate(((wv_hbm, wv), (wo_hbm, wo)))]
    piece = 8 * hd
    k_pieces, q_pieces = [[(pltpu.make_async_copy(src.at[:, pl.ds(i * piece, piece)], dst.at[:, pl.ds(i * piece, piece)], piece_sem.at[first + i]), i)
                           for i in range(src.shape[1] // piece)] for src, dst, first in ((wk_hbm, wk, 0), (wq_hbm, wq, n_heads // 8))]
    k_in = [pltpu.make_async_copy(kc_hbm.at[pl.ds(c * tc, tc)], kbuf.at[pl.ds(c * tc, tc)], in_sem.at[4 + c]) for c in range(n_chunk)]
    v_in = [pltpu.make_async_copy(vc_hbm.at[pl.ds(c * tc, tc)], vbuf.at[pl.ds(c * tc, tc)], in_sem.at[4 + n_chunk + c]) for c in range(n_chunk)]
    k_out = [pltpu.make_async_copy(kbuf.at[pl.ds(c * tc, tc)], kn_hbm.at[pl.ds(c * tc, tc)], out_sem.at[c]) for c in range(n_chunk)]
    v_out = [pltpu.make_async_copy(vbuf.at[pl.ds(c * tc, tc)], vn_hbm.at[pl.ds(c * tc, tc)], out_sem.at[n_chunk + c]) for c in range(n_chunk)]
    small = [pltpu.make_async_copy(src, dst, small_sem.at[i]) for i, (src, dst) in enumerate((
        (h_hbm, h_ref), (lens_hbm, lens_ref), (ids_hbm, ids_ref), (ln_a_hbm, ln_a_ref), (qg_hbm, qg_ref), (kg_hbm, kg_ref), (ln_m_hbm, ln_m_ref), (wr_hbm, wr_ref)))]
    for copy in small + [c for c, _ in k_pieces + q_pieces]:
        copy.start()
    for copy in small:
        copy.wait()
    for copy in k_in:
        copy.start()

    def vector(ref):
        rows = ref[...].astype(F32)
        return jnp.concatenate([rows[i:i + 1, :] for i in range(rows.shape[0])], axis=1)

    h32 = h_ref[...].astype(F32)
    mean_sq = jnp.mean(h32 * h32, axis=1, keepdims=True)
    x = (h32 * lax.rsqrt(mean_sq + EPS) * vector(ln_a_ref)).astype(BF16)

    lens = lens_ref[...]
    f_iota = lax.broadcasted_iota(jnp.int32, (half, n_seq), 0)
    inv_freq = np.power(np.float32(ROPE_BASE), -np.arange(0, hd, 2).astype(np.float32) / np.float32(hd))
    freq = jnp.zeros((half, n_seq), F32)
    for i in range(half):
        freq = jnp.where(f_iota == i, float(inv_freq[i]), freq)
    angles = lens.astype(F32) * freq
    cos_v = jnp.cos(angles)
    sin_v = jnp.sin(angles)

    def gain_tile(g_ref):
        row = g_ref[...].astype(F32)
        row = jnp.concatenate([row] * (n_seq // hd), axis=1)
        return jnp.transpose(jnp.broadcast_to(row, (n_seq, n_seq)))[:hd, :]

    def rope_heads(proj, gain, dst, first):
        for i in range(0, proj.shape[1] // hd, 2):
            pair = jnp.transpose(proj[:, i * hd:(i + 2) * hd])
            for j in range(2):
                vals = pair[j * hd:(j + 1) * hd, :]
                ms = jnp.mean(vals * vals, axis=0, keepdims=True)
                vals = vals * lax.rsqrt(ms + EPS) * gain
                low, high = vals[:half, :], vals[half:, :]
                at = first + (i + j) * hd
                dst[at:at + half, :] = (low * cos_v - high * sin_v).astype(BF16).astype(F32)
                dst[at + half:at + hd, :] = (high * cos_v + low * sin_v).astype(BF16).astype(F32)

    k_gain, q_gain = gain_tile(kg_ref), gain_tile(qg_ref)
    held = None
    for pieces, w, gain, dst in ((k_pieces, wk, k_gain, knew), (q_pieces, wq, q_gain, qrot)):
        for copy, i in pieces:
            copy.wait()
            if held is None:
                for other in w_copies[:1] + v_in + w_copies[1:]:
                    other.start()
            proj = jnp.dot(x, w[:, i * piece:(i + 1) * piece], preferred_element_type=F32)
            if held is not None:
                rope_heads(*held)
            held = proj, gain, dst, i * piece
    rope_heads(*held)

    sub = lax.broadcasted_iota(jnp.int32, (8, n_seq), 0)

    def fold(terms):
        top = sub < 4
        pairs = [jnp.where(top, a, b) + pltpu.roll(jnp.where(top, b, a), 4, 0)
                 for a, b in ((terms[0], terms[4]), (terms[2], terms[6]), (terms[1], terms[5]), (terms[3], terms[7]))]
        for shift, keep in ((2, sub % 4 < 2), (1, sub % 2 < 1)):
            pairs = [jnp.where(keep, a, pltpu.roll(b, shift, 0)) + jnp.where(keep, pltpu.roll(a, 8 - shift, 0), b)
                     for a, b in zip(pairs[0::2], pairs[1::2])]
        return pairs[0]

    for c in range(n_chunk):
        k_in[c].wait()

        def k_body(kv, carry, c=c):
            new = knew[pl.ds(pl.multiple_of(kv * hd, hd), hd), :]
            qs = [qrot[pl.ds(pl.multiple_of((kv * grp + g) * hd, hd), hd), :] for g in range(grp)]
            rows = [[] for _ in range(grp)]
            for tt in range(tc):
                t = c * tc + tt
                kt = jnp.where(lens == t, new, kbuf[t, kv].astype(F32))
                kbuf[t, kv] = kt.astype(BF16)
                for g in range(grp):
                    rows[g].append(jnp.sum((kt * qs[g]).reshape(hd // 8, 8, n_seq), axis=0))
            for g in range(grp):
                score[kv * grp + g, c * tc:(c + 1) * tc, :] = fold(rows[g])
            return carry

        lax.fori_loop(0, n_kv, k_body, 0)
        k_out[c].start()

    w_copies[0].wait()
    v_proj = jnp.dot(x, wv[...], preferred_element_type=F32)
    for i in range(0, n_kv, 2):
        vnew[i * hd:(i + 2) * hd, :] = jnp.transpose(v_proj[:, i * hd:(i + 2) * hd]).astype(BF16).astype(F32)

    visible = lax.broadcasted_iota(jnp.int32, (t_max, n_seq), 0) <= lens

    def soft_body(j, carry):
        s = jnp.where(visible, score[j] * (hd ** -0.5), -1e30)
        e = jnp.exp(s - jnp.max(s, axis=0, keepdims=True))
        score[j] = (e / jnp.sum(e, axis=0, keepdims=True)).astype(BF16).astype(F32)
        return carry

    lax.fori_loop(0, n_heads, soft_body, 0, unroll=2)

    for c in range(n_chunk):
        v_in[c].wait()

        def v_body(kv, carry, c=c):
            new = vnew[pl.ds(pl.multiple_of(kv * hd, hd), hd), :]
            at = [pl.ds(pl.multiple_of((kv * grp + g) * hd, hd), hd) for g in range(grp)]
            acc = [None if c == 0 else attn[at[g], :] for g in range(grp)]
            for tt in range(tc):
                t = c * tc + tt
                vt = jnp.where(lens == t, new, vbuf[t, kv].astype(F32))
                vbuf[t, kv] = vt.astype(BF16)
                for g in range(grp):
                    term = vt * score[kv * grp + g, t:t + 1, :]
                    acc[g] = term if acc[g] is None else acc[g] + term
            for g in range(grp):
                attn[at[g], :] = acc[g]
            if c == n_chunk - 1:
                head = pl.ds(c * tc, tc), pl.ds(kv, 1)
                pltpu.make_async_copy(vbuf.at[head], vn_hbm.at[head], out_sem.at[n_chunk + c]).start()
            return carry

        lax.fori_loop(0, n_kv, v_body, 0)
        if c < n_chunk - 1:
            v_out[c].start()

    w_copies[1].wait()
    a_rows = jnp.concatenate([jnp.transpose(attn[i * n_seq:(i + 1) * n_seq, :]).astype(BF16) for i in range(n_heads * hd // n_seq)], axis=1)
    y = h32 + jnp.dot(a_rows, wo[...], preferred_element_type=F32)
    y_ref[...] = y
    mean_sq = jnp.mean(y * y, axis=1, keepdims=True)
    r = (y * lax.rsqrt(mean_sq + EPS) * vector(ln_m_ref)).astype(BF16)
    r_ref[...] = r
    logits = lax.dot_general(wr_ref[...], r, (((1,), (1,)), ((), ())), preferred_element_type=F32)
    e_iota = lax.broadcasted_iota(jnp.int32, logits.shape, 0)
    ids = ids_ref[...]
    chosen = e_iota == ids[0:1, :]
    for i in range(1, ids.shape[0]):
        chosen = chosen | (e_iota == ids[i:i + 1, :])
    top = jnp.max(jnp.where(chosen, logits, -jnp.inf), axis=0, keepdims=True)
    e = jnp.where(chosen, jnp.exp(logits - top), 0.0)
    gates = e / jnp.sum(e, axis=0, keepdims=True)
    picked = jnp.concatenate([jnp.sum(jnp.where(e_iota == ids[i:i + 1, :], gates, 0.0), axis=0, keepdims=True) for i in range(ids.shape[0])], axis=0)
    ids32 = ids.astype(F32)
    low = lax.broadcasted_iota(jnp.int32, ids.shape, 1) < n_seq // 2
    gate_ref[0] = jnp.where(low, picked, pltpu.roll(ids32, n_seq // 2, 1))
    gate_ref[1] = jnp.where(low, pltpu.roll(picked, n_seq // 2, 1), ids32)

    for copy in k_out + v_out:
        copy.wait()


def attend(hidden, k_t, v_t, lens, ids_t, ln_attn, w_q, w_k, w_v, q_gain, k_gain, w_o, ln_moe, w_router_t):
    n_seq, d = hidden.shape
    t_max, n_kv, hd, _ = k_t.shape
    hq, hk = w_q.shape[1], w_k.shape[1]
    n_heads = hq // hd
    vm = pl.BlockSpec(memory_space=pltpu.VMEM)
    hbm = pl.BlockSpec(memory_space=pltpu.HBM)
    small = (hidden, lens, ids_t, ln_attn, q_gain, k_gain, ln_moe, w_router_t)
    return pl.pallas_call(
        attend_kernel,
        out_shape=(
            jax.ShapeDtypeStruct(k_t.shape, k_t.dtype),
            jax.ShapeDtypeStruct(v_t.shape, v_t.dtype),
            jax.ShapeDtypeStruct((n_seq, d), F32),
            jax.ShapeDtypeStruct((n_seq, d), BF16),
            jax.ShapeDtypeStruct((2, ids_t.shape[0], n_seq), F32),
        ),
        in_specs=[hbm] * 14,
        out_specs=(hbm, hbm, vm, vm, vm),
        scratch_shapes=[pltpu.VMEM(a.shape, a.dtype) for a in small] + [
            pltpu.VMEM(k_t.shape, BF16), pltpu.VMEM(v_t.shape, BF16),
            pltpu.VMEM(w_q.shape, BF16), pltpu.VMEM(w_k.shape, BF16), pltpu.VMEM(w_v.shape, BF16), pltpu.VMEM(w_o.shape, BF16),
            pltpu.VMEM((hq, n_seq), F32), pltpu.VMEM((hk, n_seq), F32), pltpu.VMEM((hk, n_seq), F32),
            pltpu.VMEM((n_heads, t_max, n_seq), F32), pltpu.VMEM((hq, n_seq), F32),
            pltpu.SemaphoreType.DMA((len(small),)), pltpu.SemaphoreType.DMA((2 * n_heads // 8,)), pltpu.SemaphoreType.DMA((12,)), pltpu.SemaphoreType.DMA((8,)),
        ],
        compiler_params=pltpu.CompilerParams(vmem_limit_bytes=30 * 1024 * 1024),
        name="attend",
    )(*in_hbm(*small, w_q, w_k, w_v, w_o, k_t, v_t))


def rs_order(half):
    seq = [(half - 2, 3), (half + 1, 0), (half - 1, 2), (half, 1)]
    last = dict((c, q) for q, c in seq)
    for c in (0, 3, 1, 0, 2, 1, 0, 2, 1, 0):
        last[c] -= 1
        seq.append((last[c], c))
    return seq


def moe_kernel(n, r_ref, gate_ref, y_ref, wg_hbm, wu_hbm, wd_hbm, out_ref,
               xbuf, gbuf, cbuf, cpart, inc, wg, wu, wd, act, gcol,
               w_sem, ring_send, ring_recv, gate_send, gate_recv,
               pair_send, pair_recv, pgate_send, pgate_recv,
               sum_send, sum_recv, rs_send, rs_recv):
    me = lax.axis_index("ep")
    chip = me // 2
    core = lax.rem(me, 2)
    other = 1 - core
    half = n // 2
    rows, d = r_ref.shape
    n_local = wg_hbm.shape[0]
    hr = rows // 2
    qr = hr // 2
    ring = [{"ep": 2 * lax.rem(chip + 1, n) + core}, {"ep": 2 * lax.rem(chip + n - 1, n) + core}]
    pair = {"ep": 2 * chip + other}

    def remote(src, dst, ssem, rsem, dev):
        return pltpu.make_async_remote_copy(src_ref=src, dst_ref=dst, send_sem=ssem, recv_sem=rsem, device_id=dev, device_id_type=MESH)

    barrier = pltpu.get_barrier_semaphore()
    for dev in ring + [pair]:
        pl.semaphore_signal(barrier, inc=1, device_id=dev, device_id_type=MESH)
    w_copies = [pltpu.make_async_copy(src, dst, w_sem.at[i]) for i, (src, dst) in enumerate(((wg_hbm, wg), (wu_hbm, wu), (wd_hbm, wd)))]
    for copy in w_copies:
        copy.start()
    pl.semaphore_wait(barrier, 3)

    def ring_copies(direction, v, x_src, g_src):
        return [remote(g_src, gbuf.at[v + 1, direction, core], gate_send.at[direction, v], gate_recv.at[direction, v], ring[direction]),
                remote(x_src, xbuf.at[v + 1, direction, core], ring_send.at[direction, v], ring_recv.at[direction, v], ring[direction])]

    def pair_copies(direction, k, c, x_src, g_src):
        return [remote(g_src, gbuf.at[k, direction, c], pgate_send.at[k, direction], pgate_recv.at[k, direction], pair),
                remote(x_src, xbuf.at[k, direction, c], pair_send.at[k, direction], pair_recv.at[k, direction], pair)]

    def held(direction, k, c):
        return xbuf.at[k, direction, c], gbuf.at[k, direction, c]

    def own(h):
        return r_ref.at[pl.ds(h * hr, hr)], gate_ref.at[h]

    def own_half(direction, v):
        return v if direction == 0 else 1 - v

    for v in range(2):
        for direction in range(2):
            for copy in ring_copies(direction, v, *own(own_half(direction, v))):
                copy.start()
        if v == 0:
            for h in range(2):
                for copy in pair_copies(h, 0, core, *own(h)):
                    copy.start()
    for h in range(2):
        xbuf[0, h, core] = r_ref[h * hr:(h + 1) * hr, :]
        gbuf[0, h, core] = gate_ref[h]

    def sum_copy(k, direction):
        return remote(cbuf.at[k, direction, other], cpart.at[k, direction], sum_send.at[k, direction], sum_recv.at[k, direction], pair)

    order = rs_order(half)

    def quarter(direction, chain):
        return chain if direction == 0 else 3 - chain

    def rs_place(direction, u):
        q, chain = order[u]
        i = quarter(direction, chain)
        step = q if direction == 0 else -q
        step = step - n if step > half else step + n if step <= -half else step
        h = i // 2
        if step == half:
            k, side = n - 1, h
        elif step > 0:
            k, side = 2 * step - h, 1
        else:
            k, side = -2 * step - 1 + h, 0
        return k, side, pl.ds((i % 2) * qr, qr)

    def rs_copy(direction, u):
        q, chain = order[u]
        k, side, at = rs_place(direction, u)
        return remote(cbuf.at[k, side, core, at], inc.at[direction, q - 1, chain], rs_send.at[direction, u], rs_recv.at[direction, u], ring[direction])

    def rs_step(direction, u):
        q, chain = order[u]
        k, side, at = rs_place(direction, u)
        total = cbuf[k, side, core, at, :] + cpart[k, side, at, :]
        if (q + 1, chain) in order:
            rs_copy(direction, order.index((q + 1, chain))).wait_recv()
            total = total + inc[direction, q, chain]
        cbuf[k, side, core, at, :] = total
        rs_copy(direction, u).start()

    low_lanes = lax.broadcasted_iota(jnp.int32, gate_ref.shape[1:], 1) < hr

    def compute(k):
        x = xbuf[k].reshape(2 * rows, d)
        for e in range(n_local):
            for direction in range(2):
                a, b = gbuf[k, direction, 0], gbuf[k, direction, 1]
                mine = (n_local * me + e).astype(F32)
                both = jnp.where(low_lanes, a, pltpu.roll(b, hr, 1))
                ids = jnp.where(low_lanes, pltpu.roll(a, hr, 1), b)
                row = jnp.max(jnp.where(ids == mine, both, -1.0), axis=0, keepdims=True)
                gcol[e, direction * rows:(direction + 1) * rows, :] = jnp.transpose(jnp.broadcast_to(row, (rows, rows)))
        ft = 256
        for e in range(n_local):
            for nt in range(wg.shape[2] // ft):
                cols = slice(nt * ft, (nt + 1) * ft)
                g = jnp.dot(x, wg[e, :, cols], preferred_element_type=F32)
                u = jnp.dot(x, wu[e, :, cols], preferred_element_type=F32)
                act[:, cols] = (jax.nn.silu(g) * u).astype(BF16)
            a = act[...]
            gc = gcol[e]
            chosen = gc >= 0.0
            for nt in range(d // ft):
                f = jnp.dot(a, wd[e, :, nt * ft:(nt + 1) * ft], preferred_element_type=F32).astype(BF16).astype(F32)
                for l in range(ft // rows):
                    cols = slice(nt * ft + l * rows, nt * ft + (l + 1) * rows)
                    term = jnp.where(chosen, f[:, l * rows:(l + 1) * rows] * gc, 0.0).reshape(2, 2, hr, rows)
                    cbuf[k, :, :, :, cols] = term if e == 0 else cbuf[k, :, :, :, cols] + term

    def take(k):
        for direction in range(2):
            x_src, g_src = held(direction, k, core)
            for copy in ring_copies(direction, k - 1, x_src, g_src):
                copy.wait_recv()

            @pl.when(k <= n - 3)
            def _():
                for copy in ring_copies(direction, k + 1, x_src, g_src):
                    copy.start()

            for copy in pair_copies(direction, k, core, x_src, g_src):
                copy.start()

    def body(i, carry):
        k = jnp.where(i < half, i, i + 1 - 2 * lax.rem(i, 2))

        @pl.when(i <= n - 2)
        def _():
            take(i + 1)

        @pl.when(i == 0)
        def _():
            for copy in w_copies:
                copy.wait()

        @pl.when(i == n - 4)
        def _():
            for side in range(2):
                sum_copy(n - 5, side).wait_recv()
            for direction in range(2):
                rs_step(direction, 0)

        @pl.when(i == n - 2)
        def _():
            for side in range(2):
                sum_copy(n - 3, side).wait_recv()
            for u in range(1, 3):
                for direction in range(2):
                    rs_step(direction, u)

        for direction in range(2):
            for copy in pair_copies(direction, k, other, *held(direction, k, other)):
                copy.wait_recv()
        compute(k)
        for direction in range(2):
            sum_copy(k, direction).start()
        return carry

    lax.fori_loop(0, n, body, 0)

    summed = {(n - 5, 0), (n - 5, 1), (n - 3, 0), (n - 3, 1)}

    def wait_sum(k, side):
        if (k, side) not in summed:
            sum_copy(k, side).wait_recv()
            summed.add((k, side))

    for u in range(3, len(order)):
        for direction in range(2):
            wait_sum(*rs_place(direction, u)[:2])
            rs_step(direction, u)
    for h in range(2):
        wait_sum(0, h)
    seen = set()
    for u, (q, chain) in enumerate(order):
        for direction in range(2) if q == 1 else ():
            rs_copy(direction, u).wait_recv()
            i = quarter(direction, chain)
            part = pl.ds((i % 2) * qr, qr)
            at = pl.ds(i * qr, qr)
            if i in seen:
                out_ref[at, :] = (cbuf[0, i // 2, core, part, :] + inc[direction, 0, chain]).astype(out_ref.dtype)
            else:
                seen.add(i)
                cbuf[0, i // 2, core, part, :] = y_ref[at, :] + ((cbuf[0, i // 2, core, part, :] + cpart[0, i // 2, part, :]) + inc[direction, 0, chain])

    for direction in range(2):
        for v in range(n - 1):
            src = own(own_half(direction, v)) if v < 2 else held(direction, v - 1, core)
            for copy in ring_copies(direction, v, *src):
                copy.wait_send()
        for k in range(n):
            src = own(direction) if k == 0 else held(direction, k, core)
            for copy in pair_copies(direction, k, core, *src):
                copy.wait_send()
            sum_copy(k, direction).wait_send()
        for u in range(len(order)):
            rs_copy(direction, u).wait_send()


def moe(n_ep, r, gates, y, w_gate, w_up, w_down):
    n = n_ep // 2
    rows, d = r.shape
    n_local, _, ff = w_gate.shape
    vm = pl.BlockSpec(memory_space=pltpu.VMEM)
    hbm = pl.BlockSpec(memory_space=pltpu.HBM)
    dma = pltpu.SemaphoreType.DMA
    n_rs = 2 * (n - 1)
    return pl.pallas_call(
        functools.partial(moe_kernel, n),
        out_shape=jax.ShapeDtypeStruct((rows, d), BF16),
        in_specs=[vm] * 3 + [hbm] * 3,
        out_specs=vm,
        scratch_shapes=[
            pltpu.VMEM((n, 2, 2, rows // 2, d), BF16),
            pltpu.VMEM((n, 2, 2) + gates.shape[1:], F32),
            pltpu.VMEM((n, 2, 2, rows // 2, d), F32),
            pltpu.VMEM((n, 2, rows // 2, d), F32),
            pltpu.VMEM((2, n // 2 + 1, 4, rows // 4, d), F32),
            pltpu.VMEM(w_gate.shape, BF16), pltpu.VMEM(w_up.shape, BF16), pltpu.VMEM(w_down.shape, BF16),
            pltpu.VMEM((2 * rows, ff), BF16),
            pltpu.VMEM((n_local, 2 * rows, rows), F32),
            dma((3,)),
            dma((2, n - 1)), dma((2, n - 1)), dma((2, n - 1)), dma((2, n - 1)),
            dma((n, 2)), dma((n, 2)), dma((n, 2)), dma((n, 2)),
            dma((n, 2)), dma((n, 2)),
            dma((2, n_rs)), dma((2, n_rs)),
        ],
        compiler_params=pltpu.CompilerParams(collective_id=0, has_side_effects=True, vmem_limit_bytes=40 * 1024 * 1024),
        name="moe",
    )(r, gates, y, *in_hbm(w_gate, w_up, w_down))


def solution(mesh):
    n_ep = mesh.shape['ep']
    row_spec = P(('dp', 'ep'), None)
    cache_spec = P(('dp', 'ep'), None, None, None)
    len_spec = P(('dp', 'ep'))
    rep_vec = P(None)
    rep_mat = P(None, None)
    exp_spec = P('ep', None, None)

    def local_step(hidden, k_cache, v_cache, seq_lens, expert_ids, ln_attn, w_q, w_k, w_v, q_gain, k_gain, w_o, ln_moe, w_router, w_gate, w_up, w_down):
        k_t = jnp.transpose(k_cache, (1, 2, 3, 0))
        v_t = jnp.transpose(v_cache, (1, 2, 3, 0))
        k_new, v_new, y, r, gates = attend(
            hidden, k_t, v_t, seq_lens[None, :], expert_ids.T, ln_attn.reshape(-1, 128), w_q, w_k, w_v,
            q_gain[None, :], k_gain[None, :], w_o, ln_moe.reshape(-1, 128), w_router.T)
        out = moe(n_ep, r, gates, y, w_gate, w_up, w_down)
        return out, jnp.transpose(k_new, (3, 0, 1, 2)), jnp.transpose(v_new, (3, 0, 1, 2))

    return jax.shard_map(local_step, mesh=mesh, in_specs=(row_spec, cache_spec, cache_spec, len_spec, row_spec, rep_vec, rep_mat, rep_mat, rep_mat, rep_vec, rep_vec, rep_mat, rep_vec, rep_mat, exp_spec, exp_spec, exp_spec), out_specs=(row_spec, cache_spec, cache_spec), check_vma=False)
```

```python
import functools

import jax
import jax.numpy as jnp
import numpy as np
from jax import lax
from jax.experimental import pallas as pl
from jax.experimental.pallas import tpu as pltpu
from jax.sharding import PartitionSpec as P

EPS = 1e-6
ROPE_BASE = 1000000.0
F32 = jnp.float32
BF16 = jnp.bfloat16
MESH = pl.DeviceIdType.MESH


def in_hbm(*arrays):
    return [pltpu.with_memory_space_constraint(a, pltpu.HBM) for a in arrays]


def attend_kernel(h_hbm, lens_hbm, ids_hbm, ln_a_hbm, qg_hbm, kg_hbm, ln_m_hbm, wr_hbm,
                  wq_hbm, wk_hbm, wv_hbm, wo_hbm, kc_hbm, vc_hbm,
                  kn_hbm, vn_hbm, y_ref, r_ref, gate_ref, v_last,
                  h_ref, lens_ref, ids_ref, ln_a_ref, qg_ref, kg_ref, ln_m_ref, wr_ref,
                  kbuf, vbuf, wq, wk, wv, wo, qrot, knew, vnew, score, attn, small_sem, in_sem, out_sem):
    t_max, n_kv, hd, n_seq = kc_hbm.shape
    n_heads = wq_hbm.shape[1] // hd
    grp = n_heads // n_kv
    half = hd // 2
    n_chunk = 4
    tc = t_max // n_chunk

    w_copies = [pltpu.make_async_copy(src, dst, in_sem.at[i])
                for i, (src, dst) in enumerate(((wk_hbm, wk), (wq_hbm, wq), (wv_hbm, wv), (wo_hbm, wo)))]
    k_in = [pltpu.make_async_copy(kc_hbm.at[pl.ds(c * tc, tc)], kbuf.at[pl.ds(c * tc, tc)], in_sem.at[4 + c]) for c in range(n_chunk)]
    v_in = [pltpu.make_async_copy(vc_hbm.at[pl.ds(c * tc, tc)], vbuf.at[pl.ds(c * tc, tc)], in_sem.at[4 + n_chunk + c]) for c in range(n_chunk)]
    k_out = [pltpu.make_async_copy(kbuf.at[pl.ds(c * tc, tc)], kn_hbm.at[pl.ds(c * tc, tc)], out_sem.at[c]) for c in range(n_chunk)]
    v_out = [pltpu.make_async_copy(vbuf.at[pl.ds(c * tc, tc)], vn_hbm.at[pl.ds(c * tc, tc)], out_sem.at[n_chunk + c]) for c in range(n_chunk - 1)]
    small = [pltpu.make_async_copy(src, dst, small_sem.at[i]) for i, (src, dst) in enumerate((
        (h_hbm, h_ref), (lens_hbm, lens_ref), (ids_hbm, ids_ref), (ln_a_hbm, ln_a_ref), (qg_hbm, qg_ref), (kg_hbm, kg_ref), (ln_m_hbm, ln_m_ref), (wr_hbm, wr_ref)))]
    for copy in small + w_copies[:2]:
        copy.start()
    for copy in small:
        copy.wait()
    for copy in k_in:
        copy.start()

    def vector(ref):
        rows = ref[...].astype(F32)
        return jnp.concatenate([rows[i:i + 1, :] for i in range(rows.shape[0])], axis=1)

    h32 = h_ref[...].astype(F32)
    mean_sq = jnp.mean(h32 * h32, axis=1, keepdims=True)
    x = (h32 * lax.rsqrt(mean_sq + EPS) * vector(ln_a_ref)).astype(BF16)

    lens = lens_ref[...]
    f_iota = lax.broadcasted_iota(jnp.int32, (half, n_seq), 0)
    inv_freq = np.power(np.float32(ROPE_BASE), -np.arange(0, hd, 2).astype(np.float32) / np.float32(hd))
    freq = jnp.zeros((half, n_seq), F32)
    for i in range(half):
        freq = jnp.where(f_iota == i, float(inv_freq[i]), freq)
    angles = lens.astype(F32) * freq
    cos_v = jnp.cos(angles)
    sin_v = jnp.sin(angles)

    def gain_tile(g_ref):
        row = g_ref[...].astype(F32)
        row = jnp.concatenate([row] * (n_seq // hd), axis=1)
        return jnp.transpose(jnp.broadcast_to(row, (n_seq, n_seq)))[:hd, :]

    def rope_heads(proj, gain, dst, heads):
        for i in range(heads):
            if i % 2 == 0:
                pair = jnp.transpose(proj[:, i * hd:(i + 2) * hd])
            vals = pair[(i % 2) * hd:(i % 2 + 1) * hd, :]
            ms = jnp.mean(vals * vals, axis=0, keepdims=True)
            vals = vals * lax.rsqrt(ms + EPS) * gain
            low, high = vals[:half, :], vals[half:, :]
            dst[i * hd:i * hd + half, :] = (low * cos_v - high * sin_v).astype(BF16).astype(F32)
            dst[i * hd + half:(i + 1) * hd, :] = (high * cos_v + low * sin_v).astype(BF16).astype(F32)

    w_copies[0].wait()
    for copy in w_copies[2:3] + v_in + w_copies[3:]:
        copy.start()
    rope_heads(jnp.dot(x, wk[...], preferred_element_type=F32), gain_tile(kg_ref), knew, n_kv)
    w_copies[1].wait()
    rope_heads(jnp.dot(x, wq[...], preferred_element_type=F32), gain_tile(qg_ref), qrot, n_heads)
    sub = lax.broadcasted_iota(jnp.int32, (8, n_seq), 0)

    def fold(terms):
        top = sub < 4
        pairs = [jnp.where(top, a, b) + pltpu.roll(jnp.where(top, b, a), 4, 0)
                 for a, b in ((terms[0], terms[4]), (terms[2], terms[6]), (terms[1], terms[5]), (terms[3], terms[7]))]
        for shift, keep in ((2, sub % 4 < 2), (1, sub % 2 < 1)):
            pairs = [jnp.where(keep, a, pltpu.roll(b, shift, 0)) + jnp.where(keep, pltpu.roll(a, 8 - shift, 0), b)
                     for a, b in zip(pairs[0::2], pairs[1::2])]
        return pairs[0]

    for c in range(n_chunk):
        k_in[c].wait()

        def k_body(kv, carry, c=c):
            new = knew[pl.ds(pl.multiple_of(kv * hd, hd), hd), :]
            qs = [qrot[pl.ds(pl.multiple_of((kv * grp + g) * hd, hd), hd), :] for g in range(grp)]
            rows = [[] for _ in range(grp)]
            for tt in range(tc):
                t = c * tc + tt
                kt = jnp.where(lens == t, new, kbuf[t, kv].astype(F32))
                kbuf[t, kv] = kt.astype(BF16)
                for g in range(grp):
                    rows[g].append(jnp.sum((kt * qs[g]).reshape(hd // 8, 8, n_seq), axis=0))
            for g in range(grp):
                score[kv * grp + g, c * tc:(c + 1) * tc, :] = fold(rows[g])
            return carry

        lax.fori_loop(0, n_kv, k_body, 0)
        k_out[c].start()

    w_copies[2].wait()
    v_proj = jnp.dot(x, wv[...], preferred_element_type=F32)
    for i in range(0, n_kv, 2):
        vnew[i * hd:(i + 2) * hd, :] = jnp.transpose(v_proj[:, i * hd:(i + 2) * hd]).astype(BF16).astype(F32)

    visible = lax.broadcasted_iota(jnp.int32, (t_max, n_seq), 0) <= lens

    def soft_body(j, carry):
        s = jnp.where(visible, score[j] * (hd ** -0.5), -1e30)
        e = jnp.exp(s - jnp.max(s, axis=0, keepdims=True))
        score[j] = (e / jnp.sum(e, axis=0, keepdims=True)).astype(BF16).astype(F32)
        return carry

    lax.fori_loop(0, n_heads, soft_body, 0, unroll=2)

    for c in range(n_chunk):
        v_in[c].wait()

        def v_body(kv, carry, c=c):
            new = vnew[pl.ds(pl.multiple_of(kv * hd, hd), hd), :]
            at = [pl.ds(pl.multiple_of((kv * grp + g) * hd, hd), hd) for g in range(grp)]
            acc = [None if c == 0 else attn[at[g], :] for g in range(grp)]
            for tt in range(tc):
                t = c * tc + tt
                vt = jnp.where(lens == t, new, vbuf[t, kv].astype(F32))
                if c < n_chunk - 1:
                    vbuf[t, kv] = vt.astype(BF16)
                else:
                    v_last[tt, kv] = vt.astype(BF16)
                for g in range(grp):
                    term = vt * score[kv * grp + g, t:t + 1, :]
                    acc[g] = term if acc[g] is None else acc[g] + term
            for g in range(grp):
                attn[at[g], :] = acc[g]
            return carry

        lax.fori_loop(0, n_kv, v_body, 0)
        if c < n_chunk - 1:
            v_out[c].start()

    w_copies[3].wait()
    a_rows = jnp.concatenate([jnp.transpose(attn[i * n_seq:(i + 1) * n_seq, :]).astype(BF16) for i in range(n_heads * hd // n_seq)], axis=1)
    y = h32 + jnp.dot(a_rows, wo[...], preferred_element_type=F32)
    y_ref[...] = y
    mean_sq = jnp.mean(y * y, axis=1, keepdims=True)
    r = (y * lax.rsqrt(mean_sq + EPS) * vector(ln_m_ref)).astype(BF16)
    r_ref[...] = r
    logits = lax.dot_general(wr_ref[...], r, (((1,), (1,)), ((), ())), preferred_element_type=F32)
    e_iota = lax.broadcasted_iota(jnp.int32, logits.shape, 0)
    ids = ids_ref[...]
    chosen = e_iota == ids[0:1, :]
    for i in range(1, ids.shape[0]):
        chosen = chosen | (e_iota == ids[i:i + 1, :])
    top = jnp.max(jnp.where(chosen, logits, -jnp.inf), axis=0, keepdims=True)
    e = jnp.where(chosen, jnp.exp(logits - top), 0.0)
    gates = e / jnp.sum(e, axis=0, keepdims=True)
    picked = jnp.concatenate([jnp.sum(jnp.where(e_iota == ids[i:i + 1, :], gates, 0.0), axis=0, keepdims=True) for i in range(ids.shape[0])], axis=0)
    ids32 = ids.astype(F32)
    low = lax.broadcasted_iota(jnp.int32, ids.shape, 1) < n_seq // 2
    gate_ref[0] = jnp.where(low, picked, pltpu.roll(ids32, n_seq // 2, 1))
    gate_ref[1] = jnp.where(low, pltpu.roll(picked, n_seq // 2, 1), ids32)

    for copy in k_out + v_out:
        copy.wait()


def attend(hidden, k_t, v_t, lens, ids_t, ln_attn, w_q, w_k, w_v, q_gain, k_gain, w_o, ln_moe, w_router_t):
    n_seq, d = hidden.shape
    t_max, n_kv, hd, _ = k_t.shape
    hq, hk = w_q.shape[1], w_k.shape[1]
    n_heads = hq // hd
    vm = pl.BlockSpec(memory_space=pltpu.VMEM)
    hbm = pl.BlockSpec(memory_space=pltpu.HBM)
    small = (hidden, lens, ids_t, ln_attn, q_gain, k_gain, ln_moe, w_router_t)
    return pl.pallas_call(
        attend_kernel,
        out_shape=(
            jax.ShapeDtypeStruct(k_t.shape, k_t.dtype),
            jax.ShapeDtypeStruct(v_t.shape, v_t.dtype),
            jax.ShapeDtypeStruct((n_seq, d), F32),
            jax.ShapeDtypeStruct((n_seq, d), BF16),
            jax.ShapeDtypeStruct((2, ids_t.shape[0], n_seq), F32),
            pltpu.VMEM((t_max // 4,) + v_t.shape[1:], v_t.dtype),
        ),
        in_specs=[hbm] * 14,
        out_specs=(hbm, hbm, vm, vm, vm, vm),
        scratch_shapes=[pltpu.VMEM(a.shape, a.dtype) for a in small] + [
            pltpu.VMEM(k_t.shape, BF16), pltpu.VMEM(v_t.shape, BF16),
            pltpu.VMEM(w_q.shape, BF16), pltpu.VMEM(w_k.shape, BF16), pltpu.VMEM(w_v.shape, BF16), pltpu.VMEM(w_o.shape, BF16),
            pltpu.VMEM((hq, n_seq), F32), pltpu.VMEM((hk, n_seq), F32), pltpu.VMEM((hk, n_seq), F32),
            pltpu.VMEM((n_heads, t_max, n_seq), F32), pltpu.VMEM((hq, n_seq), F32),
            pltpu.SemaphoreType.DMA((len(small),)), pltpu.SemaphoreType.DMA((12,)), pltpu.SemaphoreType.DMA((8,)),
        ],
        compiler_params=pltpu.CompilerParams(vmem_limit_bytes=30 * 1024 * 1024),
        name="attend",
    )(*in_hbm(*small, w_q, w_k, w_v, w_o, k_t, v_t))


def rs_order(half):
    seq = [(half - 2, 3), (half + 1, 0), (half - 1, 2), (half, 1)]
    last = dict((c, q) for q, c in seq)
    for c in (0, 3, 1, 0, 2, 1, 0, 2, 1, 0):
        last[c] -= 1
        seq.append((last[c], c))
    return seq


def moe_kernel(n, r_ref, gate_ref, y_ref, wg_hbm, wu_hbm, wd_hbm, out_ref,
               xbuf, gbuf, cbuf, cpart, inc, wg, wu, wd, act, gcol,
               w_sem, ring_send, ring_recv, gate_send, gate_recv,
               pair_send, pair_recv, pgate_send, pgate_recv,
               sum_send, sum_recv, rs_send, rs_recv):
    me = lax.axis_index("ep")
    chip = me // 2
    core = lax.rem(me, 2)
    other = 1 - core
    half = n // 2
    rows, d = r_ref.shape
    n_local = wg_hbm.shape[0]
    hr = rows // 2
    qr = hr // 2
    ring = [{"ep": 2 * lax.rem(chip + 1, n) + core}, {"ep": 2 * lax.rem(chip + n - 1, n) + core}]
    pair = {"ep": 2 * chip + other}

    def remote(src, dst, ssem, rsem, dev):
        return pltpu.make_async_remote_copy(src_ref=src, dst_ref=dst, send_sem=ssem, recv_sem=rsem, device_id=dev, device_id_type=MESH)

    barrier = pltpu.get_barrier_semaphore()
    for dev in ring + [pair]:
        pl.semaphore_signal(barrier, inc=1, device_id=dev, device_id_type=MESH)
    w_copies = [pltpu.make_async_copy(src, dst, w_sem.at[i]) for i, (src, dst) in enumerate(((wg_hbm, wg), (wu_hbm, wu), (wd_hbm, wd)))]
    for copy in w_copies:
        copy.start()
    pl.semaphore_wait(barrier, 3)

    def ring_copies(direction, v, x_src, g_src):
        return [remote(g_src, gbuf.at[v + 1, direction, core], gate_send.at[direction, v], gate_recv.at[direction, v], ring[direction]),
                remote(x_src, xbuf.at[v + 1, direction, core], ring_send.at[direction, v], ring_recv.at[direction, v], ring[direction])]

    def pair_copies(direction, k, c, x_src, g_src):
        return [remote(g_src, gbuf.at[k, direction, c], pgate_send.at[k, direction], pgate_recv.at[k, direction], pair),
                remote(x_src, xbuf.at[k, direction, c], pair_send.at[k, direction], pair_recv.at[k, direction], pair)]

    def held(direction, k, c):
        return xbuf.at[k, direction, c], gbuf.at[k, direction, c]

    def own(h):
        return r_ref.at[pl.ds(h * hr, hr)], gate_ref.at[h]

    def own_half(direction, v):
        return v if direction == 0 else 1 - v

    for v in range(2):
        for direction in range(2):
            for copy in ring_copies(direction, v, *own(own_half(direction, v))):
                copy.start()
        if v == 0:
            for h in range(2):
                for copy in pair_copies(h, 0, core, *own(h)):
                    copy.start()
    for h in range(2):
        xbuf[0, h, core] = r_ref[h * hr:(h + 1) * hr, :]
        gbuf[0, h, core] = gate_ref[h]

    def sum_copy(k, direction):
        return remote(cbuf.at[k, direction, other], cpart.at[k, direction], sum_send.at[k, direction], sum_recv.at[k, direction], pair)

    order = rs_order(half)

    def quarter(direction, chain):
        return chain if direction == 0 else 3 - chain

    def rs_place(direction, u):
        q, chain = order[u]
        i = quarter(direction, chain)
        step = q if direction == 0 else -q
        step = step - n if step > half else step + n if step <= -half else step
        h = i // 2
        if step == half:
            k, side = n - 1, h
        elif step > 0:
            k, side = 2 * step - h, 1
        else:
            k, side = -2 * step - 1 + h, 0
        return k, side, pl.ds((i % 2) * qr, qr)

    def rs_copy(direction, u):
        q, chain = order[u]
        k, side, at = rs_place(direction, u)
        return remote(cbuf.at[k, side, core, at], inc.at[direction, q - 1, chain], rs_send.at[direction, u], rs_recv.at[direction, u], ring[direction])

    def rs_step(direction, u):
        q, chain = order[u]
        k, side, at = rs_place(direction, u)
        total = cbuf[k, side, core, at, :] + cpart[k, side, at, :]
        if (q + 1, chain) in order:
            rs_copy(direction, order.index((q + 1, chain))).wait_recv()
            total = total + inc[direction, q, chain]
        cbuf[k, side, core, at, :] = total
        rs_copy(direction, u).start()

    low_lanes = lax.broadcasted_iota(jnp.int32, gate_ref.shape[1:], 1) < hr

    def compute(k):
        x = xbuf[k].reshape(2 * rows, d)
        for e in range(n_local):
            for direction in range(2):
                a, b = gbuf[k, direction, 0], gbuf[k, direction, 1]
                mine = (n_local * me + e).astype(F32)
                both = jnp.where(low_lanes, a, pltpu.roll(b, hr, 1))
                ids = jnp.where(low_lanes, pltpu.roll(a, hr, 1), b)
                row = jnp.max(jnp.where(ids == mine, both, -1.0), axis=0, keepdims=True)
                gcol[e, direction * rows:(direction + 1) * rows, :] = jnp.transpose(jnp.broadcast_to(row, (rows, rows)))
        ft = 256
        for e in range(n_local):
            for nt in range(wg.shape[2] // ft):
                cols = slice(nt * ft, (nt + 1) * ft)
                g = jnp.dot(x, wg[e, :, cols], preferred_element_type=F32)
                u = jnp.dot(x, wu[e, :, cols], preferred_element_type=F32)
                act[:, cols] = (jax.nn.silu(g) * u).astype(BF16)
            a = act[...]
            gc = gcol[e]
            chosen = gc >= 0.0
            for nt in range(d // ft):
                f = jnp.dot(a, wd[e, :, nt * ft:(nt + 1) * ft], preferred_element_type=F32).astype(BF16).astype(F32)
                for l in range(ft // rows):
                    cols = slice(nt * ft + l * rows, nt * ft + (l + 1) * rows)
                    term = jnp.where(chosen, f[:, l * rows:(l + 1) * rows] * gc, 0.0).reshape(2, 2, hr, rows)
                    cbuf[k, :, :, :, cols] = term if e == 0 else cbuf[k, :, :, :, cols] + term

    def take(k):
        for direction in range(2):
            x_src, g_src = held(direction, k, core)
            for copy in ring_copies(direction, k - 1, x_src, g_src):
                copy.wait_recv()

            @pl.when(k <= n - 3)
            def _():
                for copy in ring_copies(direction, k + 1, x_src, g_src):
                    copy.start()

            for copy in pair_copies(direction, k, core, x_src, g_src):
                copy.start()

    def body(i, carry):
        k = jnp.where(i < half, i, i + 1 - 2 * lax.rem(i, 2))

        @pl.when(i <= n - 2)
        def _():
            take(i + 1)

        @pl.when(i == 0)
        def _():
            for copy in w_copies:
                copy.wait()

        @pl.when(i == n - 4)
        def _():
            for side in range(2):
                sum_copy(n - 5, side).wait_recv()
            for direction in range(2):
                rs_step(direction, 0)

        @pl.when(i == n - 2)
        def _():
            for side in range(2):
                sum_copy(n - 3, side).wait_recv()
            for u in range(1, 3):
                for direction in range(2):
                    rs_step(direction, u)

        for direction in range(2):
            for copy in pair_copies(direction, k, other, *held(direction, k, other)):
                copy.wait_recv()
        compute(k)
        for direction in range(2):
            sum_copy(k, direction).start()
        return carry

    lax.fori_loop(0, n, body, 0)

    summed = {(n - 5, 0), (n - 5, 1), (n - 3, 0), (n - 3, 1)}

    def wait_sum(k, side):
        if (k, side) not in summed:
            sum_copy(k, side).wait_recv()
            summed.add((k, side))

    for u in range(3, len(order)):
        for direction in range(2):
            wait_sum(*rs_place(direction, u)[:2])
            rs_step(direction, u)
    for h in range(2):
        wait_sum(0, h)
    seen = set()
    for u, (q, chain) in enumerate(order):
        for direction in range(2) if q == 1 else ():
            rs_copy(direction, u).wait_recv()
            i = quarter(direction, chain)
            part = pl.ds((i % 2) * qr, qr)
            at = pl.ds(i * qr, qr)
            if i in seen:
                out_ref[at, :] = (cbuf[0, i // 2, core, part, :] + inc[direction, 0, chain]).astype(out_ref.dtype)
            else:
                seen.add(i)
                cbuf[0, i // 2, core, part, :] = y_ref[at, :] + ((cbuf[0, i // 2, core, part, :] + cpart[0, i // 2, part, :]) + inc[direction, 0, chain])

    for direction in range(2):
        for v in range(n - 1):
            src = own(own_half(direction, v)) if v < 2 else held(direction, v - 1, core)
            for copy in ring_copies(direction, v, *src):
                copy.wait_send()
        for k in range(n):
            src = own(direction) if k == 0 else held(direction, k, core)
            for copy in pair_copies(direction, k, core, *src):
                copy.wait_send()
            sum_copy(k, direction).wait_send()
        for u in range(len(order)):
            rs_copy(direction, u).wait_send()


def moe(n_ep, r, gates, y, w_gate, w_up, w_down):
    n = n_ep // 2
    rows, d = r.shape
    n_local, _, ff = w_gate.shape
    vm = pl.BlockSpec(memory_space=pltpu.VMEM)
    hbm = pl.BlockSpec(memory_space=pltpu.HBM)
    dma = pltpu.SemaphoreType.DMA
    n_rs = 2 * (n - 1)
    return pl.pallas_call(
        functools.partial(moe_kernel, n),
        out_shape=jax.ShapeDtypeStruct((rows, d), BF16),
        in_specs=[vm] * 3 + [hbm] * 3,
        out_specs=vm,
        scratch_shapes=[
            pltpu.VMEM((n, 2, 2, rows // 2, d), BF16),
            pltpu.VMEM((n, 2, 2) + gates.shape[1:], F32),
            pltpu.VMEM((n, 2, 2, rows // 2, d), F32),
            pltpu.VMEM((n, 2, rows // 2, d), F32),
            pltpu.VMEM((2, n // 2 + 1, 4, rows // 4, d), F32),
            pltpu.VMEM(w_gate.shape, BF16), pltpu.VMEM(w_up.shape, BF16), pltpu.VMEM(w_down.shape, BF16),
            pltpu.VMEM((2 * rows, ff), BF16),
            pltpu.VMEM((n_local, 2 * rows, rows), F32),
            dma((3,)),
            dma((2, n - 1)), dma((2, n - 1)), dma((2, n - 1)), dma((2, n - 1)),
            dma((n, 2)), dma((n, 2)), dma((n, 2)), dma((n, 2)),
            dma((n, 2)), dma((n, 2)),
            dma((2, n_rs)), dma((2, n_rs)),
        ],
        compiler_params=pltpu.CompilerParams(collective_id=0, has_side_effects=True, vmem_limit_bytes=40 * 1024 * 1024),
        name="moe",
    )(r, gates, y, *in_hbm(w_gate, w_up, w_down))


def finish_kernel(out_ref, v_last, v_in_hbm, out_hbm, v_hbm, sem):
    rows = v_last.shape[0]
    copies = [pltpu.make_async_copy(v_last, v_hbm.at[pl.ds(v_hbm.shape[0] - rows, rows)], sem.at[0]),
              pltpu.make_async_copy(out_ref, out_hbm, sem.at[1])]
    for copy in copies:
        copy.start()
    for copy in copies:
        copy.wait()


def finish(out, v_last, v_new):
    vm = pl.BlockSpec(memory_space=pltpu.VMEM)
    hbm = pl.BlockSpec(memory_space=pltpu.HBM)
    return pl.pallas_call(
        finish_kernel,
        out_shape=(jax.ShapeDtypeStruct(out.shape, out.dtype), jax.ShapeDtypeStruct(v_new.shape, v_new.dtype)),
        in_specs=[vm, vm, hbm],
        out_specs=(hbm, hbm),
        scratch_shapes=[pltpu.SemaphoreType.DMA((2,))],
        input_output_aliases={2: 1},
        compiler_params=pltpu.CompilerParams(vmem_limit_bytes=4 * 1024 * 1024),
        name="finish",
    )(out, pltpu.with_memory_space_constraint(v_last, pltpu.VMEM), v_new)


def solution(mesh):
    n_ep = mesh.shape['ep']
    row_spec = P(('dp', 'ep'), None)
    cache_spec = P(('dp', 'ep'), None, None, None)
    len_spec = P(('dp', 'ep'))
    rep_vec = P(None)
    rep_mat = P(None, None)
    exp_spec = P('ep', None, None)

    def local_step(hidden, k_cache, v_cache, seq_lens, expert_ids, ln_attn, w_q, w_k, w_v, q_gain, k_gain, w_o, ln_moe, w_router, w_gate, w_up, w_down):
        k_t = jnp.transpose(k_cache, (1, 2, 3, 0))
        v_t = jnp.transpose(v_cache, (1, 2, 3, 0))
        k_new, v_new, y, r, gates, v_last = attend(
            hidden, k_t, v_t, seq_lens[None, :], expert_ids.T, ln_attn.reshape(-1, 128), w_q, w_k, w_v,
            q_gain[None, :], k_gain[None, :], w_o, ln_moe.reshape(-1, 128), w_router.T)
        out, v_new = finish(moe(n_ep, r, gates, y, w_gate, w_up, w_down), v_last, v_new)
        return out, jnp.transpose(k_new, (3, 0, 1, 2)), jnp.transpose(v_new, (3, 0, 1, 2))

    return jax.shard_map(local_step, mesh=mesh, in_specs=(row_spec, cache_spec, cache_spec, len_spec, row_spec, rep_vec, rep_mat, rep_mat, rep_mat, rep_vec, rep_vec, rep_mat, rep_vec, rep_mat, exp_spec, exp_spec, exp_spec), out_specs=(row_spec, cache_spec, cache_spec), check_vma=False)
```

```python
import functools

import jax
import jax.numpy as jnp
import numpy as np
from jax import lax
from jax.experimental import pallas as pl
from jax.experimental.pallas import tpu as pltpu
from jax.sharding import PartitionSpec as P

EPS = 1e-6
ROPE_BASE = 1000000.0
F32 = jnp.float32
BF16 = jnp.bfloat16
MESH = pl.DeviceIdType.MESH


def in_hbm(*arrays):
    return [pltpu.with_memory_space_constraint(a, pltpu.HBM) for a in arrays]


def attend_kernel(h_hbm, lens_hbm, ids_hbm, ln_a_hbm, qg_hbm, kg_hbm, ln_m_hbm, wr_hbm,
                  wq_hbm, wk_hbm, wv_hbm, wo_hbm, kc_hbm, vc_hbm,
                  kn_hbm, vn_hbm, y_ref, r_ref, gate_ref,
                  h_ref, lens_ref, ids_ref, ln_a_ref, qg_ref, kg_ref, ln_m_ref, wr_ref,
                  kbuf, vbuf, wq, wk, wv, wo, qrot, knew, vnew, score, attn, small_sem, in_sem, out_sem):
    t_max, n_kv, hd, n_seq = kc_hbm.shape
    n_heads = wq_hbm.shape[1] // hd
    grp = n_heads // n_kv
    half = hd // 2
    n_chunk = 4
    tc = t_max // n_chunk

    w_copies = [pltpu.make_async_copy(src, dst, in_sem.at[i])
                for i, (src, dst) in enumerate(((wk_hbm, wk), (wq_hbm, wq), (wv_hbm, wv), (wo_hbm, wo)))]
    k_in = [pltpu.make_async_copy(kc_hbm.at[pl.ds(c * tc, tc)], kbuf.at[pl.ds(c * tc, tc)], in_sem.at[4 + c]) for c in range(n_chunk)]
    v_in = [pltpu.make_async_copy(vc_hbm.at[pl.ds(c * tc, tc)], vbuf.at[pl.ds(c * tc, tc)], in_sem.at[4 + n_chunk + c]) for c in range(n_chunk)]
    k_out = [pltpu.make_async_copy(kbuf.at[pl.ds(c * tc, tc)], kn_hbm.at[pl.ds(c * tc, tc)], out_sem.at[c]) for c in range(n_chunk)]
    v_out = [pltpu.make_async_copy(vbuf.at[pl.ds(c * tc, tc)], vn_hbm.at[pl.ds(c * tc, tc)], out_sem.at[n_chunk + c]) for c in range(n_chunk)]
    small = [pltpu.make_async_copy(src, dst, small_sem.at[i]) for i, (src, dst) in enumerate((
        (h_hbm, h_ref), (lens_hbm, lens_ref), (ids_hbm, ids_ref), (ln_a_hbm, ln_a_ref), (qg_hbm, qg_ref), (kg_hbm, kg_ref), (ln_m_hbm, ln_m_ref), (wr_hbm, wr_ref)))]
    for copy in small + w_copies[:2]:
        copy.start()
    for copy in small:
        copy.wait()

    def vector(ref):
        rows = ref[...].astype(F32)
        return jnp.concatenate([rows[i:i + 1, :] for i in range(rows.shape[0])], axis=1)

    h32 = h_ref[...].astype(F32)
    mean_sq = jnp.mean(h32 * h32, axis=1, keepdims=True)
    x = (h32 * lax.rsqrt(mean_sq + EPS) * vector(ln_a_ref)).astype(BF16)

    lens = lens_ref[...]
    f_iota = lax.broadcasted_iota(jnp.int32, (half, n_seq), 0)
    inv_freq = np.power(np.float32(ROPE_BASE), -np.arange(0, hd, 2).astype(np.float32) / np.float32(hd))
    freq = jnp.zeros((half, n_seq), F32)
    for i in range(half):
        freq = jnp.where(f_iota == i, float(inv_freq[i]), freq)
    angles = lens.astype(F32) * freq
    cos_v = jnp.cos(angles)
    sin_v = jnp.sin(angles)

    def gain_tile(g_ref):
        row = g_ref[...].astype(F32)
        row = jnp.concatenate([row] * (n_seq // hd), axis=1)
        return jnp.transpose(jnp.broadcast_to(row, (n_seq, n_seq)))[:hd, :]

    def rope_heads(proj, gain, dst, heads):
        for i in range(heads):
            if i % 2 == 0:
                pair = jnp.transpose(proj[:, i * hd:(i + 2) * hd])
            vals = pair[(i % 2) * hd:(i % 2 + 1) * hd, :]
            ms = jnp.mean(vals * vals, axis=0, keepdims=True)
            vals = vals * lax.rsqrt(ms + EPS) * gain
            low, high = vals[:half, :], vals[half:, :]
            dst[i * hd:i * hd + half, :] = (low * cos_v - high * sin_v).astype(BF16).astype(F32)
            dst[i * hd + half:(i + 1) * hd, :] = (high * cos_v + low * sin_v).astype(BF16).astype(F32)

    w_copies[0].wait()
    for copy in k_in[:2]:
        copy.start()
    rope_heads(jnp.dot(x, wk[...], preferred_element_type=F32), gain_tile(kg_ref), knew, n_kv)
    w_copies[1].wait()
    for copy in k_in[2:] + w_copies[2:3]:
        copy.start()
    rope_heads(jnp.dot(x, wq[...], preferred_element_type=F32), gain_tile(qg_ref), qrot, n_heads)
    sub = lax.broadcasted_iota(jnp.int32, (8, n_seq), 0)

    def fold(terms):
        top = sub < 4
        pairs = [jnp.where(top, a, b) + pltpu.roll(jnp.where(top, b, a), 4, 0)
                 for a, b in ((terms[0], terms[4]), (terms[2], terms[6]), (terms[1], terms[5]), (terms[3], terms[7]))]
        for shift, keep in ((2, sub % 4 < 2), (1, sub % 2 < 1)):
            pairs = [jnp.where(keep, a, pltpu.roll(b, shift, 0)) + jnp.where(keep, pltpu.roll(a, 8 - shift, 0), b)
                     for a, b in zip(pairs[0::2], pairs[1::2])]
        return pairs[0]

    for c in range(n_chunk):
        k_in[c].wait()
        for copy in (v_in[:2], v_in[2:], w_copies[3:], [])[c]:
            copy.start()

        def k_body(kv, carry, c=c):
            new = knew[pl.ds(pl.multiple_of(kv * hd, hd), hd), :]
            qs = [qrot[pl.ds(pl.multiple_of((kv * grp + g) * hd, hd), hd), :] for g in range(grp)]
            rows = [[] for _ in range(grp)]
            for tt in range(tc):
                t = c * tc + tt
                kt = jnp.where(lens == t, new, kbuf[t, kv].astype(F32))
                kbuf[t, kv] = kt.astype(BF16)
                for g in range(grp):
                    rows[g].append(jnp.sum((kt * qs[g]).reshape(hd // 8, 8, n_seq), axis=0))
            for g in range(grp):
                score[kv * grp + g, c * tc:(c + 1) * tc, :] = fold(rows[g])
            return carry

        lax.fori_loop(0, n_kv, k_body, 0)
        k_out[c].start()

    w_copies[2].wait()
    v_proj = jnp.dot(x, wv[...], preferred_element_type=F32)
    for i in range(0, n_kv, 2):
        vnew[i * hd:(i + 2) * hd, :] = jnp.transpose(v_proj[:, i * hd:(i + 2) * hd]).astype(BF16).astype(F32)

    visible = lax.broadcasted_iota(jnp.int32, (t_max, n_seq), 0) <= lens

    def soft_body(j, carry):
        s = jnp.where(visible, score[j] * (hd ** -0.5), -1e30)
        e = jnp.exp(s - jnp.max(s, axis=0, keepdims=True))
        score[j] = (e / jnp.sum(e, axis=0, keepdims=True)).astype(BF16).astype(F32)
        return carry

    lax.fori_loop(0, n_heads, soft_body, 0, unroll=2)

    for c in range(n_chunk):
        v_in[c].wait()

        def v_body(kv, carry, c=c):
            new = vnew[pl.ds(pl.multiple_of(kv * hd, hd), hd), :]
            at = [pl.ds(pl.multiple_of((kv * grp + g) * hd, hd), hd) for g in range(grp)]
            acc = [None if c == 0 else attn[at[g], :] for g in range(grp)]
            for tt in range(tc):
                t = c * tc + tt
                vt = jnp.where(lens == t, new, vbuf[t, kv].astype(F32))
                vbuf[t, kv] = vt.astype(BF16)
                for g in range(grp):
                    term = vt * score[kv * grp + g, t:t + 1, :]
                    acc[g] = term if acc[g] is None else acc[g] + term
            for g in range(grp):
                attn[at[g], :] = acc[g]
            return carry

        lax.fori_loop(0, n_kv, v_body, 0)
        v_out[c].start()

    w_copies[3].wait()
    a_rows = jnp.concatenate([jnp.transpose(attn[i * n_seq:(i + 1) * n_seq, :]).astype(BF16) for i in range(n_heads * hd // n_seq)], axis=1)
    y = h32 + jnp.dot(a_rows, wo[...], preferred_element_type=F32)
    y_ref[...] = y
    mean_sq = jnp.mean(y * y, axis=1, keepdims=True)
    r = (y * lax.rsqrt(mean_sq + EPS) * vector(ln_m_ref)).astype(BF16)
    r_ref[...] = r
    logits = lax.dot_general(wr_ref[...], r, (((1,), (1,)), ((), ())), preferred_element_type=F32)
    e_iota = lax.broadcasted_iota(jnp.int32, logits.shape, 0)
    ids = ids_ref[...]
    chosen = e_iota == ids[0:1, :]
    for i in range(1, ids.shape[0]):
        chosen = chosen | (e_iota == ids[i:i + 1, :])
    top = jnp.max(jnp.where(chosen, logits, -jnp.inf), axis=0, keepdims=True)
    e = jnp.where(chosen, jnp.exp(logits - top), 0.0)
    gates = e / jnp.sum(e, axis=0, keepdims=True)
    picked = jnp.concatenate([jnp.sum(jnp.where(e_iota == ids[i:i + 1, :], gates, 0.0), axis=0, keepdims=True) for i in range(ids.shape[0])], axis=0)
    ids32 = ids.astype(F32)
    low = lax.broadcasted_iota(jnp.int32, ids.shape, 1) < n_seq // 2
    gate_ref[0] = jnp.where(low, picked, pltpu.roll(ids32, n_seq // 2, 1))
    gate_ref[1] = jnp.where(low, pltpu.roll(picked, n_seq // 2, 1), ids32)

    for copy in k_out + v_out:
        copy.wait()


def attend(hidden, k_t, v_t, lens, ids_t, ln_attn, w_q, w_k, w_v, q_gain, k_gain, w_o, ln_moe, w_router_t):
    n_seq, d = hidden.shape
    t_max, n_kv, hd, _ = k_t.shape
    hq, hk = w_q.shape[1], w_k.shape[1]
    n_heads = hq // hd
    vm = pl.BlockSpec(memory_space=pltpu.VMEM)
    hbm = pl.BlockSpec(memory_space=pltpu.HBM)
    small = (hidden, lens, ids_t, ln_attn, q_gain, k_gain, ln_moe, w_router_t)
    return pl.pallas_call(
        attend_kernel,
        out_shape=(
            jax.ShapeDtypeStruct(k_t.shape, k_t.dtype),
            jax.ShapeDtypeStruct(v_t.shape, v_t.dtype),
            jax.ShapeDtypeStruct((n_seq, d), F32),
            jax.ShapeDtypeStruct((n_seq, d), BF16),
            jax.ShapeDtypeStruct((2, ids_t.shape[0], n_seq), F32),
        ),
        in_specs=[hbm] * 14,
        out_specs=(hbm, hbm, vm, vm, vm),
        scratch_shapes=[pltpu.VMEM(a.shape, a.dtype) for a in small] + [
            pltpu.VMEM(k_t.shape, BF16), pltpu.VMEM(v_t.shape, BF16),
            pltpu.VMEM(w_q.shape, BF16), pltpu.VMEM(w_k.shape, BF16), pltpu.VMEM(w_v.shape, BF16), pltpu.VMEM(w_o.shape, BF16),
            pltpu.VMEM((hq, n_seq), F32), pltpu.VMEM((hk, n_seq), F32), pltpu.VMEM((hk, n_seq), F32),
            pltpu.VMEM((n_heads, t_max, n_seq), F32), pltpu.VMEM((hq, n_seq), F32),
            pltpu.SemaphoreType.DMA((len(small),)), pltpu.SemaphoreType.DMA((12,)), pltpu.SemaphoreType.DMA((8,)),
        ],
        compiler_params=pltpu.CompilerParams(vmem_limit_bytes=30 * 1024 * 1024),
        name="attend",
    )(*in_hbm(*small, w_q, w_k, w_v, w_o, k_t, v_t))


def rs_order(half):
    seq = [(half - 2, 3), (half + 1, 0), (half - 1, 2), (half, 1)]
    last = dict((c, q) for q, c in seq)
    for c in (0, 3, 1, 0, 2, 1, 0, 2, 1, 0):
        last[c] -= 1
        seq.append((last[c], c))
    return seq


def moe_kernel(n, r_ref, gate_ref, y_ref, wg_hbm, wu_hbm, wd_hbm, out_ref,
               xbuf, gbuf, cbuf, cpart, inc, wg, wu, wd, act, gcol,
               w_sem, ring_send, ring_recv, gate_send, gate_recv,
               pair_send, pair_recv, pgate_send, pgate_recv,
               sum_send, sum_recv, rs_send, rs_recv):
    me = lax.axis_index("ep")
    chip = me // 2
    core = lax.rem(me, 2)
    other = 1 - core
    half = n // 2
    rows, d = r_ref.shape
    n_local = wg_hbm.shape[0]
    hr = rows // 2
    qr = hr // 2
    ring = [{"ep": 2 * lax.rem(chip + 1, n) + core}, {"ep": 2 * lax.rem(chip + n - 1, n) + core}]
    pair = {"ep": 2 * chip + other}

    def remote(src, dst, ssem, rsem, dev):
        return pltpu.make_async_remote_copy(src_ref=src, dst_ref=dst, send_sem=ssem, recv_sem=rsem, device_id=dev, device_id_type=MESH)

    barrier = pltpu.get_barrier_semaphore()
    for dev in ring + [pair]:
        pl.semaphore_signal(barrier, inc=1, device_id=dev, device_id_type=MESH)
    w_copies = [pltpu.make_async_copy(src, dst, w_sem.at[i]) for i, (src, dst) in enumerate(((wg_hbm, wg), (wu_hbm, wu), (wd_hbm, wd)))]
    for copy in w_copies:
        copy.start()
    pl.semaphore_wait(barrier, 3)

    def ring_copies(direction, v, x_src, g_src):
        return [remote(g_src, gbuf.at[v + 1, direction, core], gate_send.at[direction, v], gate_recv.at[direction, v], ring[direction]),
                remote(x_src, xbuf.at[v + 1, direction, core], ring_send.at[direction, v], ring_recv.at[direction, v], ring[direction])]

    def pair_copies(direction, k, c, x_src, g_src):
        return [remote(g_src, gbuf.at[k, direction, c], pgate_send.at[k, direction], pgate_recv.at[k, direction], pair),
                remote(x_src, xbuf.at[k, direction, c], pair_send.at[k, direction], pair_recv.at[k, direction], pair)]

    def held(direction, k, c):
        return xbuf.at[k, direction, c], gbuf.at[k, direction, c]

    def own(h):
        return r_ref.at[pl.ds(h * hr, hr)], gate_ref.at[h]

    def own_half(direction, v):
        return v if direction == 0 else 1 - v

    for v in range(2):
        for direction in range(2):
            for copy in ring_copies(direction, v, *own(own_half(direction, v))):
                copy.start()
        if v == 0:
            for h in range(2):
                for copy in pair_copies(h, 0, core, *own(h)):
                    copy.start()
    for h in range(2):
        xbuf[0, h, core] = r_ref[h * hr:(h + 1) * hr, :]
        gbuf[0, h, core] = gate_ref[h]

    def sum_copy(k, direction):
        return remote(cbuf.at[k, direction, other], cpart.at[k, direction], sum_send.at[k, direction], sum_recv.at[k, direction], pair)

    order = rs_order(half)

    def quarter(direction, chain):
        return chain if direction == 0 else 3 - chain

    def rs_place(direction, u):
        q, chain = order[u]
        i = quarter(direction, chain)
        step = q if direction == 0 else -q
        step = step - n if step > half else step + n if step <= -half else step
        h = i // 2
        if step == half:
            k, side = n - 1, h
        elif step > 0:
            k, side = 2 * step - h, 1
        else:
            k, side = -2 * step - 1 + h, 0
        return k, side, pl.ds((i % 2) * qr, qr)

    def rs_copy(direction, u):
        q, chain = order[u]
        k, side, at = rs_place(direction, u)
        return remote(cbuf.at[k, side, core, at], inc.at[direction, q - 1, chain], rs_send.at[direction, u], rs_recv.at[direction, u], ring[direction])

    def rs_step(direction, u):
        q, chain = order[u]
        k, side, at = rs_place(direction, u)
        total = cbuf[k, side, core, at, :] + cpart[k, side, at, :]
        if (q + 1, chain) in order:
            rs_copy(direction, order.index((q + 1, chain))).wait_recv()
            total = total + inc[direction, q, chain]
        cbuf[k, side, core, at, :] = total
        rs_copy(direction, u).start()

    low_lanes = lax.broadcasted_iota(jnp.int32, gate_ref.shape[1:], 1) < hr

    def compute(k):
        x = xbuf[k].reshape(2 * rows, d)
        for e in range(n_local):
            for direction in range(2):
                a, b = gbuf[k, direction, 0], gbuf[k, direction, 1]
                mine = (n_local * me + e).astype(F32)
                both = jnp.where(low_lanes, a, pltpu.roll(b, hr, 1))
                ids = jnp.where(low_lanes, pltpu.roll(a, hr, 1), b)
                row = jnp.max(jnp.where(ids == mine, both, -1.0), axis=0, keepdims=True)
                gcol[e, direction * rows:(direction + 1) * rows, :] = jnp.transpose(jnp.broadcast_to(row, (rows, rows)))
        ft = 256
        for e in range(n_local):
            for nt in range(wg.shape[2] // ft):
                cols = slice(nt * ft, (nt + 1) * ft)
                g = jnp.dot(x, wg[e, :, cols], preferred_element_type=F32)
                u = jnp.dot(x, wu[e, :, cols], preferred_element_type=F32)
                act[:, cols] = (jax.nn.silu(g) * u).astype(BF16)
            a = act[...]
            gc = gcol[e]
            chosen = gc >= 0.0
            for nt in range(d // ft):
                f = jnp.dot(a, wd[e, :, nt * ft:(nt + 1) * ft], preferred_element_type=F32).astype(BF16).astype(F32)
                for l in range(ft // rows):
                    cols = slice(nt * ft + l * rows, nt * ft + (l + 1) * rows)
                    term = jnp.where(chosen, f[:, l * rows:(l + 1) * rows] * gc, 0.0).reshape(2, 2, hr, rows)
                    cbuf[k, :, :, :, cols] = term if e == 0 else cbuf[k, :, :, :, cols] + term

    def take(k):
        for direction in range(2):
            x_src, g_src = held(direction, k, core)
            for copy in ring_copies(direction, k - 1, x_src, g_src):
                copy.wait_recv()

            @pl.when(k <= n - 3)
            def _():
                for copy in ring_copies(direction, k + 1, x_src, g_src):
                    copy.start()

            for copy in pair_copies(direction, k, core, x_src, g_src):
                copy.start()

    def body(i, carry):
        k = jnp.where(i < half, i, i + 1 - 2 * lax.rem(i, 2))

        @pl.when(i <= n - 2)
        def _():
            take(i + 1)

        @pl.when(i == 0)
        def _():
            for copy in w_copies:
                copy.wait()

        @pl.when(i == n - 4)
        def _():
            for side in range(2):
                sum_copy(n - 5, side).wait_recv()
            for direction in range(2):
                rs_step(direction, 0)

        @pl.when(i == n - 2)
        def _():
            for side in range(2):
                sum_copy(n - 3, side).wait_recv()
            for u in range(1, 3):
                for direction in range(2):
                    rs_step(direction, u)

        for direction in range(2):
            for copy in pair_copies(direction, k, other, *held(direction, k, other)):
                copy.wait_recv()
        compute(k)
        for direction in range(2):
            sum_copy(k, direction).start()
        return carry

    lax.fori_loop(0, n, body, 0)

    summed = {(n - 5, 0), (n - 5, 1), (n - 3, 0), (n - 3, 1)}

    def wait_sum(k, side):
        if (k, side) not in summed:
            sum_copy(k, side).wait_recv()
            summed.add((k, side))

    for u in range(3, len(order)):
        for direction in range(2):
            wait_sum(*rs_place(direction, u)[:2])
            rs_step(direction, u)
    for h in range(2):
        wait_sum(0, h)
    seen = set()
    for u, (q, chain) in enumerate(order):
        for direction in range(2) if q == 1 else ():
            rs_copy(direction, u).wait_recv()
            i = quarter(direction, chain)
            part = pl.ds((i % 2) * qr, qr)
            at = pl.ds(i * qr, qr)
            if i in seen:
                out_ref[at, :] = (cbuf[0, i // 2, core, part, :] + inc[direction, 0, chain]).astype(out_ref.dtype)
            else:
                seen.add(i)
                cbuf[0, i // 2, core, part, :] = y_ref[at, :] + ((cbuf[0, i // 2, core, part, :] + cpart[0, i // 2, part, :]) + inc[direction, 0, chain])

    for direction in range(2):
        for v in range(n - 1):
            src = own(own_half(direction, v)) if v < 2 else held(direction, v - 1, core)
            for copy in ring_copies(direction, v, *src):
                copy.wait_send()
        for k in range(n):
            src = own(direction) if k == 0 else held(direction, k, core)
            for copy in pair_copies(direction, k, core, *src):
                copy.wait_send()
            sum_copy(k, direction).wait_send()
        for u in range(len(order)):
            rs_copy(direction, u).wait_send()


def moe(n_ep, r, gates, y, w_gate, w_up, w_down):
    n = n_ep // 2
    rows, d = r.shape
    n_local, _, ff = w_gate.shape
    vm = pl.BlockSpec(memory_space=pltpu.VMEM)
    hbm = pl.BlockSpec(memory_space=pltpu.HBM)
    dma = pltpu.SemaphoreType.DMA
    n_rs = 2 * (n - 1)
    return pl.pallas_call(
        functools.partial(moe_kernel, n),
        out_shape=jax.ShapeDtypeStruct((rows, d), BF16),
        in_specs=[vm] * 3 + [hbm] * 3,
        out_specs=vm,
        scratch_shapes=[
            pltpu.VMEM((n, 2, 2, rows // 2, d), BF16),
            pltpu.VMEM((n, 2, 2) + gates.shape[1:], F32),
            pltpu.VMEM((n, 2, 2, rows // 2, d), F32),
            pltpu.VMEM((n, 2, rows // 2, d), F32),
            pltpu.VMEM((2, n // 2 + 1, 4, rows // 4, d), F32),
            pltpu.VMEM(w_gate.shape, BF16), pltpu.VMEM(w_up.shape, BF16), pltpu.VMEM(w_down.shape, BF16),
            pltpu.VMEM((2 * rows, ff), BF16),
            pltpu.VMEM((n_local, 2 * rows, rows), F32),
            dma((3,)),
            dma((2, n - 1)), dma((2, n - 1)), dma((2, n - 1)), dma((2, n - 1)),
            dma((n, 2)), dma((n, 2)), dma((n, 2)), dma((n, 2)),
            dma((n, 2)), dma((n, 2)),
            dma((2, n_rs)), dma((2, n_rs)),
        ],
        compiler_params=pltpu.CompilerParams(collective_id=0, has_side_effects=True, vmem_limit_bytes=40 * 1024 * 1024),
        name="moe",
    )(r, gates, y, *in_hbm(w_gate, w_up, w_down))


def solution(mesh):
    n_ep = mesh.shape['ep']
    row_spec = P(('dp', 'ep'), None)
    cache_spec = P(('dp', 'ep'), None, None, None)
    len_spec = P(('dp', 'ep'))
    rep_vec = P(None)
    rep_mat = P(None, None)
    exp_spec = P('ep', None, None)

    def local_step(hidden, k_cache, v_cache, seq_lens, expert_ids, ln_attn, w_q, w_k, w_v, q_gain, k_gain, w_o, ln_moe, w_router, w_gate, w_up, w_down):
        k_t = jnp.transpose(k_cache, (1, 2, 3, 0))
        v_t = jnp.transpose(v_cache, (1, 2, 3, 0))
        k_new, v_new, y, r, gates = attend(
            hidden, k_t, v_t, seq_lens[None, :], expert_ids.T, ln_attn.reshape(-1, 128), w_q, w_k, w_v,
            q_gain[None, :], k_gain[None, :], w_o, ln_moe.reshape(-1, 128), w_router.T)
        out = moe(n_ep, r, gates, y, w_gate, w_up, w_down)
        return out, jnp.transpose(k_new, (3, 0, 1, 2)), jnp.transpose(v_new, (3, 0, 1, 2))

    return jax.shard_map(local_step, mesh=mesh, in_specs=(row_spec, cache_spec, cache_spec, len_spec, row_spec, rep_vec, rep_mat, rep_mat, rep_mat, rep_vec, rep_vec, rep_mat, rep_vec, rep_mat, exp_spec, exp_spec, exp_spec), out_specs=(row_spec, cache_spec, cache_spec), check_vma=False)
```
